256 devices in a mesh: ga: 32 (over y, x, z_hi), band: 8 (over z_lo, core).
Axes of the slice: x: 4, y: 4, z: 8 (z_hi: 2, z_lo: 4; z = z_hi * 4 + z_lo), core: 2. Of those that a mesh axis runs over, the one named last changes fastest.
Arguments:
- coefficients: float32 [2048, 2, 16384], P('band', None, 'ga'), may hold values from -6 to 6
- rotation: float32 [2, 2048, 256], P(None, 'band', 'ga'), may hold values from -0.1875 to 0.1875
- potential: float32 [64, 4096], P(None, 'ga'), may hold values from -2 to 0.5
- index_map: int32 [16384], replicated, may hold values from 0 to 262143, as said below
- counts: int32 [32], replicated, may hold values from 384 to 512, as said below
Outputs:
- applied_panel: float32 [256, 2, 32, 1024], P(('band', 'ga'))
The draws below stay inside these ranges and needn't reach their ends.
Inputs may be any that keep to these rules, and one draw needn't show every extreme that they name: counts[i] counts the live slots of index i of ga, which are its slots 0 to counts[i] - 1 of 512; the counts sum to 14336, and some index has exactly 512. `index_map`: live slots name distinct cells, and together exactly 14336 cells whose signed frequency vector has a squared length no larger than that of any cell not named (a ball about the anchor), every signed component of a live cell lying in -16 to 15; dead slots name arbitrary cells.
All inputs are finite; a program needn't handle non-finite values.
Results may differ from the reference program's by a relative error of at most 0.00008.
Values sent between devices are 32-bit elements; how exact they have to be, the bound alone decides.
A program may use at most 128 MiB of HBM per device.

```python
import jax
import jax.numpy as jnp
from jax import lax

BANDS = 2048
BOX = 64
SLOT_DEV = 512
PW_DEV = 448
NPW = 14336
PANEL = 256
N_GA = 32


def layout_draw(key):
    folded = jax.random.fold_in(key, 7)
    key_ties, key_shuffle, key_pairs, key_order, key_dead = jax.random.split(folded, 5)
    cell_count = BOX * BOX * BOX
    flat_cells = jnp.arange(cell_count, dtype=jnp.int32)
    freq_x = flat_cells // (BOX * BOX)
    freq_y = flat_cells // BOX % BOX
    freq_z = flat_cells % BOX
    freq_x = jnp.where(freq_x >= BOX // 2, freq_x - BOX, freq_x)
    freq_y = jnp.where(freq_y >= BOX // 2, freq_y - BOX, freq_y)
    freq_z = jnp.where(freq_z >= BOX // 2, freq_z - BOX, freq_z)
    squared_norm = freq_x * freq_x + freq_y * freq_y + freq_z * freq_z
    ties_rank = jax.random.permutation(key_ties, cell_count).astype(jnp.int32)
    ranking = jnp.argsort(squared_norm * cell_count + ties_rank, stable=True).astype(jnp.int32)
    ball_cells = jax.random.permutation(key_shuffle, ranking[:NPW])
    dead_mean = SLOT_DEV - PW_DEV
    pair_count = N_GA // 2
    shifts = jax.random.randint(key_pairs, (pair_count,), -dead_mean, dead_mean + 1).astype(jnp.int32)
    shifts = shifts.at[0].set(dead_mean)
    dead_slots = jnp.concatenate([dead_mean + shifts, dead_mean - shifts])
    dead_slots = jax.random.permutation(key_order, dead_slots)
    counts = (SLOT_DEV - dead_slots).astype(jnp.int32)
    offsets = jnp.cumsum(counts) - counts
    slot_ids = jnp.arange(SLOT_DEV, dtype=jnp.int32)
    slot_pos = jnp.clip(offsets[:, None] + slot_ids[None, :], 0, NPW - 1)
    live_mask = slot_ids[None, :] < counts[:, None]
    filler = jax.random.randint(key_dead, (N_GA, SLOT_DEV), 0, cell_count).astype(jnp.int32)
    index_map = jnp.where(live_mask, ball_cells[slot_pos], filler).reshape(-1).astype(jnp.int32)
    return (index_map, counts)


def draw_index_map(key, part):
    return layout_draw(key)[0]


def draw_counts(key, part):
    return layout_draw(key)[1]


def spiked(entries, rng, source, target, shards_of, factor):
    owner, partner = [(jnp.arange(entries.shape[dim]) // (entries.shape[dim] // shards_of)).reshape([-1 if axis == dim else 1 for axis in range(entries.ndim)]) for dim in (source, target)]
    chosen = jax.random.permutation(rng, shards_of)[partner]
    strong = (owner == chosen) | (owner == (partner + shards_of // 2) % shards_of)
    return jnp.where(strong, factor * entries, entries)


def level_of(own_key, extent, cuts, least, largest):
    level = 1.0
    for axis_at, shards_of in cuts:
        draws = jax.random.uniform(jax.random.fold_in(jax.random.fold_in(own_key, 6), axis_at), (shards_of,), jnp.float32, least / len(cuts), largest / len(cuts))
        level = level * jnp.repeat(jnp.exp(draws), extent[axis_at] // shards_of).reshape((-1,) + (1,) * (len(extent) - 1 - axis_at))
    return level


def normal_values(rng, extent, deviation, limit, pieces=(), held_as=jnp.bfloat16):
    values = deviation * jax.random.normal(rng, extent, jnp.float32)
    if pieces:
        values = values * level_of(rng, extent, pieces, -0.22, 0.18)
    return jnp.clip(values, -limit, limit).astype(held_as)


def noise_with(key, dims, width, limit, pieces, heavy, kind=jnp.bfloat16):
    result = width * jax.random.normal(key, dims, jnp.float32)
    if pieces:
        result = result * level_of(key, dims, pieces, -0.22, 0.18)
    return jnp.clip(spiked(result, jax.random.fold_in(key, 3), *heavy), -limit, limit).astype(kind)


def setup_inputs(seed: int = 0) -> dict:
    streams_of = jax.random.split(jax.random.key(seed), 6)
    coefficients = normal_values(streams_of[0], (BANDS, 2, SLOT_DEV * N_GA), 1.0, 6.0, ((0, 8), (2, 32)), jnp.float32)
    rotation = noise_with(streams_of[1], (2, BANDS, PANEL), (2 * BANDS) ** -0.5, 0.1875, ((1, 8), (2, 32)), (1, 2, 32, 2.75), jnp.float32)
    potential = jnp.clip(-2.0 + 2.5 * jax.random.uniform(streams_of[2], (BOX, BOX * BOX), jnp.float32) ** level_of(streams_of[2], (BOX, BOX * BOX), ((1, 32),), -0.2, 0.2), -2.0, 0.5)
    index_map = draw_index_map(jax.random.fold_in(streams_of[5], 71), 0)
    counts = draw_counts(jax.random.fold_in(streams_of[5], 71), 0)
    return {"coefficients": coefficients, "rotation": rotation, "potential": potential, "index_map": index_map, "counts": counts}


def mixing(columns):
    real_cols = columns[0].T
    imag_cols = columns[1].T
    upper_rows = jnp.stack([real_cols, -imag_cols], axis=-1)
    lower_rows = jnp.stack([imag_cols, real_cols], axis=-1)
    stacked = jnp.stack([upper_rows, lower_rows], axis=1)
    return stacked.reshape(2 * real_cols.shape[0], 2 * real_cols.shape[1])


def kinetic_grid(box_edge):
    ticks_index = jnp.arange(box_edge, dtype=jnp.int32)
    signed = jnp.where(ticks_index >= box_edge // 2, ticks_index - box_edge, ticks_index).astype(jnp.float32)
    squared = signed[:, None, None] ** 2 + signed[None, :, None] ** 2 + signed[None, None, :] ** 2
    return (8.0 / (box_edge * box_edge)) * squared


def reference(coefficients, rotation, potential, index_map, counts):
    band_count = coefficients.shape[0]
    slot_total = coefficients.shape[2]
    mixer_rows = mixing(rotation)
    rotated = jnp.dot(mixer_rows, coefficients.reshape(2 * band_count, slot_total),
                      precision=lax.Precision.HIGHEST).reshape(PANEL, 2, slot_total)
    slot_ids = jnp.arange(SLOT_DEV, dtype=jnp.int32)
    live_mask = (slot_ids[None, :] < counts[:, None]).reshape(-1).astype(jnp.float32)
    kinetic = kinetic_grid(BOX)
    pot_grid = potential.reshape(BOX, BOX, BOX)
    window = BOX // 2
    window_ids = ((jnp.arange(window, dtype=jnp.int32) - window // 2) % BOX).astype(jnp.int32)

    def one_band(values):
        masked = values * live_mask[None, :]
        box_cells = jnp.zeros((2, BOX * BOX * BOX), jnp.float32).at[:, index_map].add(masked)
        grid_field = (box_cells[0] + 1j * box_cells[1]).reshape(BOX, BOX, BOX)
        real_space = jnp.fft.ifftn(grid_field)
        applied = jnp.fft.fftn(pot_grid * real_space) + kinetic * grid_field
        applied = jnp.take(applied, window_ids, axis=0)
        applied = jnp.take(applied, window_ids, axis=1)
        applied = jnp.take(applied, window_ids, axis=2)
        return jnp.stack([applied.real, applied.imag]).reshape(2, window, window * window)

    return lax.map(one_band, rotated)
```

```python
import functools
import math

import jax
import jax.numpy as jnp
import numpy as np
from jax import lax
from jax.experimental import pallas as pl
from jax.experimental.pallas import tpu as pltpu
from jax.sharding import PartitionSpec as P

F32 = jnp.float32
BF16 = jnp.bfloat16


def split_parts(values):
    high = values.astype(BF16)
    return high, (values - high.astype(F32)).astype(BF16)


def two_parts(table):
    high = table.astype(BF16)
    low = (table - high.astype(np.float32)).astype(BF16)
    return np.stack([high, low])


def tables(box, window, radix):
    half = window // 2
    coarse = window // radix
    k_all = np.arange(box)
    k_coarse = np.arange(box // radix)
    n_signed = np.arange(window) - half
    low = np.arange(radix)
    y_phase = (radix * np.arange(coarse) - half)[:, None] * low[None, :]
    z_phase = n_signed[:, None] * k_all[None, :]
    right = y_phase[:, None, :, None] + z_phase[None, :, None, :]
    right = right.reshape(coarse * window, radix * box) % box
    x_phase = k_all[:, None] * n_signed[None, :]
    l_phase = radix * k_coarse[:, None] * low[None, :]
    left = l_phase[:, None, :, None] + x_phase[None, :, None, :]
    left = left.reshape(k_coarse.size * box, radix * window) % box
    twist = np.repeat(low[:, None] * low[None, :], box, axis=1) % box

    def pair(phase, scale=1.0):
        angle = phase * (2.0 * math.pi / box)
        return (np.stack([np.cos(angle), np.sin(angle)]) * scale).astype(np.float32)

    right_tab = two_parts(pair(right))
    left_pair = pair(left, 1.0 / box**3)
    left_tab = two_parts(left_pair)
    back_tab = two_parts((left_pair * np.float32(box**3)).transpose(0, 2, 1).copy())
    return right_tab, left_tab, back_tab, pair(twist)


def dot3(lhs, rhs, dims=((1,), (0,))):
    def one(a, b):
        return lax.dot_general(a, b, (dims, ((), ())), preferred_element_type=F32)

    return one(lhs[0], rhs[0]) + (one(lhs[0], rhs[1]) + one(lhs[1], rhs[0]))


def block(cos, sin):
    upper = jnp.concatenate([cos, sin], axis=1)
    lower = jnp.concatenate([-sin, cos], axis=1)
    return jnp.concatenate([upper, lower], axis=0)


def whole_kernel(
    box, window, radix, coef_hbm, rot_hbm, pot_hbm, idx_hbm, cnt_hbm, right_hbm, left_hbm, back_hbm, twist_hbm,
    out_ref, coef, coef_parts, rot_own, rots, psend, drecv, ssum, zrecv, tout, land, onehot, hits, placed, acc, idx, cnt,
    pot_out, right_tab, left_tab, back_tab, twist, right_blk, left_blk, back_blk,
    load_sem, rot_send, rot_recv, pot_send, pot_recv, pair_send, pair_recv, line_send, line_recv, val_send, val_recv
):
    band = lax.axis_index("band")
    me = lax.axis_index("ga")
    groups = 2 * rots.shape[1]
    plane = groups // 2
    lines = ssum.shape[1]
    line, core = band // 2, lax.rem(band, 2)
    cell, side = me // 2, lax.rem(me, 2)
    across = cell * 2 + (1 - side)
    sibling = line * 2 + (1 - core)
    mirror = (lines - 1 - line) * 2 + core
    half_rows = pot_hbm.shape[0] // 2
    share = pl.ds(pl.multiple_of(core * half_rows, half_rows), half_rows)
    slots = coef.shape[2]

    def local(src, dst, i):
        copy = pltpu.make_async_copy(src, dst, load_sem.at[i])
        copy.start()
        return copy

    rot_load = local(rot_hbm.at[0], rot_own, 0)
    idx_load = local(idx_hbm, idx, 1)
    cnt_load = local(cnt_hbm, cnt, 2)
    coef_loads = [local(coef_hbm.at[:, c, :], coef.at[c], 3 + c) for c in range(2)]
    pot_load = local(pot_hbm, pot_out.at[me], 5)
    tab_loads = [
        local(src, dst, 6 + i)
        for i, (src, dst) in enumerate(
            ((right_hbm, right_tab), (left_hbm, left_tab), (back_hbm, back_tab), (twist_hbm, twist))
        )
    ]

    barrier = pltpu.get_barrier_semaphore()

    def greet(to_band, to):
        pl.semaphore_signal(
            barrier, inc=1, device_id={"band": to_band, "ga": to}, device_id_type=pl.DeviceIdType.MESH
        )

    def peers(act):
        def body(step, carry):
            act(lax.rem(cell + step, plane))
            return carry

        lax.fori_loop(1, plane, body, 0)

    def lines_other(act):
        for step in range(1, lines):
            act(lax.rem(line + step, lines))

    def remote(src, dst, send, recv, to_band, to):
        return pltpu.make_async_remote_copy(
            src_ref=src, dst_ref=dst, send_sem=send, recv_sem=recv,
            device_id={"band": to_band, "ga": to}, device_id_type=pl.DeviceIdType.MESH,
        )

    with jax.named_scope("barrier"):
        peers(lambda q: greet(band, q * 2 + side))
        greet(band, across)
        greet(mirror, across)
        greet(sibling, me)
        lines_other(lambda l: greet(l * 2 + core, me))
        pl.semaphore_wait(barrier, plane - 1 + 3 + lines - 1)

    def rot_swap():
        return remote(rot_own, rots.at[side, cell], rot_send.at[0], rot_recv.at[0], band, across)

    def rot_copy(which, held, q):
        slot = rots.at[held, cell]
        src = rot_own if which == 1 else slot
        return remote(src, slot, rot_send.at[which], rot_recv.at[which], band, q * 2 + side)

    def rot_all(which):
        part = rots.at[0, pl.ds(0, plane - 1)]
        return remote(part, part, rot_send.at[which], rot_recv.at[which], band, across)

    def pot_swap():
        part = pot_out.at[me, share]
        return remote(part, part, pot_send.at[0], pot_recv.at[0], mirror, across)

    def pot_copy(which, piece, q):
        part = pot_out.at[piece, share]
        return remote(part, part, pot_send.at[which], pot_recv.at[which], band, q * 2 + side)

    def pot_all(which):
        part = pot_out.at[pl.ds(0, plane - 1), pl.ds(0, half_rows)]
        return remote(part, part, pot_send.at[which], pot_recv.at[which], band, across)

    def pot_pair():
        part = pot_out.at[:, share]
        return remote(part, part, pot_send.at[3], pot_recv.at[3], sibling, me)

    def pair_copy(step):
        return remote(psend.at[step], drecv.at[step], pair_send.at[step], pair_recv.at[step], sibling, me)

    def line_copy(step, l):
        return remote(
            ssum.at[step, l], zrecv.at[step, line], line_send.at[step], line_recv.at[step], l * 2 + core, me
        )

    def line_all(step):
        part = zrecv.at[step, pl.ds(0, lines - 1)]
        return remote(part, part, line_send.at[step], line_recv.at[step], sibling, me)

    def val_copy(step, i, to):
        return remote(
            tout.at[step, i], land.at[side, cell], val_send.at[step], val_recv.at[step], band, to
        )

    def val_all(step, recv_at, count):
        part = land.at[0, pl.ds(0, count)]
        return remote(part, part, val_send.at[step], val_recv.at[recv_at], band, across)

    with jax.named_scope("send_rot"):
        rot_load.wait()
        rot_swap().start()
        peers(lambda q: rot_copy(1, side, q).start())
        rots[side, cell] = rot_own[...]
        pot_load.wait()
        pot_swap().start()

    def mark(src, carry):
        at = pl.ds(pl.multiple_of(src * slots, slots), slots)
        to = pl.ds(pl.multiple_of(src // 2 * slots, slots), slots)
        half = window // 2
        cells = idx[:, at]
        cell_x = (cells // (box * box) + half) % box
        cell_y = (cells // box % box + half) % box
        cell_z = (cells % box + half) % box
        inside = (cell_x < window) & (cell_y < window) & (cell_z < window)
        live = lax.broadcasted_iota(jnp.int32, (1, slots), 1) < cnt[src]
        row_id = jnp.where(live & inside, cell_y % radix * window + cell_x, -1)
        col_id = cell_y // radix * window + cell_z
        rows, cols = onehot.shape[1], hits.shape[1]
        picks = lax.broadcasted_iota(jnp.int32, (rows, slots), 0) == row_id
        onehot[lax.rem(src, 2), :, to] = jnp.where(picks, 1.0, 0.0).astype(BF16)
        found = lax.broadcasted_iota(jnp.int32, (cols, slots), 0) == col_id
        hits[lax.rem(src, 2), :, to] = jnp.where(found, 1.0, 0.0).astype(BF16)
        return carry

    with jax.named_scope("split_coef"):
        for c in range(2):
            coef_loads[c].wait()
            high, low = split_parts(coef[c])
            coef_parts[2 * c] = high
            coef_parts[2 * c + 1] = low
    with jax.named_scope("mark0"):
        idx_load.wait()
        cnt_load.wait()
        lax.fori_loop(0, plane // 2, mark, 0)

    with jax.named_scope("relay_rot"):
        rot_swap().wait_recv()
        peers(lambda q: rot_copy(2, 1 - side, q).start())

    def rotate(held, to_core):
        blocks = []
        for l in range(lines):
            for r in range(2):
                blocks.append(rots[held, l * 4 + to_core * 2 + r])
        a = jnp.concatenate(blocks, axis=0)
        b = jnp.concatenate(
            [piece for blk in blocks for piece in (-blk[8:], blk[:8])], axis=0
        )
        a_high, a_low = split_parts(a)
        b_high, b_low = split_parts(b)
        lhs = jnp.concatenate([a_high, a_low, a_high, b_high, b_low, b_high], axis=1)
        rhs = jnp.concatenate(
            [coef_parts[0], coef_parts[0], coef_parts[1], coef_parts[2], coef_parts[2], coef_parts[3]], axis=0
        )
        return jnp.dot(lhs, rhs, preferred_element_type=F32).reshape(lines, 2, 2, 8, slots)

    def first_part(step, held):
        with jax.named_scope(f"rotate{step}"):
            psend[step] = rotate(held, 1 - core)
            pair_copy(step).start()
            ssum[step] = rotate(held, core)

    def second_part(step):
        with jax.named_scope(f"pair{step}"):
            pair_copy(step).wait_recv()
            ssum[step] = ssum[step] + drecv[step]
            lines_other(lambda l: line_copy(step, l).start())

    def third_part(step, held):
        with jax.named_scope(f"wait_line{step}"):
            line_all(step).wait_recv()
        with jax.named_scope(f"send_val{step}"):
            total = ssum[step, line]
            for other in range(1, lines):
                total = total + zrecv[step, lax.rem(line + other, lines)]
            for r in range(2):
                for c in range(2):
                    tout[step, r * 8 : (r + 1) * 8, c, :] = total[r, c]

            def send(i, carry):
                to = i // 8 * 16 + held * 8 + lax.rem(i, 8)

                @pl.when(to != me)
                def _():
                    val_copy(step, i, to).start()

                @pl.when(to == me)
                def _():
                    land[side, cell] = tout[step, i]

                return carry

            lax.fori_loop(0, 16, send, 0)

    with jax.named_scope("wait_rot0"):
        rot_all(1).wait_recv()
    first_part(0, side)
    with jax.named_scope("relay_pot"):
        pot_swap().wait_recv()
        peers(lambda q: pot_copy(1, me, q).start())
        peers(lambda q: pot_copy(2, across, q).start())
    second_part(0)
    with jax.named_scope("wait_rot1"):
        rot_all(2).wait_recv()
    first_part(1, 1 - side)
    second_part(1)
    with jax.named_scope("mark1"):
        lax.fori_loop(plane // 2, groups, mark, 0)
    with jax.named_scope("blocks"):
        for tab in tab_loads:
            tab.wait()
        for i in range(2):
            right_blk[i] = block(right_tab[i, 0], right_tab[i, 1])
            left_blk[i] = block(left_tab[i, 0], -left_tab[i, 1])
            back_blk[i] = block(back_tab[i, 0], back_tab[i, 1])
    third_part(0, side)
    third_part(1, 1 - side)
    with jax.named_scope("pair_pot"):
        pot_all(1).wait_recv()
        pot_all(2).wait_recv()
        pot_pair().start()

    early = lax.rem(me // 8, 2)
    mine_first = early == side

    def gather(parity, alone, recv_at):
        @pl.when(alone)
        def _():
            val_all(0, recv_at, plane - 1).wait_recv()

        @pl.when(jnp.logical_not(alone))
        def _():
            val_all(0, recv_at, plane).wait_recv()

        def put(u, carry):
            to = pl.ds(pl.multiple_of(u * slots, slots), slots)
            high, low = split_parts(land[parity, u])
            mask = hits[parity, :, to]
            cols = hits.shape[1]
            for n, part in enumerate((high, low)):
                part = part.astype(F32)
                for c in range(2):
                    row = jnp.broadcast_to(part[c : c + 1, :], (16, slots)).astype(BF16)
                    full = jnp.concatenate([row] * (cols // 16), axis=0)
                    at = (2 * n + c) * cols
                    placed[at : at + cols, to] = mask * full
            return carry

        lax.fori_loop(0, plane, put, 0)
        return lax.dot_general(
            onehot[parity], placed[...], (((1,), (1,)), ((), ())), preferred_element_type=F32
        )

    acc[...] = jnp.zeros_like(acc)

    def collect(batch, carry):
        parity = lax.rem(early + batch, 2)
        with jax.named_scope("collect"):
            acc[...] += gather(parity, parity == side, batch)
        return carry

    lax.fori_loop(0, 2, collect, 0)
    cols = hits.shape[1]
    grid_field = acc[:, : 2 * cols] + acc[:, 2 * cols :]

    def pot_ready():
        pot_pair().wait_recv()

    apply_kernel(
        box, window, radix, 0, pot_ready, grid_field, pot_out, right_blk, left_blk, back_blk, twist, out_ref
    )
    with jax.named_scope("wait_sends"):
        rot_swap().wait_send()
        rot_all(1).wait_send()
        rot_all(2).wait_send()
        pot_swap().wait_send()
        pot_all(1).wait_send()
        pot_all(2).wait_send()
        pot_pair().wait_send()
        for step in range(2):
            pair_copy(step).wait_send()
            line_all(step).wait_send()
            alone = mine_first if step == 0 else jnp.logical_not(mine_first)

            @pl.when(alone)
            def _():
                val_all(step, 0, plane - 1).wait_send()

            @pl.when(jnp.logical_not(alone))
            def _():
                val_all(step, 0, plane).wait_send()


def run(coefficients, rotation, potential, index_map, counts, consts, box, window, radix):
    bands, groups = lax.axis_size("band"), lax.axis_size("ga")
    depth, _, slots = coefficients.shape
    cols = rotation.shape[2]
    assert (bands, groups, cols) == (8, 32, 8)
    lines, plane = bands // 2, groups // 2
    rot = rotation.transpose(0, 2, 1).reshape(1, 2 * cols, depth)
    hbm = pl.BlockSpec(memory_space=pl.ANY)
    vmem = pl.BlockSpec(memory_space=pltpu.VMEM)
    dma = pltpu.SemaphoreType.DMA
    rows, wide = radix * window, window // radix * window
    blocks = (2, lines, 2, 2, 8, slots)
    tabs = consts[:3]
    return pl.pallas_call(
        functools.partial(whole_kernel, box, window, radix),
        out_shape=jax.ShapeDtypeStruct((1, 2, window, window * window), F32),
        in_specs=[hbm] * 9,
        out_specs=vmem,
        scratch_shapes=[
            pltpu.VMEM((2, depth, slots), F32),
            pltpu.VMEM((4, depth, slots), BF16),
            pltpu.VMEM((2 * cols, depth), F32),
            pltpu.VMEM((2, plane, 2 * cols, depth), F32),
            pltpu.VMEM(blocks, F32),
            pltpu.VMEM(blocks, F32),
            pltpu.VMEM(blocks, F32),
            pltpu.VMEM(blocks, F32),
            pltpu.VMEM((2, 16, 2, slots), F32),
            pltpu.VMEM((2, plane, 2, slots), F32),
            pltpu.VMEM((2, rows, plane * slots), BF16),
            pltpu.VMEM((2, wide, plane * slots), BF16),
            pltpu.VMEM((4 * wide, plane * slots), BF16),
            pltpu.VMEM((rows, 4 * wide), F32),
            pltpu.VMEM((1, groups * slots), jnp.int32),
            pltpu.SMEM((groups,), jnp.int32),
            pltpu.VMEM((groups,) + potential.shape, F32),
            *[pltpu.VMEM(table.shape, table.dtype) for table in consts],
            *[pltpu.VMEM((2, 2 * table.shape[2], 2 * table.shape[3]), table.dtype) for table in tabs],
            dma((10,)),
            dma((3,)),
            dma((3,)),
            dma((4,)),
            dma((4,)),
            dma((2,)),
            dma((2,)),
            dma((2,)),
            dma((2,)),
            dma((2,)),
            dma((2,)),
        ],
        compiler_params=pltpu.CompilerParams(
            collective_id=0, has_side_effects=True, vmem_limit_bytes=60 * 1024 * 1024
        ),
    )(coefficients, rot, potential, index_map[None], counts, *consts)


def apply_kernel(
    box, window, radix, index, pot_ready, grid_field, pot_ref, right_ref, left_ref, back_ref, twist_ref, out_ref
):
    coarse = window // radix
    rows = radix * window
    cols = coarse * window
    wide = radix * box

    with jax.named_scope("fwd_fft"):
        right = [right_ref[i] for i in range(2)]
        field = dot3(split_parts(grid_field), right)
        cos = twist_ref[0][:, None, :]
        sin = twist_ref[1][:, None, :]
        real = field[:, :wide].reshape(radix, window, wide)
        imag = field[:, wide:].reshape(radix, window, wide)
        turned = jnp.concatenate(
            [
                (real * cos - imag * sin).reshape(rows, wide),
                (real * sin + imag * cos).reshape(rows, wide),
            ],
            axis=0,
        )
        left = [left_ref[i] for i in range(2)]
        space = dot3(left, split_parts(turned))
    if pot_ready is not None:
        with jax.named_scope("wait_pot"):
            pot_ready()
    per = pot_ref.shape[0] // (box // radix)
    pot = jnp.concatenate(
        [
            jnp.concatenate([pot_ref[k * per + i] for i in range(per)], axis=1)
            for k in range(box // radix)
        ],
        axis=0,
    )
    space = space * jnp.concatenate([pot, pot], axis=0)
    with jax.named_scope("back_fft"):
        back = [back_ref[i] for i in range(2)]
        field = dot3(back, split_parts(space))
        real = field[:rows].reshape(radix, window, wide)
        imag = field[rows:].reshape(radix, window, wide)
        turned = jnp.concatenate(
            [
                (real * cos + imag * sin).reshape(rows, wide),
                (imag * cos - real * sin).reshape(rows, wide),
            ],
            axis=1,
        )
        applied = dot3(split_parts(turned), right, ((1,), (1,)))

    half = window // 2
    row_at = lax.broadcasted_iota(jnp.int32, (rows, cols), 0)
    col_at = lax.broadcasted_iota(jnp.int32, (rows, cols), 1)
    n_x = (row_at % window - half).astype(F32)
    n_y = (col_at // window * radix + row_at // window - half).astype(F32)
    n_z = (col_at % window - half).astype(F32)
    kinetic = (8.0 / (box * box)) * (n_x * n_x + n_y * n_y + n_z * n_z)
    applied = applied + jnp.concatenate([kinetic, kinetic], axis=1) * grid_field
    for c in range(2):
        pieces = [
            applied[lo * window : (lo + 1) * window, c * cols + hi * window : c * cols + (hi + 1) * window]
            for hi in range(coarse)
            for lo in range(radix)
        ]
        out_ref[index, c] = jnp.concatenate(pieces, axis=1)


def per_device(coefficients, rotation, potential, index_map, counts):
    box = potential.shape[0]
    window = box // 2
    radix = math.isqrt(box)
    assert radix * radix == box
    consts = [jnp.asarray(t) for t in tables(box, window, radix)]
    return run(coefficients, rotation, potential, index_map, counts, consts, box, window, radix)


def solution(mesh):
    placed = (P("band", None, "ga"), P(None, "band", "ga"), P(None, "ga"), P(), P())
    return jax.shard_map(
        per_device,
        mesh=mesh,
        in_specs=placed,
        out_specs=P(("band", "ga"), None, None, None),
        check_vma=False,
    )
```

```python
import functools
import math

import jax
import jax.numpy as jnp
import numpy as np
from jax import lax
from jax.experimental import pallas as pl
from jax.experimental.pallas import tpu as pltpu
from jax.sharding import PartitionSpec as P

F32 = jnp.float32
BF16 = jnp.bfloat16


def split_parts(values):
    high = values.astype(BF16)
    return high, (values - high.astype(F32)).astype(BF16)


def two_parts(table):
    high = table.astype(BF16)
    low = (table - high.astype(np.float32)).astype(BF16)
    return np.stack([high, low])


def tables(box, window, radix):
    half = window // 2
    coarse = window // radix
    k_all = np.arange(box)
    n_signed = np.arange(window) - half
    low = np.arange(radix)
    y_phase = (radix * np.arange(coarse) - half)[:, None] * low[None, :]
    z_phase = n_signed[:, None] * k_all[None, :]
    right = y_phase[:, None, :, None] + z_phase[None, :, None, :]
    right = right.reshape(coarse * window, radix * box) % box
    x_phase = k_all[:, None] * n_signed[None, :] % box
    twist = np.repeat(low[:, None] * low[None, :], box, axis=1) % box

    def pair(phase, scale=1.0):
        angle = phase * (2.0 * math.pi / box)
        return (np.stack([np.cos(angle), np.sin(angle)]) * scale).astype(np.float32)

    right_tab = two_parts(pair(right))
    cos, sin = pair(x_phase)
    left_high, left_low = two_parts(np.block([[cos, -sin], [sin, cos]]) / np.float32(box**3))
    left_tab = np.concatenate([left_high, left_low, left_high, left_low], axis=1)
    back_high, back_low = two_parts(np.block([[cos.T, sin.T], [-sin.T, cos.T]]))
    back_tab = np.block([[back_high, back_high], [back_low, back_low]])
    return right_tab, left_tab, back_tab, pair(twist)


def fft8(values, sign):
    root = math.sqrt(0.5)

    def add(a, b):
        return a[0] + b[0], a[1] + b[1]

    def sub(a, b):
        return a[0] - b[0], a[1] - b[1]

    def turn(a):
        return (-a[1], a[0]) if sign > 0 else (a[1], -a[0])

    def fft4(a, b, c, d):
        total, diff = add(a, c), sub(a, c)
        other, cross = add(b, d), turn(sub(b, d))
        return add(total, other), add(diff, cross), sub(total, other), sub(diff, cross)

    even = fft4(*values[0::2])
    odd = list(fft4(*values[1::2]))
    one, three = odd[1], odd[3]
    one_turn, three_turn = turn(one), turn(three)
    odd[1] = ((one[0] + one_turn[0]) * root, (one[1] + one_turn[1]) * root)
    odd[2] = turn(odd[2])
    odd[3] = ((three_turn[0] - three[0]) * root, (three_turn[1] - three[1]) * root)
    return [add(a, b) for a, b in zip(even, odd)] + [sub(a, b) for a, b in zip(even, odd)]


def dot3(lhs, rhs, dims=((1,), (0,))):
    def one(a, b):
        return lax.dot_general(a, b, (dims, ((), ())), preferred_element_type=F32)

    return one(lhs[0], rhs[0]) + (one(lhs[0], rhs[1]) + one(lhs[1], rhs[0]))


def block(cos, sin):
    upper = jnp.concatenate([cos, sin], axis=1)
    lower = jnp.concatenate([-sin, cos], axis=1)
    return jnp.concatenate([upper, lower], axis=0)


def whole_kernel(
    box, window, radix, coef_hbm, rot_hbm, pot_hbm, idx_hbm, cnt_hbm, right_hbm, left_hbm, back_hbm, twist_hbm,
    out_ref, coef, coef_parts, rot_own, rots, psend, drecv, ssum, zrecv, tout, land, onehot, hits, placed, acc, idx, cnt,
    pot_out, right_tab, left_tab, back_tab, twist, right_blk, field, mixed, unmixed, turned,
    load_sem, rot_send, rot_recv, pot_send, pot_recv, pair_send, pair_recv, line_send, line_recv, val_send, val_recv
):
    band = lax.axis_index("band")
    me = lax.axis_index("ga")
    groups = 2 * rots.shape[1]
    plane = groups // 2
    lines = ssum.shape[1]
    line, core = band // 2, lax.rem(band, 2)
    cell, side = me // 2, lax.rem(me, 2)
    across = cell * 2 + (1 - side)
    sibling = line * 2 + (1 - core)
    mirror = (lines - 1 - line) * 2 + core
    half_rows = pot_hbm.shape[0] // 2
    share = pl.ds(pl.multiple_of(core * half_rows, half_rows), half_rows)
    slots = coef.shape[2]

    def local(src, dst, i):
        copy = pltpu.make_async_copy(src, dst, load_sem.at[i])
        copy.start()
        return copy

    rot_load = local(rot_hbm.at[0], rot_own, 0)
    idx_load = local(idx_hbm, idx, 1)
    cnt_load = local(cnt_hbm, cnt, 2)
    coef_loads = [local(coef_hbm.at[:, c, :], coef.at[c], 3 + c) for c in range(2)]
    pot_load = local(pot_hbm, pot_out.at[me], 5)
    tab_loads = [
        local(src, dst, 6 + i)
        for i, (src, dst) in enumerate(
            ((right_hbm, right_tab), (left_hbm, left_tab), (back_hbm, back_tab), (twist_hbm, twist))
        )
    ]

    barrier = pltpu.get_barrier_semaphore()

    def greet(to_band, to):
        pl.semaphore_signal(
            barrier, inc=1, device_id={"band": to_band, "ga": to}, device_id_type=pl.DeviceIdType.MESH
        )

    def peers(act):
        def body(step, carry):
            act(lax.rem(cell + step, plane))
            return carry

        lax.fori_loop(1, plane, body, 0)

    def lines_other(act):
        for step in range(1, lines):
            act(lax.rem(line + step, lines))

    def remote(src, dst, send, recv, to_band, to):
        return pltpu.make_async_remote_copy(
            src_ref=src, dst_ref=dst, send_sem=send, recv_sem=recv,
            device_id={"band": to_band, "ga": to}, device_id_type=pl.DeviceIdType.MESH,
        )

    with jax.named_scope("barrier"):
        peers(lambda q: greet(band, q * 2 + side))
        greet(band, across)
        greet(mirror, across)
        greet(sibling, me)
        lines_other(lambda l: greet(l * 2 + core, me))
        pl.semaphore_wait(barrier, plane - 1 + 3 + lines - 1)

    def rot_swap():
        return remote(rot_own, rots.at[side, cell], rot_send.at[0], rot_recv.at[0], band, across)

    def rot_copy(which, held, q):
        slot = rots.at[held, cell]
        src = rot_own if which == 1 else slot
        return remote(src, slot, rot_send.at[which], rot_recv.at[which], band, q * 2 + side)

    def rot_all(which):
        part = rots.at[0, pl.ds(0, plane - 1)]
        return remote(part, part, rot_send.at[which], rot_recv.at[which], band, across)

    def pot_swap():
        part = pot_out.at[me, share]
        return remote(part, part, pot_send.at[0], pot_recv.at[0], mirror, across)

    def pot_copy(which, piece, q):
        part = pot_out.at[piece, share]
        return remote(part, part, pot_send.at[which], pot_recv.at[which], band, q * 2 + side)

    def pot_all(which):
        part = pot_out.at[pl.ds(0, plane - 1), pl.ds(0, half_rows)]
        return remote(part, part, pot_send.at[which], pot_recv.at[which], band, across)

    def pot_pair():
        part = pot_out.at[:, share]
        return remote(part, part, pot_send.at[3], pot_recv.at[3], sibling, me)

    def pair_copy(step):
        return remote(psend.at[step], drecv.at[step], pair_send.at[step], pair_recv.at[step], sibling, me)

    def line_copy(step, l):
        return remote(
            ssum.at[step, l], zrecv.at[step, line], line_send.at[step], line_recv.at[step], l * 2 + core, me
        )

    def line_all(step):
        part = zrecv.at[step, pl.ds(0, lines - 1)]
        return remote(part, part, line_send.at[step], line_recv.at[step], sibling, me)

    def val_copy(step, i, to):
        return remote(
            tout.at[step, i], land.at[side, cell], val_send.at[step], val_recv.at[step, cell // 4], band, to
        )

    def val_all(step, batch, row, count):
        part = land.at[0, pl.ds(0, count)]
        return remote(part, part, val_send.at[step], val_recv.at[batch, row], band, across)

    with jax.named_scope("send_rot"):
        rot_load.wait()
        rot_swap().start()
        peers(lambda q: rot_copy(1, side, q).start())
        rots[side, cell] = rot_own[...]
        pot_load.wait()
        pot_swap().start()

    def mark(src, carry):
        at = pl.ds(pl.multiple_of(src * slots, slots), slots)
        to = pl.ds(pl.multiple_of(src // 2 * slots, slots), slots)
        half = window // 2
        cells = idx[:, at]
        cell_x = (cells // (box * box) + half) % box
        cell_y = (cells // box % box + half) % box
        cell_z = (cells % box + half) % box
        inside = (cell_x < window) & (cell_y < window) & (cell_z < window)
        live = lax.broadcasted_iota(jnp.int32, (1, slots), 1) < cnt[src]
        row_id = jnp.where(live & inside, cell_y % radix * window + cell_x, -1)
        col_id = cell_y // radix * window + cell_z
        rows, cols = onehot.shape[1], hits.shape[1]
        picks = lax.broadcasted_iota(jnp.int32, (rows, slots), 0) == row_id
        onehot[lax.rem(src, 2), :, to] = jnp.where(picks, 1.0, 0.0).astype(BF16)
        found = lax.broadcasted_iota(jnp.int32, (cols, slots), 0) == col_id
        hits[lax.rem(src, 2), :, to] = jnp.where(found, 1.0, 0.0).astype(BF16)
        return carry

    with jax.named_scope("split_coef"):
        for c in range(2):
            coef_loads[c].wait()
            high, low = split_parts(coef[c])
            coef_parts[2 * c] = high
            coef_parts[2 * c + 1] = low
    with jax.named_scope("mark0"):
        idx_load.wait()
        cnt_load.wait()
        lax.fori_loop(0, plane // 2, mark, 0)

    with jax.named_scope("relay_rot"):
        rot_swap().wait_recv()
        peers(lambda q: rot_copy(2, 1 - side, q).start())

    def rotate(held, to_core):
        blocks = []
        for l in range(lines):
            for r in range(2):
                blocks.append(rots[held, l * 4 + to_core * 2 + r])
        a = jnp.concatenate(blocks, axis=0)
        b = jnp.concatenate(
            [piece for blk in blocks for piece in (-blk[8:], blk[:8])], axis=0
        )
        a_high, a_low = split_parts(a)
        b_high, b_low = split_parts(b)
        lhs = jnp.concatenate([a_high, a_low, a_high, b_high, b_low, b_high], axis=1)
        rhs = jnp.concatenate(
            [coef_parts[0], coef_parts[0], coef_parts[1], coef_parts[2], coef_parts[2], coef_parts[3]], axis=0
        )
        return jnp.dot(lhs, rhs, preferred_element_type=F32).reshape(lines, 2, 2, 8, slots)

    def first_part(step, held):
        with jax.named_scope(f"rotate{step}"):
            psend[step] = rotate(held, 1 - core)
            pair_copy(step).start()
            ssum[step] = rotate(held, core)

    def second_part(step):
        with jax.named_scope(f"pair{step}"):
            pair_copy(step).wait_recv()
            ssum[step] = ssum[step] + drecv[step]
            lines_other(lambda l: line_copy(step, l).start())

    def third_part(step, held):
        with jax.named_scope(f"wait_line{step}"):
            line_all(step).wait_recv()
        with jax.named_scope(f"send_val{step}"):
            total = ssum[step, line]
            for other in range(1, lines):
                total = total + zrecv[step, lax.rem(line + other, lines)]
            for r in range(2):
                for c in range(2):
                    tout[step, r * 8 : (r + 1) * 8, c, :] = total[r, c]

            def send(i, carry):
                to = i // 8 * 16 + held * 8 + lax.rem(i, 8)

                @pl.when(to != me)
                def _():
                    val_copy(step, i, to).start()

                @pl.when(to == me)
                def _():
                    land[side, cell] = tout[step, i]

                return carry

            lax.fori_loop(0, 16, send, 0)

    with jax.named_scope("wait_rot0"):
        rot_all(1).wait_recv()
    first_part(0, side)
    with jax.named_scope("relay_pot"):
        pot_swap().wait_recv()
        peers(lambda q: pot_copy(1, me, q).start())
        peers(lambda q: pot_copy(2, across, q).start())
    second_part(0)
    with jax.named_scope("wait_rot1"):
        rot_all(2).wait_recv()
    first_part(1, 1 - side)
    second_part(1)
    with jax.named_scope("mark1"):
        lax.fori_loop(plane // 2, groups, mark, 0)
    with jax.named_scope("blocks"):
        for tab in tab_loads:
            tab.wait()
        for i in range(2):
            right_blk[i] = block(right_tab[i, 0], right_tab[i, 1])
    third_part(0, side)
    third_part(1, 1 - side)
    with jax.named_scope("pair_pot"):
        pot_all(1).wait_recv()
        pot_all(2).wait_recv()
        pot_pair().start()

    early = lax.rem(me // 8, 2)
    mine_first = early == side
    acc[...] = jnp.zeros_like(acc)

    def collect(step, carry):
        batch, near = step // 4, lax.rem(step, 4)
        parity = lax.rem(early + batch, 2)
        row = lax.rem(cell // 4 + near + near // 2 - 2 * (near // 3), 4)
        alone = (parity == side) & (row == cell // 4)

        @pl.when(alone)
        def _():
            val_all(0, batch, row, 3).wait_recv()

        @pl.when(jnp.logical_not(alone))
        def _():
            val_all(0, batch, row, 4).wait_recv()

        deep = 4 * slots
        span = pl.ds(pl.multiple_of(row * deep, deep), deep)
        cols = hits.shape[1]
        for u in range(4):
            to = pl.ds(pl.multiple_of(row * deep + u * slots, slots), slots)
            high, low = split_parts(land[parity, row * 4 + u])
            mask = hits[parity, :, to]
            for n, part in enumerate((high, low)):
                part = part.astype(F32)
                for c in range(2):
                    line_of = jnp.broadcast_to(part[c : c + 1, :], (16, slots)).astype(BF16)
                    full = jnp.concatenate([line_of] * (cols // 16), axis=0)
                    at = (2 * n + c) * cols
                    placed[at : at + cols, u * slots : (u + 1) * slots] = mask * full
        acc[...] += lax.dot_general(
            onehot[parity, :, span], placed[...], (((1,), (1,)), ((), ())), preferred_element_type=F32
        )
        return carry

    with jax.named_scope("collect"):
        lax.fori_loop(0, 8, collect, 0)
    cols = hits.shape[1]
    grid_field = acc[:, : 2 * cols] + acc[:, 2 * cols :]

    def pot_ready():
        pot_pair().wait_recv()

    apply_kernel(
        box, window, radix, pot_ready, grid_field, pot_out, right_blk, left_tab, back_tab, twist,
        field, mixed, unmixed, turned, out_ref
    )
    with jax.named_scope("wait_sends"):
        rot_swap().wait_send()
        rot_all(1).wait_send()
        rot_all(2).wait_send()
        pot_swap().wait_send()
        pot_all(1).wait_send()
        pot_all(2).wait_send()
        pot_pair().wait_send()
        for step in range(2):
            pair_copy(step).wait_send()
            line_all(step).wait_send()
            alone = mine_first if step == 0 else jnp.logical_not(mine_first)

            @pl.when(alone)
            def _():
                val_all(step, 0, 0, plane - 1).wait_send()

            @pl.when(jnp.logical_not(alone))
            def _():
                val_all(step, 0, 0, plane).wait_send()


def run(coefficients, rotation, potential, index_map, counts, consts, box, window, radix):
    bands, groups = lax.axis_size("band"), lax.axis_size("ga")
    depth, _, slots = coefficients.shape
    cols = rotation.shape[2]
    assert (bands, groups, cols) == (8, 32, 8)
    lines, plane = bands // 2, groups // 2
    rot = rotation.transpose(0, 2, 1).reshape(1, 2 * cols, depth)
    hbm = pl.BlockSpec(memory_space=pl.ANY)
    vmem = pl.BlockSpec(memory_space=pltpu.VMEM)
    dma = pltpu.SemaphoreType.DMA
    rows, wide = radix * window, window // radix * window
    blocks = (2, lines, 2, 2, 8, slots)
    return pl.pallas_call(
        functools.partial(whole_kernel, box, window, radix),
        out_shape=jax.ShapeDtypeStruct((1, 2, window, window * window), F32),
        in_specs=[hbm] * 9,
        out_specs=vmem,
        scratch_shapes=[
            pltpu.VMEM((2, depth, slots), F32),
            pltpu.VMEM((4, depth, slots), BF16),
            pltpu.VMEM((2 * cols, depth), F32),
            pltpu.VMEM((2, plane, 2 * cols, depth), F32),
            pltpu.VMEM(blocks, F32),
            pltpu.VMEM(blocks, F32),
            pltpu.VMEM(blocks, F32),
            pltpu.VMEM(blocks, F32),
            pltpu.VMEM((2, 16, 2, slots), F32),
            pltpu.VMEM((2, plane, 2, slots), F32),
            pltpu.VMEM((2, rows, plane * slots), BF16),
            pltpu.VMEM((2, wide, plane * slots), BF16),
            pltpu.VMEM((4 * wide, 4 * slots), BF16),
            pltpu.VMEM((rows, 4 * wide), F32),
            pltpu.VMEM((1, groups * slots), jnp.int32),
            pltpu.SMEM((groups,), jnp.int32),
            pltpu.VMEM((groups,) + potential.shape, F32),
            *[pltpu.VMEM(table.shape, table.dtype) for table in consts],
            pltpu.VMEM((2, 2 * wide, 2 * radix * box), BF16),
            pltpu.VMEM((rows, 2 * radix * box), F32),
            pltpu.VMEM((2, radix, 2 * window, radix * box), BF16),
            pltpu.VMEM((radix, 2 * window, radix * box), F32),
            pltpu.VMEM((2, rows, 2 * radix * box), BF16),
            dma((10,)),
            dma((3,)),
            dma((3,)),
            dma((4,)),
            dma((4,)),
            dma((2,)),
            dma((2,)),
            dma((2,)),
            dma((2,)),
            dma((2,)),
            dma((2, 4)),
        ],
        compiler_params=pltpu.CompilerParams(
            collective_id=0, has_side_effects=True, vmem_limit_bytes=60 * 1024 * 1024
        ),
    )(coefficients, rot, potential, index_map[None], counts, *consts)


def apply_kernel(
    box, window, radix, pot_ready, grid_field, pot_ref, right_ref, left_ref, back_ref, twist_ref,
    field_ref, mixed_ref, unmixed_ref, turned_ref, out_ref
):
    coarse = window // radix
    rows = radix * window
    cols = coarse * window
    wide = radix * box
    lanes = 128
    per = wide // pot_ref.shape[2]

    with jax.named_scope("fwd_right"):
        right = [right_ref[i] for i in range(2)]
        field_ref[...] = dot3(split_parts(grid_field), right)

    def mix(tile, carry):
        at = pl.ds(pl.multiple_of(tile * lanes, lanes), lanes)
        imag_at = pl.ds(pl.multiple_of(wide + tile * lanes, lanes), lanes)
        values = []
        for low in range(radix):
            real = field_ref[low * window : (low + 1) * window, at]
            imag = field_ref[low * window : (low + 1) * window, imag_at]
            cos, sin = twist_ref[0, low : low + 1, at], twist_ref[1, low : low + 1, at]
            values.append((real * cos - imag * sin, real * sin + imag * cos))
        for k, pair in enumerate(fft8(values, 1)):
            for c in range(2):
                high, low = split_parts(pair[c])
                mixed_ref[0, k, c * window : (c + 1) * window, at] = high
                mixed_ref[1, k, c * window : (c + 1) * window, at] = low
        return carry

    with jax.named_scope("mix"):
        lax.fori_loop(0, wide // lanes, mix, 0)
    with jax.named_scope("wait_pot"):
        pot_ready()

    with jax.named_scope("left"):
        for k in range(radix):
            high, low = mixed_ref[0, k], mixed_ref[1, k]
            space = jnp.dot(
                left_ref[...], jnp.concatenate([high, high, low, low], axis=0), preferred_element_type=F32
            )
            pot = jnp.concatenate([pot_ref[k * per + i] for i in range(per)], axis=1)
            high, low = split_parts(space * jnp.concatenate([pot, pot], axis=0))
            both = jnp.dot(back_ref[...], jnp.concatenate([high, low], axis=0), preferred_element_type=F32)
            unmixed_ref[k] = both[: 2 * window] + both[2 * window :]

    def unmix(tile, carry):
        at = pl.ds(pl.multiple_of(tile * lanes, lanes), lanes)
        imag_at = pl.ds(pl.multiple_of(wide + tile * lanes, lanes), lanes)
        values = [
            (unmixed_ref[k, :window, at], unmixed_ref[k, window:, at]) for k in range(radix)
        ]
        for low, (real, imag) in enumerate(fft8(values, -1)):
            cos, sin = twist_ref[0, low : low + 1, at], twist_ref[1, low : low + 1, at]
            turned = (real * cos + imag * sin, imag * cos - real * sin)
            for value, to in zip(turned, (at, imag_at)):
                for i, part in enumerate(split_parts(value)):
                    turned_ref[i, low * window : (low + 1) * window, to] = part
        return carry

    with jax.named_scope("unmix"):
        lax.fori_loop(0, wide // lanes, unmix, 0)
    with jax.named_scope("back_right"):
        applied = dot3([turned_ref[0], turned_ref[1]], right, ((1,), (1,)))

    half = window // 2
    row_at = lax.broadcasted_iota(jnp.int32, (rows, cols), 0)
    col_at = lax.broadcasted_iota(jnp.int32, (rows, cols), 1)
    n_x = (row_at % window - half).astype(F32)
    n_y = (col_at // window * radix + row_at // window - half).astype(F32)
    n_z = (col_at % window - half).astype(F32)
    kinetic = (8.0 / (box * box)) * (n_x * n_x + n_y * n_y + n_z * n_z)
    applied = applied + jnp.concatenate([kinetic, kinetic], axis=1) * grid_field
    for c in range(2):
        pieces = [
            applied[lo * window : (lo + 1) * window, c * cols + hi * window : c * cols + (hi + 1) * window]
            for hi in range(coarse)
            for lo in range(radix)
        ]
        out_ref[0, c] = jnp.concatenate(pieces, axis=1)


def per_device(coefficients, rotation, potential, index_map, counts):
    box = potential.shape[0]
    window = box // 2
    radix = math.isqrt(box)
    assert radix * radix == box
    consts = [jnp.asarray(t) for t in tables(box, window, radix)]
    return run(coefficients, rotation, potential, index_map, counts, consts, box, window, radix)


def solution(mesh):
    placed = (P("band", None, "ga"), P(None, "band", "ga"), P(None, "ga"), P(), P())
    return jax.shard_map(
        per_device,
        mesh=mesh,
        in_specs=placed,
        out_specs=P(("band", "ga"), None, None, None),
        check_vma=False,
    )
```

```python
import functools
import math

import jax
import jax.numpy as jnp
import numpy as np
from jax import lax
from jax.experimental import pallas as pl
from jax.experimental.pallas import tpu as pltpu
from jax.sharding import PartitionSpec as P

F32 = jnp.float32
BF16 = jnp.bfloat16


def split_parts(values):
    high = values.astype(BF16)
    return high, (values - high.astype(F32)).astype(BF16)


def two_parts(table):
    high = table.astype(BF16)
    low = (table - high.astype(np.float32)).astype(BF16)
    return np.stack([high, low])


def tables(box, window, radix):
    half = window // 2
    coarse = window // radix
    k_all = np.arange(box)
    n_signed = np.arange(window) - half
    low = np.arange(radix)
    y_phase = (radix * np.arange(coarse) - half)[:, None] * low[None, :]
    z_phase = n_signed[:, None] * k_all[None, :]
    right = y_phase[:, None, :, None] + z_phase[None, :, None, :]
    right = right.reshape(coarse * window, radix * box) % box
    x_phase = k_all[:, None] * n_signed[None, :] % box
    twist = np.repeat(low[:, None] * low[None, :], box, axis=1) % box

    def pair(phase, scale=1.0):
        angle = phase * (2.0 * math.pi / box)
        return (np.stack([np.cos(angle), np.sin(angle)]) * scale).astype(np.float32)

    right_tab = two_parts(pair(right))
    cos, sin = pair(x_phase)
    left_high, left_low = two_parts(np.block([[cos, -sin], [sin, cos]]) / np.float32(box**3))
    left_tab = np.concatenate([left_high, left_low, left_high, left_low], axis=1)
    back_high, back_low = two_parts(np.block([[cos.T, sin.T], [-sin.T, cos.T]]))
    back_tab = np.block([[back_high, back_high], [back_low, back_low]])
    return right_tab, left_tab, back_tab, pair(twist)


def fft8(values, sign):
    root = math.sqrt(0.5)

    def add(a, b):
        return a[0] + b[0], a[1] + b[1]

    def sub(a, b):
        return a[0] - b[0], a[1] - b[1]

    def turn(a):
        return (-a[1], a[0]) if sign > 0 else (a[1], -a[0])

    def fft4(a, b, c, d):
        total, diff = add(a, c), sub(a, c)
        other, cross = add(b, d), turn(sub(b, d))
        return add(total, other), add(diff, cross), sub(total, other), sub(diff, cross)

    even = fft4(*values[0::2])
    odd = list(fft4(*values[1::2]))
    one, three = odd[1], odd[3]
    one_turn, three_turn = turn(one), turn(three)
    odd[1] = ((one[0] + one_turn[0]) * root, (one[1] + one_turn[1]) * root)
    odd[2] = turn(odd[2])
    odd[3] = ((three_turn[0] - three[0]) * root, (three_turn[1] - three[1]) * root)
    return [add(a, b) for a, b in zip(even, odd)] + [sub(a, b) for a, b in zip(even, odd)]


def dot3(lhs, rhs, dims=((1,), (0,))):
    def one(a, b):
        return lax.dot_general(a, b, (dims, ((), ())), preferred_element_type=F32)

    return one(lhs[0], rhs[0]) + (one(lhs[0], rhs[1]) + one(lhs[1], rhs[0]))


def block(cos, sin):
    upper = jnp.concatenate([cos, sin], axis=1)
    lower = jnp.concatenate([-sin, cos], axis=1)
    return jnp.concatenate([upper, lower], axis=0)


def whole_kernel(
    box, window, radix, coef_hbm, rot_hbm, pot_hbm, idx_hbm, cnt_hbm, right_hbm, left_hbm, back_hbm, twist_hbm,
    out_ref, coef, coef_parts, rot_raw, rot_own, rots, psend, drecv, ssum, zrecv, tout, land, onehot, hits, placed, acc, idx, cnt,
    pot_out, right_tab, left_tab, back_tab, twist, right_blk, field, mixed, unmixed, turned,
    load_sem, rot_send, rot_recv, pot_send, pot_recv, pair_send, pair_recv, line_send, line_recv, val_send, val_recv
):
    band = lax.axis_index("band")
    me = lax.axis_index("ga")
    groups = 2 * rots.shape[1]
    plane = groups // 2
    lines = ssum.shape[1]
    line, core = band // 2, lax.rem(band, 2)
    cell, side = me // 2, lax.rem(me, 2)
    across = cell * 2 + (1 - side)
    sibling = line * 2 + (1 - core)
    mirror = (lines - 1 - line) * 2 + core
    half_rows = pot_hbm.shape[0] // 2
    share = pl.ds(pl.multiple_of(core * half_rows, half_rows), half_rows)
    slots = coef.shape[2]

    def local(src, dst, i):
        copy = pltpu.make_async_copy(src, dst, load_sem.at[i])
        copy.start()
        return copy

    rot_load = local(rot_hbm.at[0], rot_raw, 0)
    idx_load = local(idx_hbm, idx, 1)
    cnt_load = local(cnt_hbm, cnt, 2)
    coef_loads = [local(coef_hbm.at[:, c, :], coef.at[c], 3 + c) for c in range(2)]
    pot_load = local(pot_hbm, pot_out.at[me], 5)
    tab_loads = [
        local(src, dst, 6 + i)
        for i, (src, dst) in enumerate(
            ((right_hbm, right_tab), (left_hbm, left_tab), (back_hbm, back_tab), (twist_hbm, twist))
        )
    ]

    barrier = pltpu.get_barrier_semaphore()

    def greet(to_band, to):
        pl.semaphore_signal(
            barrier, inc=1, device_id={"band": to_band, "ga": to}, device_id_type=pl.DeviceIdType.MESH
        )

    def peers(act):
        def body(step, code):
            shift = lax.rem(code, 16)
            act(lax.rem(cell // 4 + shift // 4, 4) * 4 + lax.rem(cell + shift, 4))
            return code // 16

        lax.fori_loop(0, 8, body, jnp.int32(0x528E6B9A))
        lax.fori_loop(0, 7, body, jnp.int32(0xC431FD7))

    def lines_other(act):
        low = 1 - line // 2
        for step in range(lines):
            l = low * (lines - 1 - step) + (1 - low) * step

            @pl.when(l != line)
            def _(l=l):
                act(l)

    def remote(src, dst, send, recv, to_band, to):
        return pltpu.make_async_remote_copy(
            src_ref=src, dst_ref=dst, send_sem=send, recv_sem=recv,
            device_id={"band": to_band, "ga": to}, device_id_type=pl.DeviceIdType.MESH,
        )

    def split_coef():
        for c in range(2):
            coef_loads[c].wait()
            high, low = split_parts(coef[c])
            coef_parts[2 * c] = high
            coef_parts[2 * c + 1] = low
        rot_load.wait()
        for e in range(2):
            for c in range(2):
                for x in range(4):
                    rot_own[e, 4 * c + x] = rot_raw[8 * c + 2 * x + e]

    with jax.named_scope("barrier"):
        peers(lambda q: greet(band, q * 2 + side))
        greet(band, across)
        greet(mirror, across)
        greet(sibling, me)
        lines_other(lambda l: greet(l * 2 + core, me))
        split_coef()
        pl.semaphore_wait(barrier, plane - 1 + 3 + lines - 1)

    def rot_swap():
        return remote(rot_own, rots.at[side, cell], rot_send.at[0], rot_recv.at[0], band, across)

    def rot_copy(which, held, q):
        slot = rots.at[held, cell]
        src = rot_own if which == 1 else slot
        return remote(src, slot, rot_send.at[which], rot_recv.at[which], band, q * 2 + side)

    def rot_all(which):
        part = rots.at[0, pl.ds(0, plane - 1)]
        return remote(part, part, rot_send.at[which], rot_recv.at[which], band, across)

    def pot_swap():
        part = pot_out.at[me, share]
        return remote(part, part, pot_send.at[0], pot_recv.at[0], mirror, across)

    def pot_copy(which, piece, q):
        part = pot_out.at[piece, share]
        return remote(part, part, pot_send.at[which], pot_recv.at[which], band, q * 2 + side)

    def pot_all(which):
        part = pot_out.at[pl.ds(0, plane - 1), pl.ds(0, half_rows)]
        return remote(part, part, pot_send.at[which], pot_recv.at[which], band, across)

    def pot_pair():
        part = pot_out.at[:, share]
        return remote(part, part, pot_send.at[3], pot_recv.at[3], sibling, me)

    def pair_copy(step):
        return remote(psend.at[step], drecv.at[step], pair_send.at[step], pair_recv.at[step], sibling, me)

    def line_copy(step, l):
        return remote(
            ssum.at[step, l], zrecv.at[step, line], line_send.at[step], line_recv.at[step], l * 2 + core, me
        )

    def line_all(step):
        part = zrecv.at[step, pl.ds(0, lines - 1)]
        return remote(part, part, line_send.at[step], line_recv.at[step], sibling, me)

    def val_copy(step, i, to_band, to):
        return remote(
            tout.at[step, i], land.at[side, cell], val_send.at[step], val_recv.at[step, cell // 4], to_band, to
        )

    def val_all(step, batch, row, count):
        part = land.at[0, pl.ds(0, count)]
        return remote(part, part, val_send.at[step], val_recv.at[batch, row], band, across)

    with jax.named_scope("send_rot"):
        rot_swap().start()
        peers(lambda q: rot_copy(1, side, q).start())
        rots[side, cell] = rot_own[...]
        pot_load.wait()
        pot_swap().start()

    def mark(src, carry):
        at = pl.ds(pl.multiple_of(src * slots, slots), slots)
        to = pl.ds(pl.multiple_of(src // 2 * slots, slots), slots)
        half = window // 2
        cells = idx[:, at]
        cell_x = (cells // (box * box) + half) % box
        cell_y = (cells // box % box + half) % box
        cell_z = (cells % box + half) % box
        inside = (cell_x < window) & (cell_y < window) & (cell_z < window)
        live = lax.broadcasted_iota(jnp.int32, (1, slots), 1) < cnt[src]
        row_id = jnp.where(live & inside, cell_y % radix * window + cell_x, -1)
        col_id = cell_y // radix * window + cell_z
        rows, cols = onehot.shape[1], hits.shape[1]
        picks = lax.broadcasted_iota(jnp.int32, (rows, slots), 0) == row_id
        onehot[lax.rem(src, 2), :, to] = jnp.where(picks, 1.0, 0.0).astype(BF16)
        found = lax.broadcasted_iota(jnp.int32, (cols, slots), 0) == col_id
        hits[lax.rem(src, 2), :, to] = jnp.where(found, 1.0, 0.0).astype(BF16)
        return carry

    with jax.named_scope("mark0"):
        idx_load.wait()
        cnt_load.wait()
        lax.fori_loop(0, 4, mark, 0)

    with jax.named_scope("relay_rot"):
        rot_swap().wait_recv()
        peers(lambda q: rot_copy(2, 1 - side, q).start())
        lax.fori_loop(4, 8, mark, 0)

    def rotate(held, to_core):
        blocks = []
        for l in range(lines):
            for l_of, e in ((l, side), (lines - 1 - l, 1 - side)):
                for r in range(2):
                    blocks.append(rots[held, l_of * 4 + to_core * 2 + r, e])
        a = jnp.concatenate(blocks, axis=0)
        b = jnp.concatenate([piece for blk in blocks for piece in (-blk[4:], blk[:4])], axis=0)
        a_high, a_low = split_parts(a)
        b_high, b_low = split_parts(b)
        lhs = jnp.concatenate([a_high, a_low, a_high, b_high, b_low, b_high], axis=1)
        rhs = jnp.concatenate(
            [coef_parts[0], coef_parts[0], coef_parts[1], coef_parts[2], coef_parts[2], coef_parts[3]], axis=0
        )
        return jnp.dot(lhs, rhs, preferred_element_type=F32).reshape(lines, 2, 2, 8, slots)

    def first_part(step, held):
        with jax.named_scope(f"rotate{step}"):
            psend[step] = rotate(held, 1 - core)
            pair_copy(step).start()
            ssum[step] = rotate(held, core)

    def second_part(step):
        with jax.named_scope(f"pair{step}"):
            pair_copy(step).wait_recv()
            ssum[step] = ssum[step] + drecv[step]
            lines_other(lambda l: line_copy(step, l).start())

    def third_part(step, held):
        with jax.named_scope(f"wait_line{step}"):
            line_all(step).wait_recv()
        with jax.named_scope(f"send_val{step}"):
            total = ssum[step, line]
            for other in range(1, lines):
                total = total + zrecv[step, lax.rem(line + other, lines)]
            for e in range(2):
                for r in range(2):
                    for c in range(2):
                        at = e * 8 + r * 4
                        tout[step, at : at + 4, c, :] = total[e, r, c * 4 : c * 4 + 4]

            def send(n, carry):
                e = 1 - n // 8
                r = lax.rem(cell // 8 + 1 + n // 4, 2)
                m = lax.rem(n, 4)
                x = lax.rem(cell + jnp.where(m == 0, 2, jnp.where(m == 1, 1, jnp.where(m == 2, 3, 0))), 4)
                to = (r * 8 + held * 4 + x) * 2 + lax.rem(side + e, 2)
                i = e * 8 + r * 4 + x

                @pl.when(to != me)
                def _():
                    val_copy(step, i, (1 - e) * band + e * mirror, to).start()

                @pl.when(to == me)
                def _():
                    land[side, cell] = tout[step, i]

                return carry

            lax.fori_loop(0, 16, send, 0)

    with jax.named_scope("wait_rot0"):
        rot_all(1).wait_recv()
    first_part(0, side)
    with jax.named_scope("relay_pot"):
        pot_swap().wait_recv()
        peers(lambda q: pot_copy(1, me, q).start())
        peers(lambda q: pot_copy(2, across, q).start())
    second_part(0)
    with jax.named_scope("wait_rot1"):
        rot_all(2).wait_recv()
    first_part(1, 1 - side)
    second_part(1)
    with jax.named_scope("mark1"):
        lax.fori_loop(8, 16, mark, 0)
        for tab in tab_loads:
            tab.wait()
        for i in range(2):
            right_blk[i] = block(right_tab[i, 0], right_tab[i, 1])
    with jax.named_scope("pair_pot"):
        pot_all(1).wait_recv()
        pot_all(2).wait_recv()
        pot_pair().start()
    third_part(0, side)
    with jax.named_scope("mark2"):
        lax.fori_loop(16, groups, mark, 0)
    third_part(1, 1 - side)

    early = lax.rem(me // 8, 2)
    mine_first = early == side
    acc[...] = jnp.zeros_like(acc)

    def collect(step, carry):
        batch, near = step // 4, lax.rem(step, 4)
        parity = lax.rem(early + batch, 2)
        row = lax.rem(cell // 4 + near + near // 2 - 2 * (near // 3), 4)
        alone = (parity == side) & (row == cell // 4)

        @pl.when(alone)
        def _():
            val_all(0, batch, row, 3).wait_recv()

        @pl.when(jnp.logical_not(alone))
        def _():
            val_all(0, batch, row, 4).wait_recv()

        deep = 4 * slots
        span = pl.ds(pl.multiple_of(row * deep, deep), deep)
        cols = hits.shape[1]
        for u in range(4):
            to = pl.ds(pl.multiple_of(row * deep + u * slots, slots), slots)
            high, low = split_parts(land[parity, row * 4 + u])
            mask = hits[parity, :, to]
            for n, part in enumerate((high, low)):
                part = part.astype(F32)
                for c in range(2):
                    line_of = jnp.broadcast_to(part[c : c + 1, :], (16, slots)).astype(BF16)
                    full = jnp.concatenate([line_of] * (cols // 16), axis=0)
                    at = (2 * n + c) * cols
                    placed[at : at + cols, u * slots : (u + 1) * slots] = mask * full
        acc[...] += lax.dot_general(
            onehot[parity, :, span], placed[...], (((1,), (1,)), ((), ())), preferred_element_type=F32
        )
        return carry

    with jax.named_scope("collect"):
        lax.fori_loop(0, 8, collect, 0)
    cols = hits.shape[1]
    grid_field = acc[:, : 2 * cols] + acc[:, 2 * cols :]

    def pot_ready():
        pot_pair().wait_recv()

    apply_kernel(
        box, window, radix, pot_ready, grid_field, pot_out, right_blk, left_tab, back_tab, twist,
        field, mixed, unmixed, turned, out_ref
    )
    with jax.named_scope("wait_sends"):
        rot_swap().wait_send()
        rot_all(1).wait_send()
        rot_all(2).wait_send()
        pot_swap().wait_send()
        pot_all(1).wait_send()
        pot_all(2).wait_send()
        pot_pair().wait_send()
        for step in range(2):
            pair_copy(step).wait_send()
            line_all(step).wait_send()
            alone = mine_first if step == 0 else jnp.logical_not(mine_first)

            @pl.when(alone)
            def _():
                val_all(step, 0, 0, plane - 1).wait_send()

            @pl.when(jnp.logical_not(alone))
            def _():
                val_all(step, 0, 0, plane).wait_send()


def run(coefficients, rotation, potential, index_map, counts, consts, box, window, radix):
    bands, groups = lax.axis_size("band"), lax.axis_size("ga")
    depth, _, slots = coefficients.shape
    cols = rotation.shape[2]
    assert (bands, groups, cols) == (8, 32, 8)
    lines, plane = bands // 2, groups // 2
    rot = rotation.transpose(0, 2, 1).reshape(1, 2 * cols, depth)
    hbm = pl.BlockSpec(memory_space=pl.ANY)
    vmem = pl.BlockSpec(memory_space=pltpu.VMEM)
    dma = pltpu.SemaphoreType.DMA
    rows, wide = radix * window, window // radix * window
    blocks = (2, lines, 2, 2, 8, slots)
    return pl.pallas_call(
        functools.partial(whole_kernel, box, window, radix),
        out_shape=jax.ShapeDtypeStruct((1, 2, window, window * window), F32),
        in_specs=[hbm] * 9,
        out_specs=vmem,
        scratch_shapes=[
            pltpu.VMEM((2, depth, slots), F32),
            pltpu.VMEM((4, depth, slots), BF16),
            pltpu.VMEM((2 * cols, depth), F32),
            pltpu.VMEM((2, cols, depth), F32),
            pltpu.VMEM((2, plane, 2, cols, depth), F32),
            pltpu.VMEM(blocks, F32),
            pltpu.VMEM(blocks, F32),
            pltpu.VMEM(blocks, F32),
            pltpu.VMEM(blocks, F32),
            pltpu.VMEM((2, 16, 2, slots), F32),
            pltpu.VMEM((2, plane, 2, slots), F32),
            pltpu.VMEM((2, rows, plane * slots), BF16),
            pltpu.VMEM((2, wide, plane * slots), BF16),
            pltpu.VMEM((4 * wide, 4 * slots), BF16),
            pltpu.VMEM((rows, 4 * wide), F32),
            pltpu.VMEM((1, groups * slots), jnp.int32),
            pltpu.SMEM((groups,), jnp.int32),
            pltpu.VMEM((groups,) + potential.shape, F32),
            *[pltpu.VMEM(table.shape, table.dtype) for table in consts],
            pltpu.VMEM((2, 2 * wide, 2 * radix * box), BF16),
            pltpu.VMEM((rows, 2 * radix * box), F32),
            pltpu.VMEM((2, radix, 2 * window, radix * box), BF16),
            pltpu.VMEM((radix, 2 * window, radix * box), F32),
            pltpu.VMEM((2, rows, 2 * radix * box), BF16),
            dma((10,)),
            dma((3,)),
            dma((3,)),
            dma((4,)),
            dma((4,)),
            dma((2,)),
            dma((2,)),
            dma((2,)),
            dma((2,)),
            dma((2,)),
            dma((2, 4)),
        ],
        compiler_params=pltpu.CompilerParams(
            collective_id=0, has_side_effects=True, vmem_limit_bytes=60 * 1024 * 1024
        ),
    )(coefficients, rot, potential, index_map[None], counts, *consts)


def apply_kernel(
    box, window, radix, pot_ready, grid_field, pot_ref, right_ref, left_ref, back_ref, twist_ref,
    field_ref, mixed_ref, unmixed_ref, turned_ref, out_ref
):
    coarse = window // radix
    rows = radix * window
    cols = coarse * window
    wide = radix * box
    lanes = 128
    per = wide // pot_ref.shape[2]

    with jax.named_scope("fwd_right"):
        right = [right_ref[i] for i in range(2)]
        field_ref[...] = dot3(split_parts(grid_field), right)

    def mix(tile, carry):
        at = pl.ds(pl.multiple_of(tile * lanes, lanes), lanes)
        imag_at = pl.ds(pl.multiple_of(wide + tile * lanes, lanes), lanes)
        values = []
        for low in range(radix):
            real = field_ref[low * window : (low + 1) * window, at]
            imag = field_ref[low * window : (low + 1) * window, imag_at]
            cos, sin = twist_ref[0, low : low + 1, at], twist_ref[1, low : low + 1, at]
            values.append((real * cos - imag * sin, real * sin + imag * cos))
        for k, pair in enumerate(fft8(values, 1)):
            for c in range(2):
                high, low = split_parts(pair[c])
                mixed_ref[0, k, c * window : (c + 1) * window, at] = high
                mixed_ref[1, k, c * window : (c + 1) * window, at] = low
        return carry

    with jax.named_scope("mix"):
        lax.fori_loop(0, wide // lanes, mix, 0)
    with jax.named_scope("wait_pot"):
        pot_ready()

    with jax.named_scope("left"):
        for k in range(radix):
            high, low = mixed_ref[0, k], mixed_ref[1, k]
            space = jnp.dot(
                left_ref[...], jnp.concatenate([high, high, low, low], axis=0), preferred_element_type=F32
            )
            pot = jnp.concatenate([pot_ref[k * per + i] for i in range(per)], axis=1)
            high, low = split_parts(space * jnp.concatenate([pot, pot], axis=0))
            both = jnp.dot(back_ref[...], jnp.concatenate([high, low], axis=0), preferred_element_type=F32)
            unmixed_ref[k] = both[: 2 * window] + both[2 * window :]

    def unmix(tile, carry):
        at = pl.ds(pl.multiple_of(tile * lanes, lanes), lanes)
        imag_at = pl.ds(pl.multiple_of(wide + tile * lanes, lanes), lanes)
        values = [
            (unmixed_ref[k, :window, at], unmixed_ref[k, window:, at]) for k in range(radix)
        ]
        for low, (real, imag) in enumerate(fft8(values, -1)):
            cos, sin = twist_ref[0, low : low + 1, at], twist_ref[1, low : low + 1, at]
            turned = (real * cos + imag * sin, imag * cos - real * sin)
            for value, to in zip(turned, (at, imag_at)):
                for i, part in enumerate(split_parts(value)):
                    turned_ref[i, low * window : (low + 1) * window, to] = part
        return carry

    with jax.named_scope("unmix"):
        lax.fori_loop(0, wide // lanes, unmix, 0)
    with jax.named_scope("back_right"):
        applied = dot3([turned_ref[0], turned_ref[1]], right, ((1,), (1,)))

    half = window // 2
    row_at = lax.broadcasted_iota(jnp.int32, (rows, cols), 0)
    col_at = lax.broadcasted_iota(jnp.int32, (rows, cols), 1)
    n_x = (row_at % window - half).astype(F32)
    n_y = (col_at // window * radix + row_at // window - half).astype(F32)
    n_z = (col_at % window - half).astype(F32)
    kinetic = (8.0 / (box * box)) * (n_x * n_x + n_y * n_y + n_z * n_z)
    applied = applied + jnp.concatenate([kinetic, kinetic], axis=1) * grid_field
    for c in range(2):
        pieces = [
            applied[lo * window : (lo + 1) * window, c * cols + hi * window : c * cols + (hi + 1) * window]
            for hi in range(coarse)
            for lo in range(radix)
        ]
        out_ref[0, c] = jnp.concatenate(pieces, axis=1)


def per_device(coefficients, rotation, potential, index_map, counts):
    box = potential.shape[0]
    window = box // 2
    radix = math.isqrt(box)
    assert radix * radix == box
    consts = [jnp.asarray(t) for t in tables(box, window, radix)]
    return run(coefficients, rotation, potential, index_map, counts, consts, box, window, radix)


def solution(mesh):
    placed = (P("band", None, "ga"), P(None, "band", "ga"), P(None, "ga"), P(), P())
    return jax.shard_map(
        per_device,
        mesh=mesh,
        in_specs=placed,
        out_specs=P(("band", "ga"), None, None, None),
        check_vma=False,
    )
```

```python
import functools
import math

import jax
import jax.numpy as jnp
import numpy as np
from jax import lax
from jax.experimental import pallas as pl
from jax.experimental.pallas import tpu as pltpu
from jax.sharding import PartitionSpec as P

F32 = jnp.float32
BF16 = jnp.bfloat16


def split_parts(values):
    high = values.astype(BF16)
    return high, (values - high.astype(F32)).astype(BF16)


def two_parts(table):
    high = table.astype(BF16)
    low = (table - high.astype(np.float32)).astype(BF16)
    return np.stack([high, low])


def tables(box, window, radix):
    half = window // 2
    coarse = window // radix
    k_all = np.arange(box)
    n_signed = np.arange(window) - half
    low = np.arange(radix)
    y_phase = (radix * np.arange(coarse) - half)[:, None] * low[None, :]
    z_phase = n_signed[:, None] * k_all[None, :]
    right = y_phase[:, None, :, None] + z_phase[None, :, None, :]
    right = right.reshape(coarse * window, radix * box) % box
    x_phase = k_all[:, None] * n_signed[None, :] % box
    twist = np.repeat(low[:, None] * low[None, :], box, axis=1) % box

    def pair(phase, scale=1.0):
        angle = phase * (2.0 * math.pi / box)
        return (np.stack([np.cos(angle), np.sin(angle)]) * scale).astype(np.float32)

    right_tab = two_parts(pair(right))
    cos, sin = pair(x_phase)
    left_high, left_low = two_parts(np.block([[cos, -sin], [sin, cos]]) / np.float32(box**3))
    left_tab = np.concatenate([left_high, left_low, left_high, left_low], axis=1)
    back_high, back_low = two_parts(np.block([[cos.T, sin.T], [-sin.T, cos.T]]))
    back_tab = np.block([[back_high, back_high], [back_low, back_low]])
    return right_tab, left_tab, back_tab, pair(twist)


def fft8(values, sign):
    root = math.sqrt(0.5)

    def add(a, b):
        return a[0] + b[0], a[1] + b[1]

    def sub(a, b):
        return a[0] - b[0], a[1] - b[1]

    def turn(a):
        return (-a[1], a[0]) if sign > 0 else (a[1], -a[0])

    def fft4(a, b, c, d):
        total, diff = add(a, c), sub(a, c)
        other, cross = add(b, d), turn(sub(b, d))
        return add(total, other), add(diff, cross), sub(total, other), sub(diff, cross)

    even = fft4(*values[0::2])
    odd = list(fft4(*values[1::2]))
    one, three = odd[1], odd[3]
    one_turn, three_turn = turn(one), turn(three)
    odd[1] = ((one[0] + one_turn[0]) * root, (one[1] + one_turn[1]) * root)
    odd[2] = turn(odd[2])
    odd[3] = ((three_turn[0] - three[0]) * root, (three_turn[1] - three[1]) * root)
    return [add(a, b) for a, b in zip(even, odd)] + [sub(a, b) for a, b in zip(even, odd)]


def dot3(lhs, rhs, dims=((1,), (0,))):
    def one(a, b):
        return lax.dot_general(a, b, (dims, ((), ())), preferred_element_type=F32)

    return one(lhs[0], rhs[0]) + (one(lhs[0], rhs[1]) + one(lhs[1], rhs[0]))


def block(cos, sin):
    upper = jnp.concatenate([cos, sin], axis=1)
    lower = jnp.concatenate([-sin, cos], axis=1)
    return jnp.concatenate([upper, lower], axis=0)


def whole_kernel(
    box, window, radix, coef_hbm, rot_hbm, pot_hbm, idx_hbm, cnt_hbm, right_hbm, left_hbm, back_hbm, twist_hbm,
    out_ref, coef, coef_parts, rot_raw, rot_own, rots, prod, drecv, zrecv, tout, land, onehot, hits, placed, acc, idx, cnt,
    pot_out, right_tab, left_tab, back_tab, twist, right_blk, field, mixed, unmixed, turned,
    load_sem, rot_send, rot_recv, pot_send, pot_recv, pair_send, pair_recv, line_send, line_recv, val_send, val_recv
):
    band = lax.axis_index("band")
    me = lax.axis_index("ga")
    groups = 2 * rots.shape[1]
    plane = groups // 2
    lines = zrecv.shape[1]
    line, core = band // 2, lax.rem(band, 2)
    cell, side = me // 2, lax.rem(me, 2)
    across = cell * 2 + (1 - side)
    sibling = line * 2 + (1 - core)
    mirror = (lines - 1 - line) * 2 + core
    half_rows = pot_hbm.shape[0] // 2
    share = pl.ds(pl.multiple_of(core * half_rows, half_rows), half_rows)
    slots = coef.shape[2]

    def local(src, dst, i):
        copy = pltpu.make_async_copy(src, dst, load_sem.at[i])
        copy.start()
        return copy

    rot_load = local(rot_hbm.at[0], rot_raw, 0)
    idx_load = local(idx_hbm, idx, 1)
    cnt_load = local(cnt_hbm, cnt, 2)
    coef_loads = [local(coef_hbm.at[:, c, :], coef.at[c], 3 + c) for c in range(2)]
    pot_load = local(pot_hbm, pot_out.at[me], 5)
    tab_loads = [
        local(src, dst, 6 + i)
        for i, (src, dst) in enumerate(
            ((right_hbm, right_tab), (left_hbm, left_tab), (back_hbm, back_tab), (twist_hbm, twist))
        )
    ]

    barrier = pltpu.get_barrier_semaphore()

    def greet(to_band, to):
        pl.semaphore_signal(
            barrier, inc=1, device_id={"band": to_band, "ga": to}, device_id_type=pl.DeviceIdType.MESH
        )

    def peers(act):
        def body(step, code):
            shift = lax.rem(code, 16)
            act(lax.rem(cell // 4 + shift // 4, 4) * 4 + lax.rem(cell + shift, 4))
            return code // 16

        lax.fori_loop(0, 8, body, jnp.int32(0x528E6B9A))
        lax.fori_loop(0, 7, body, jnp.int32(0xC431FD7))

    def lines_other(act):
        low = 1 - line // 2
        for step in range(lines):
            l = low * (lines - 1 - step) + (1 - low) * step

            @pl.when(l != line)
            def _(l=l):
                act(l)

    def remote(src, dst, send, recv, to_band, to):
        return pltpu.make_async_remote_copy(
            src_ref=src, dst_ref=dst, send_sem=send, recv_sem=recv,
            device_id={"band": to_band, "ga": to}, device_id_type=pl.DeviceIdType.MESH,
        )

    def split_coef():
        for c in range(2):
            coef_loads[c].wait()
            high, low = split_parts(coef[c])
            coef_parts[2 * c] = high
            coef_parts[2 * c + 1] = low
        rot_load.wait()
        for e in range(2):
            for c in range(2):
                for x in range(4):
                    rot_own[e, 4 * c + x] = rot_raw[8 * c + 2 * x + e]

    with jax.named_scope("barrier"):
        peers(lambda q: greet(band, q * 2 + side))
        greet(band, across)
        greet(mirror, across)
        greet(sibling, me)
        lines_other(lambda l: greet(l * 2 + core, me))
        split_coef()
        pl.semaphore_wait(barrier, plane - 1 + 3 + lines - 1)

    def rot_swap():
        return remote(rot_own, rots.at[side, cell], rot_send.at[0], rot_recv.at[0], band, across)

    def rot_copy(which, held, q):
        slot = rots.at[held, cell]
        src = rot_own if which == 1 else slot
        return remote(src, slot, rot_send.at[which], rot_recv.at[which], band, q * 2 + side)

    def rot_all(which):
        part = rots.at[0, pl.ds(0, plane - 1)]
        return remote(part, part, rot_send.at[which], rot_recv.at[which], band, across)

    def pot_swap():
        part = pot_out.at[me, share]
        return remote(part, part, pot_send.at[0], pot_recv.at[0], mirror, across)

    def pot_copy(which, piece, q):
        part = pot_out.at[piece, share]
        return remote(part, part, pot_send.at[which], pot_recv.at[which], band, q * 2 + side)

    def pot_all(which):
        part = pot_out.at[pl.ds(0, plane - 1), pl.ds(0, half_rows)]
        return remote(part, part, pot_send.at[which], pot_recv.at[which], band, across)

    def pot_pair():
        part = pot_out.at[:, share]
        return remote(part, part, pot_send.at[3], pot_recv.at[3], sibling, me)

    def pair_copy(step):
        return remote(prod.at[step, 0], drecv.at[step], pair_send.at[step], pair_recv.at[step], sibling, me)

    def line_copy(step, l):
        return remote(
            prod.at[step, 1, l], zrecv.at[step, line], line_send.at[step], line_recv.at[step], l * 2 + core, me
        )

    def line_all(step):
        part = zrecv.at[step, pl.ds(0, lines - 1)]
        return remote(part, part, line_send.at[step], line_recv.at[step], sibling, me)

    def val_copy(step, i, to_band, to):
        return remote(
            tout.at[step, i], land.at[side, cell], val_send.at[step], val_recv.at[step, cell // 4], to_band, to
        )

    def val_all(step, batch, row, count):
        part = land.at[0, pl.ds(0, count)]
        return remote(part, part, val_send.at[step], val_recv.at[batch, row], band, across)

    with jax.named_scope("send_rot"):
        rot_swap().start()
        pot_load.wait()
        pot_swap().start()
        peers(lambda q: rot_copy(1, side, q).start())
        rots[side, cell] = rot_own[...]

    def mark(src, carry):
        at = pl.ds(pl.multiple_of(src * slots, slots), slots)
        to = pl.ds(pl.multiple_of(src // 2 * slots, slots), slots)
        half = window // 2
        cells = idx[:, at]
        cell_x = (cells // (box * box) + half) % box
        cell_y = (cells // box % box + half) % box
        cell_z = (cells % box + half) % box
        inside = (cell_x < window) & (cell_y < window) & (cell_z < window)
        live = lax.broadcasted_iota(jnp.int32, (1, slots), 1) < cnt[src]
        row_id = jnp.where(live & inside, cell_y % radix * window + cell_x, -1)
        col_id = cell_y // radix * window + cell_z
        rows, cols = onehot.shape[1], hits.shape[1]
        picks = lax.broadcasted_iota(jnp.int32, (rows, slots), 0) == row_id
        onehot[lax.rem(src, 2), :, to] = jnp.where(picks, 1.0, 0.0).astype(BF16)
        found = lax.broadcasted_iota(jnp.int32, (cols, slots), 0) == col_id
        hits[lax.rem(src, 2), :, to] = jnp.where(found, 1.0, 0.0).astype(BF16)
        return carry

    with jax.named_scope("mark0"):
        idx_load.wait()
        cnt_load.wait()
        lax.fori_loop(0, 4, mark, 0)

    with jax.named_scope("relay_rot"):
        rot_swap().wait_recv()
        pot_swap().wait_recv()
        peers(lambda q: rot_copy(2, 1 - side, q).start())
        lax.fori_loop(4, 8, mark, 0)

    def rotate(held, to_core):
        blocks = []
        for l in range(lines):
            for l_of, e in ((l, side), (lines - 1 - l, 1 - side)):
                for r in range(2):
                    blocks.append(rots[held, l_of * 4 + to_core * 2 + r, e])
        a = jnp.concatenate(blocks, axis=0)
        b = jnp.concatenate([piece for blk in blocks for piece in (-blk[4:], blk[:4])], axis=0)
        a_high, a_low = split_parts(a)
        b_high, b_low = split_parts(b)
        lhs = jnp.concatenate([a_high, a_low, a_high, b_high, b_low, b_high], axis=1)
        rhs = jnp.concatenate(
            [coef_parts[0], coef_parts[0], coef_parts[1], coef_parts[2], coef_parts[2], coef_parts[3]], axis=0
        )
        return jnp.dot(lhs, rhs, preferred_element_type=F32).reshape(lines, 2, 2, 8, slots)

    def first_half(step, carry):
        with jax.named_scope("wait_rot"):
            rot_all(1 + step).wait_recv()

        def part(i, carry):
            with jax.named_scope("rotate"):
                prod[step, i] = rotate(lax.rem(side + step, 2), lax.rem(core + 1 + i, 2))

            @pl.when(i == 0)
            def _():
                pair_copy(step).start()

            return carry

        lax.fori_loop(0, 2, part, 0)

        @pl.when(step == 1)
        def _():
            with jax.named_scope("relay_pot"):
                peers(lambda q: pot_copy(1, me, q).start())
                peers(lambda q: pot_copy(2, across, q).start())

        with jax.named_scope("pair"):
            pair_copy(step).wait_recv()
            prod[step, 1] = prod[step, 1] + drecv[step]
            lines_other(lambda l: line_copy(step, l).start())
        return carry

    lax.fori_loop(0, 2, first_half, 0)
    with jax.named_scope("blocks"):
        for tab in tab_loads:
            tab.wait()
        for i in range(2):
            right_blk[i] = block(right_tab[i, 0], right_tab[i, 1])

    def second_half(step, carry):
        with jax.named_scope("mark1"):
            lax.fori_loop(8 + 12 * step, 20 + 12 * step, mark, 0)
        with jax.named_scope("wait_line"):
            line_all(step).wait_recv()
        with jax.named_scope("send_val"):
            total = prod[step, 1, line]
            for other in range(1, lines):
                total = total + zrecv[step, lax.rem(line + other, lines)]
            for e in range(2):
                for r in range(2):
                    for c in range(2):
                        at = e * 8 + r * 4
                        tout[step, at : at + 4, c, :] = total[e, r, c * 4 : c * 4 + 4]

            def send(n, carry):
                e = 1 - n // 8
                r = lax.rem(cell // 8 + 1 + n // 4, 2)
                m = lax.rem(n, 4)
                x = lax.rem(cell + jnp.where(m == 0, 2, jnp.where(m == 1, 1, jnp.where(m == 2, 3, 0))), 4)
                to = (r * 8 + lax.rem(side + step, 2) * 4 + x) * 2 + lax.rem(side + e, 2)
                i = e * 8 + r * 4 + x

                @pl.when(to != me)
                def _():
                    val_copy(step, i, (1 - e) * band + e * mirror, to).start()

                @pl.when(to == me)
                def _():
                    land[side, cell] = tout[step, i]

                return carry

            lax.fori_loop(0, 16, send, 0)
        return carry

    lax.fori_loop(0, 2, second_half, 0)
    with jax.named_scope("pair_pot"):
        pot_all(1).wait_recv()
        pot_all(2).wait_recv()
        pot_pair().start()

    early = lax.rem(me // 8, 2)
    mine_first = early == side
    acc[...] = jnp.zeros_like(acc)

    def collect(step, carry):
        batch, near = step // 4, lax.rem(step, 4)
        parity = lax.rem(early + batch, 2)
        row = lax.rem(cell // 4 + near + near // 2 - 2 * (near // 3), 4)
        alone = (parity == side) & (row == cell // 4)

        @pl.when(alone)
        def _():
            val_all(0, batch, row, 3).wait_recv()

        @pl.when(jnp.logical_not(alone))
        def _():
            val_all(0, batch, row, 4).wait_recv()

        deep = 4 * slots
        span = pl.ds(pl.multiple_of(row * deep, deep), deep)
        cols = hits.shape[1]
        for u in range(4):
            to = pl.ds(pl.multiple_of(row * deep + u * slots, slots), slots)
            high, low = split_parts(land[parity, row * 4 + u])
            mask = hits[parity, :, to]
            for n, part in enumerate((high, low)):
                part = part.astype(F32)
                for c in range(2):
                    line_of = jnp.broadcast_to(part[c : c + 1, :], (16, slots)).astype(BF16)
                    full = jnp.concatenate([line_of] * (cols // 16), axis=0)
                    at = (2 * n + c) * cols
                    placed[at : at + cols, u * slots : (u + 1) * slots] = mask * full
        acc[...] += lax.dot_general(
            onehot[parity, :, span], placed[...], (((1,), (1,)), ((), ())), preferred_element_type=F32
        )
        return carry

    with jax.named_scope("collect"):
        lax.fori_loop(0, 8, collect, 0)
    cols = hits.shape[1]
    grid_field = acc[:, : 2 * cols] + acc[:, 2 * cols :]

    def pot_ready():
        pot_pair().wait_recv()

    apply_kernel(
        box, window, radix, pot_ready, grid_field, pot_out, right_blk, left_tab, back_tab, twist,
        field, mixed, unmixed, turned, out_ref
    )
    with jax.named_scope("wait_sends"):
        rot_swap().wait_send()
        rot_all(1).wait_send()
        rot_all(2).wait_send()
        pot_swap().wait_send()
        pot_all(1).wait_send()
        pot_all(2).wait_send()
        pot_pair().wait_send()
        for step in range(2):
            pair_copy(step).wait_send()
            line_all(step).wait_send()
            alone = mine_first if step == 0 else jnp.logical_not(mine_first)

            @pl.when(alone)
            def _():
                val_all(step, 0, 0, plane - 1).wait_send()

            @pl.when(jnp.logical_not(alone))
            def _():
                val_all(step, 0, 0, plane).wait_send()


def run(coefficients, rotation, potential, index_map, counts, consts, box, window, radix):
    bands, groups = lax.axis_size("band"), lax.axis_size("ga")
    depth, _, slots = coefficients.shape
    cols = rotation.shape[2]
    assert (bands, groups, cols) == (8, 32, 8)
    lines, plane = bands // 2, groups // 2
    rot = rotation.transpose(0, 2, 1).reshape(1, 2 * cols, depth)
    hbm = pl.BlockSpec(memory_space=pl.ANY)
    vmem = pl.BlockSpec(memory_space=pltpu.VMEM)
    dma = pltpu.SemaphoreType.DMA
    rows, wide = radix * window, window // radix * window
    blocks = (2, lines, 2, 2, 8, slots)
    return pl.pallas_call(
        functools.partial(whole_kernel, box, window, radix),
        out_shape=jax.ShapeDtypeStruct((1, 2, window, window * window), F32),
        in_specs=[hbm] * 9,
        out_specs=vmem,
        scratch_shapes=[
            pltpu.VMEM((2, depth, slots), F32),
            pltpu.VMEM((4, depth, slots), BF16),
            pltpu.VMEM((2 * cols, depth), F32),
            pltpu.VMEM((2, cols, depth), F32),
            pltpu.VMEM((2, plane, 2, cols, depth), F32),
            pltpu.VMEM((2,) + blocks, F32),
            pltpu.VMEM(blocks, F32),
            pltpu.VMEM(blocks, F32),
            pltpu.VMEM((2, 16, 2, slots), F32),
            pltpu.VMEM((2, plane, 2, slots), F32),
            pltpu.VMEM((2, rows, plane * slots), BF16),
            pltpu.VMEM((2, wide, plane * slots), BF16),
            pltpu.VMEM((4 * wide, 4 * slots), BF16),
            pltpu.VMEM((rows, 4 * wide), F32),
            pltpu.VMEM((1, groups * slots), jnp.int32),
            pltpu.SMEM((groups,), jnp.int32),
            pltpu.VMEM((groups,) + potential.shape, F32),
            *[pltpu.VMEM(table.shape, table.dtype) for table in consts],
            pltpu.VMEM((2, 2 * wide, 2 * radix * box), BF16),
            pltpu.VMEM((rows, 2 * radix * box), F32),
            pltpu.VMEM((2, radix, 2 * window, radix * box), BF16),
            pltpu.VMEM((radix, 2 * window, radix * box), F32),
            pltpu.VMEM((2, rows, 2 * radix * box), BF16),
            dma((10,)),
            dma((3,)),
            dma((3,)),
            dma((4,)),
            dma((4,)),
            dma((2,)),
            dma((2,)),
            dma((2,)),
            dma((2,)),
            dma((2,)),
            dma((2, 4)),
        ],
        compiler_params=pltpu.CompilerParams(
            collective_id=0, has_side_effects=True, vmem_limit_bytes=60 * 1024 * 1024
        ),
    )(coefficients, rot, potential, index_map[None], counts, *consts)


def apply_kernel(
    box, window, radix, pot_ready, grid_field, pot_ref, right_ref, left_ref, back_ref, twist_ref,
    field_ref, mixed_ref, unmixed_ref, turned_ref, out_ref
):
    coarse = window // radix
    rows = radix * window
    cols = coarse * window
    wide = radix * box
    lanes = 128
    per = wide // pot_ref.shape[2]

    with jax.named_scope("fwd_right"):
        parts = split_parts(grid_field)

        def spread(c, carry):
            at = pl.ds(pl.multiple_of(c * wide, wide), wide)
            field_ref[:, at] = dot3(parts, [right_ref[i, :, at] for i in range(2)])
            return carry

        lax.fori_loop(0, 2, spread, 0)

    def mix(tile, carry):
        at = pl.ds(pl.multiple_of(tile * lanes, lanes), lanes)
        imag_at = pl.ds(pl.multiple_of(wide + tile * lanes, lanes), lanes)
        values = []
        for low in range(radix):
            real = field_ref[low * window : (low + 1) * window, at]
            imag = field_ref[low * window : (low + 1) * window, imag_at]
            cos, sin = twist_ref[0, low : low + 1, at], twist_ref[1, low : low + 1, at]
            values.append((real * cos - imag * sin, real * sin + imag * cos))
        for k, pair in enumerate(fft8(values, 1)):
            for c in range(2):
                high, low = split_parts(pair[c])
                mixed_ref[0, k, c * window : (c + 1) * window, at] = high
                mixed_ref[1, k, c * window : (c + 1) * window, at] = low
        return carry

    with jax.named_scope("mix"):
        lax.fori_loop(0, wide // lanes, mix, 0)
    with jax.named_scope("wait_pot"):
        pot_ready()

    with jax.named_scope("left"):
        for k in range(radix):
            for n in range(2):
                at = slice(n * 2 * lanes, (n + 1) * 2 * lanes)
                high, low = mixed_ref[0, k, :, at], mixed_ref[1, k, :, at]
                space = jnp.dot(
                    left_ref[...], jnp.concatenate([high, high, low, low], axis=0), preferred_element_type=F32
                )
                pot = jnp.concatenate([pot_ref[k * per + 2 * n + i] for i in range(2)], axis=1)
                high, low = split_parts(space * jnp.concatenate([pot, pot], axis=0))
                both = jnp.dot(back_ref[...], jnp.concatenate([high, low], axis=0), preferred_element_type=F32)
                unmixed_ref[k, :, at] = both[: 2 * window] + both[2 * window :]

    def unmix(tile, carry):
        at = pl.ds(pl.multiple_of(tile * lanes, lanes), lanes)
        imag_at = pl.ds(pl.multiple_of(wide + tile * lanes, lanes), lanes)
        values = [
            (unmixed_ref[k, :window, at], unmixed_ref[k, window:, at]) for k in range(radix)
        ]
        for low, (real, imag) in enumerate(fft8(values, -1)):
            cos, sin = twist_ref[0, low : low + 1, at], twist_ref[1, low : low + 1, at]
            turned = (real * cos + imag * sin, imag * cos - real * sin)
            for value, to in zip(turned, (at, imag_at)):
                for i, part in enumerate(split_parts(value)):
                    turned_ref[i, low * window : (low + 1) * window, to] = part
        return carry

    with jax.named_scope("unmix"):
        lax.fori_loop(0, wide // lanes, unmix, 0)
    with jax.named_scope("back_right"):
        applied = dot3([turned_ref[0], turned_ref[1]], [right_ref[0], right_ref[1]], ((1,), (1,)))

    half = window // 2
    row_at = lax.broadcasted_iota(jnp.int32, (rows, cols), 0)
    col_at = lax.broadcasted_iota(jnp.int32, (rows, cols), 1)
    n_x = (row_at % window - half).astype(F32)
    n_y = (col_at // window * radix + row_at // window - half).astype(F32)
    n_z = (col_at % window - half).astype(F32)
    kinetic = (8.0 / (box * box)) * (n_x * n_x + n_y * n_y + n_z * n_z)
    applied = applied + jnp.concatenate([kinetic, kinetic], axis=1) * grid_field
    for c in range(2):
        pieces = [
            applied[lo * window : (lo + 1) * window, c * cols + hi * window : c * cols + (hi + 1) * window]
            for hi in range(coarse)
            for lo in range(radix)
        ]
        out_ref[0, c] = jnp.concatenate(pieces, axis=1)


def per_device(coefficients, rotation, potential, index_map, counts):
    box = potential.shape[0]
    window = box // 2
    radix = math.isqrt(box)
    assert radix * radix == box
    consts = [jnp.asarray(t) for t in tables(box, window, radix)]
    return run(coefficients, rotation, potential, index_map, counts, consts, box, window, radix)


def solution(mesh):
    placed = (P("band", None, "ga"), P(None, "band", "ga"), P(None, "ga"), P(), P())
    return jax.shard_map(
        per_device,
        mesh=mesh,
        in_specs=placed,
        out_specs=P(("band", "ga"), None, None, None),
        check_vma=False,
    )
```

```python
import functools
import math

import jax
import jax.numpy as jnp
import numpy as np
from jax import lax
from jax.experimental import pallas as pl
from jax.experimental.pallas import tpu as pltpu
from jax.sharding import PartitionSpec as P

F32 = jnp.float32
BF16 = jnp.bfloat16


def split_parts(values):
    high = values.astype(BF16)
    return high, (values - high.astype(F32)).astype(BF16)


def two_parts(table):
    high = table.astype(BF16)
    low = (table - high.astype(np.float32)).astype(BF16)
    return np.stack([high, low])


def tables(box, window, radix):
    half = window // 2
    coarse = window // radix
    k_all = np.arange(box)
    n_signed = np.arange(window) - half
    low = np.arange(radix)
    y_phase = (radix * np.arange(coarse) - half)[:, None] * low[None, :]
    z_phase = n_signed[:, None] * k_all[None, :]
    right = y_phase[:, None, :, None] + z_phase[None, :, None, :]
    right = right.reshape(coarse * window, radix * box) % box
    x_phase = k_all[:, None] * n_signed[None, :] % box
    twist = np.repeat(low[:, None] * low[None, :], box, axis=1) % box

    def pair(phase, scale=1.0):
        angle = phase * (2.0 * math.pi / box)
        return (np.stack([np.cos(angle), np.sin(angle)]) * scale).astype(np.float32)

    right_tab = two_parts(pair(right))
    cos, sin = pair(x_phase)
    left_high, left_low = two_parts(np.block([[cos, -sin], [sin, cos]]) / np.float32(box**3))
    left_tab = np.concatenate([left_high, left_low, left_high, left_low], axis=1)
    back_high, back_low = two_parts(np.block([[cos.T, sin.T], [-sin.T, cos.T]]))
    back_tab = np.block([[back_high, back_high], [back_low, back_low]])
    return right_tab, left_tab, back_tab, pair(twist)


def fft8(values, sign):
    root = math.sqrt(0.5)

    def add(a, b):
        return a[0] + b[0], a[1] + b[1]

    def sub(a, b):
        return a[0] - b[0], a[1] - b[1]

    def turn(a):
        return (-a[1], a[0]) if sign > 0 else (a[1], -a[0])

    def fft4(a, b, c, d):
        total, diff = add(a, c), sub(a, c)
        other, cross = add(b, d), turn(sub(b, d))
        return add(total, other), add(diff, cross), sub(total, other), sub(diff, cross)

    even = fft4(*values[0::2])
    odd = list(fft4(*values[1::2]))
    one, three = odd[1], odd[3]
    one_turn, three_turn = turn(one), turn(three)
    odd[1] = ((one[0] + one_turn[0]) * root, (one[1] + one_turn[1]) * root)
    odd[2] = turn(odd[2])
    odd[3] = ((three_turn[0] - three[0]) * root, (three_turn[1] - three[1]) * root)
    return [add(a, b) for a, b in zip(even, odd)] + [sub(a, b) for a, b in zip(even, odd)]


def dot3(lhs, rhs, dims=((1,), (0,))):
    def one(a, b):
        return lax.dot_general(a, b, (dims, ((), ())), preferred_element_type=F32)

    return one(lhs[0], rhs[0]) + (one(lhs[0], rhs[1]) + one(lhs[1], rhs[0]))


def block(cos, sin):
    upper = jnp.concatenate([cos, sin], axis=1)
    lower = jnp.concatenate([-sin, cos], axis=1)
    return jnp.concatenate([upper, lower], axis=0)


def whole_kernel(
    box, window, radix, coef_hbm, rot_hbm, pot_hbm, idx_hbm, cnt_hbm, right_hbm, left_hbm, back_hbm, twist_hbm,
    out_ref, coef, coef_parts, rot_raw, rot_own, rots, prod, drecv, zrecv, tout, land, onehot, hits, acc, idx, cnt,
    pot_out, right_tab, left_tab, back_tab, twist, right_blk, field, mixed, unmixed, turned, kinetic, out_buf,
    load_sem, rot_send, rot_recv, pot_send, pot_recv, pair_send, pair_recv, line_send, line_recv, val_send, val_recv,
    out_sem
):
    band = lax.axis_index("band")
    me = lax.axis_index("ga")
    groups = 2 * rots.shape[1]
    plane = groups // 2
    lines = zrecv.shape[1]
    line, core = band // 2, lax.rem(band, 2)
    cell, side = me // 2, lax.rem(me, 2)
    across = cell * 2 + (1 - side)
    sibling = line * 2 + (1 - core)
    mirror = (lines - 1 - line) * 2 + core
    half_rows = pot_hbm.shape[0] // 2
    share = pl.ds(pl.multiple_of(core * half_rows, half_rows), half_rows)
    slots = coef.shape[2]

    def local(src, dst, i):
        copy = pltpu.make_async_copy(src, dst, load_sem.at[i])
        copy.start()
        return copy

    barrier = pltpu.get_barrier_semaphore()

    def greet(to_band, to):
        pl.semaphore_signal(
            barrier, inc=1, device_id={"band": to_band, "ga": to}, device_id_type=pl.DeviceIdType.MESH
        )

    def peers(act):
        def body(step, code):
            shift = lax.rem(code, 16)
            act(lax.rem(cell // 4 + shift // 4, 4) * 4 + lax.rem(cell + shift, 4))
            return code // 16

        lax.fori_loop(0, 8, body, jnp.int32(0x528E6B9A))
        lax.fori_loop(0, 7, body, jnp.int32(0xC431FD7))

    def lines_other(act):
        low = 1 - line // 2
        for step in range(lines):
            l = low * (lines - 1 - step) + (1 - low) * step

            @pl.when(l != line)
            def _(l=l):
                act(l)

    def remote(src, dst, send, recv, to_band, to):
        return pltpu.make_async_remote_copy(
            src_ref=src, dst_ref=dst, send_sem=send, recv_sem=recv,
            device_id={"band": to_band, "ga": to}, device_id_type=pl.DeviceIdType.MESH,
        )

    with jax.named_scope("barrier"):
        greet(band, across)
        greet(mirror, across)
        peers(lambda q: greet(band, q * 2 + side))
        lines_other(lambda l: greet(l * 2 + core, me))
        greet(sibling, me)

    rot_load = local(rot_hbm.at[0], rot_raw, 0)
    idx_load = local(idx_hbm, idx, 1)
    cnt_load = local(cnt_hbm, cnt, 2)
    coef_loads = [local(coef_hbm.at[:, c, :], coef.at[c], 3 + c) for c in range(2)]
    pot_load = local(pot_hbm, pot_out.at[me], 5)
    tab_loads = [
        local(src, dst, 6 + i)
        for i, (src, dst) in enumerate(
            ((right_hbm, right_tab), (left_hbm, left_tab), (back_hbm, back_tab), (twist_hbm, twist))
        )
    ]

    def split_coef():
        for c in range(2):
            coef_loads[c].wait()
            high, low = split_parts(coef[c])
            coef_parts[2 * c] = high
            coef_parts[2 * c + 1] = low
        rot_load.wait()
        for e in range(2):
            for c in range(2):
                for x in range(4):
                    rot_own[e, 4 * c + x] = rot_raw[8 * c + 2 * x + e]

    with jax.named_scope("barrier_wait"):
        split_coef()
        pl.semaphore_wait(barrier, plane - 1 + 3 + lines - 1)

    def rot_swap():
        return remote(rot_own, rots.at[side, cell], rot_send.at[0], rot_recv.at[0], band, across)

    def rot_copy(which, held, q):
        slot = rots.at[held, cell]
        src = rot_own if which == 1 else slot
        return remote(src, slot, rot_send.at[which], rot_recv.at[which], band, q * 2 + side)

    def rot_all(which):
        part = rots.at[0, pl.ds(0, plane - 1)]
        return remote(part, part, rot_send.at[which], rot_recv.at[which], band, across)

    def pot_swap():
        part = pot_out.at[me, share]
        return remote(part, part, pot_send.at[0], pot_recv.at[0], mirror, across)

    def pot_copy(which, piece, q):
        part = pot_out.at[piece, share]
        return remote(part, part, pot_send.at[which], pot_recv.at[which], band, q * 2 + side)

    def pot_all(which):
        part = pot_out.at[pl.ds(0, plane - 1), pl.ds(0, half_rows)]
        return remote(part, part, pot_send.at[which], pot_recv.at[which], band, across)

    def pot_pair():
        part = pot_out.at[:, share]
        return remote(part, part, pot_send.at[3], pot_recv.at[3], sibling, me)

    def pair_copy(step):
        return remote(prod.at[step, 0], drecv.at[step], pair_send.at[step], pair_recv.at[step], sibling, me)

    def line_copy(step, e, l):
        return remote(
            prod.at[step, 1, l, e], zrecv.at[step, line, e], line_send.at[step, e], line_recv.at[step, e],
            l * 2 + core, me,
        )

    def line_all(step, e):
        part = zrecv.at[step, pl.ds(0, lines - 1), 0]
        return remote(part, part, line_send.at[step, e], line_recv.at[step, e], sibling, me)

    def val_copy(step, turn, i, to_band, to):
        return remote(
            tout.at[turn, i], land.at[side, cell], val_send.at[step], val_recv.at[step, cell // 4], to_band, to
        )

    def val_all(step, batch, row, count):
        part = land.at[0, pl.ds(0, count)]
        return remote(part, part, val_send.at[step], val_recv.at[batch, row], band, across)

    with jax.named_scope("send_rot"):
        rot_swap().start()
        pot_load.wait()
        pot_swap().start()
        peers(lambda q: rot_copy(1, side, q).start())
        rots[side, cell] = rot_own[...]

    def mark(src, carry):
        at = pl.ds(pl.multiple_of(src * slots, slots), slots)
        to = pl.ds(pl.multiple_of(src // 2 * slots, slots), slots)
        half = window // 2
        cells = idx[:, at]
        cell_x = (cells // (box * box) + half) % box
        cell_y = (cells // box % box + half) % box
        cell_z = (cells % box + half) % box
        inside = (cell_x < window) & (cell_y < window) & (cell_z < window)
        live = lax.broadcasted_iota(jnp.int32, (1, slots), 1) < cnt[src]
        row_id = jnp.where(live & inside, cell_y % radix * window + cell_x, -1)
        col_id = cell_y // radix * window + cell_z
        rows, cols = onehot.shape[1], hits.shape[1]
        picks = lax.broadcasted_iota(jnp.int32, (rows, slots), 0) == row_id
        onehot[lax.rem(src, 2), :, to] = jnp.where(picks, 1.0, 0.0).astype(BF16)
        found = lax.broadcasted_iota(jnp.int32, (cols, slots), 0) == col_id
        hits[lax.rem(src, 2), :, to] = jnp.where(found, 1.0, 0.0).astype(BF16)
        return carry

    with jax.named_scope("mark0"):
        idx_load.wait()
        cnt_load.wait()
        lax.fori_loop(0, 4, mark, 0)

    with jax.named_scope("relay_rot"):
        rot_swap().wait_recv()
        pot_swap().wait_recv()
        peers(lambda q: rot_copy(2, 1 - side, q).start())
        lax.fori_loop(4, 8, mark, 0)

    def rotate(held, to_core):
        blocks = []
        for l in range(lines):
            for l_of, e in ((l, side), (lines - 1 - l, 1 - side)):
                for r in range(2):
                    blocks.append(rots[held, l_of * 4 + to_core * 2 + r, e])
        a = jnp.concatenate(blocks, axis=0)
        b = jnp.concatenate([piece for blk in blocks for piece in (-blk[4:], blk[:4])], axis=0)
        a_high, a_low = split_parts(a)
        b_high, b_low = split_parts(b)
        lhs = jnp.concatenate([a_high, a_low, a_high, b_high, b_low, b_high], axis=1)
        rhs = jnp.concatenate(
            [coef_parts[0], coef_parts[0], coef_parts[1], coef_parts[2], coef_parts[2], coef_parts[3]], axis=0
        )
        return jnp.dot(lhs, rhs, preferred_element_type=F32).reshape(lines, 2, 2, 8, slots)

    def first_half(step, carry):
        with jax.named_scope("wait_rot"):
            rot_all(1 + step).wait_recv()

        def part(i, carry):
            with jax.named_scope("rotate"):
                prod[step, i] = rotate(lax.rem(side + step, 2), lax.rem(core + 1 + i, 2))

            @pl.when(i == 0)
            def _():
                pair_copy(step).start()

            return carry

        lax.fori_loop(0, 2, part, 0)

        with jax.named_scope("pair"):
            pair_copy(step).wait_recv()
            prod[step, 1] = prod[step, 1] + drecv[step]
            for e in (1, 0):
                lines_other(lambda l: line_copy(step, e, l).start())

        @pl.when(step == 1)
        def _():
            with jax.named_scope("relay_pot"):
                peers(lambda q: pot_copy(1, me, q).start())
                peers(lambda q: pot_copy(2, across, q).start())

        return carry

    lax.fori_loop(0, 2, first_half, 0)
    with jax.named_scope("blocks"):
        for tab in tab_loads:
            tab.wait()
        for i in range(2):
            right_blk[i] = block(right_tab[i, 0], right_tab[i, 1])
        kinetic[...] = kinetic_factors(box, window, radix)

    def second_half(turn, carry):
        step, e = turn // 2, 1 - lax.rem(turn, 2)
        with jax.named_scope("mark1"):
            before = jnp.where(turn == 0, 8, jnp.where(turn == 1, 20, jnp.where(turn == 2, 30, groups)))
            lax.fori_loop(jnp.where(turn == 0, 8, jnp.where(turn == 1, 8, jnp.where(turn == 2, 20, 30))), before, mark, 0)
        with jax.named_scope("wait_line"):
            line_all(step, e).wait_recv()
        with jax.named_scope("send_val"):
            total = prod[step, 1, line, e]
            for other in range(1, lines):
                total = total + zrecv[step, lax.rem(line + other, lines), e]
            for r in range(2):
                for c in range(2):
                    tout[turn, r * 4 : r * 4 + 4, c, :] = total[r, c * 4 : c * 4 + 4]

            def send(n, carry):
                r = lax.rem(cell // 8 + 1 + n // 4, 2)
                m = lax.rem(n, 4)
                x = lax.rem(cell + jnp.where(m == 0, 2, jnp.where(m == 1, 1, jnp.where(m == 2, 3, 0))), 4)
                to = (r * 8 + lax.rem(side + step, 2) * 4 + x) * 2 + lax.rem(side + e, 2)
                i = r * 4 + x

                @pl.when(to != me)
                def _():
                    val_copy(step, turn, i, (1 - e) * band + e * mirror, to).start()

                @pl.when(to == me)
                def _():
                    land[side, cell] = tout[turn, i]

                return carry

            lax.fori_loop(0, 8, send, 0)
        return carry

    lax.fori_loop(0, 4, second_half, 0)
    with jax.named_scope("pair_pot"):
        pot_all(1).wait_recv()
        pot_all(2).wait_recv()
        pot_pair().start()

    early = lax.rem(me // 8, 2)
    mine_first = early == side
    acc[...] = jnp.zeros_like(acc)

    def collect(step, carry):
        batch, near = step // 4, lax.rem(step, 4)
        parity = lax.rem(early + batch, 2)
        row = lax.rem(cell // 4 + near + near // 2 - 2 * (near // 3), 4)
        alone = (parity == side) & (row == cell // 4)

        @pl.when(alone)
        def _():
            val_all(0, batch, row, 3).wait_recv()

        @pl.when(jnp.logical_not(alone))
        def _():
            val_all(0, batch, row, 4).wait_recv()

        deep = 4 * slots
        span = pl.ds(pl.multiple_of(row * deep, deep), deep)
        cols = hits.shape[1]
        placed = [[], []]
        for u in range(4):
            to = pl.ds(pl.multiple_of(row * deep + u * slots, slots), slots)
            mask = hits[parity, :, to]
            for n, part in enumerate(split_parts(land[parity, row * 4 + u])):
                part = part.astype(F32)
                pieces = []
                for c in range(2):
                    line_of = jnp.broadcast_to(part[c : c + 1, :], (16, slots)).astype(BF16)
                    pieces.append(mask * jnp.concatenate([line_of] * (cols // 16), axis=0))
                placed[n].append(jnp.concatenate(pieces, axis=0))
        picked = onehot[parity, :, span]
        high, low = (
            lax.dot_general(
                picked, jnp.concatenate(part, axis=1), (((1,), (1,)), ((), ())), preferred_element_type=F32
            )
            for part in placed
        )
        acc[...] += high + low
        return carry

    with jax.named_scope("collect"):
        lax.fori_loop(0, 8, collect, 0)
    grid_field = acc[...]

    def pot_ready():
        pot_pair().wait_recv()

    def out_copy(c):
        return pltpu.make_async_copy(out_buf.at[c], out_ref.at[0, c], out_sem.at[c])

    apply_kernel(
        box, window, radix, band >= 0, pot_ready, grid_field, pot_out, right_blk, left_tab, back_tab, twist,
        field, mixed, unmixed, turned, kinetic, out_buf, lambda c: out_copy(c).start()
    )
    with jax.named_scope("wait_sends"):
        for c in range(2):
            out_copy(c).wait()
        rot_swap().wait_send()
        rot_all(1).wait_send()
        rot_all(2).wait_send()
        pot_swap().wait_send()
        pot_all(1).wait_send()
        pot_all(2).wait_send()
        pot_pair().wait_send()
        for step in range(2):
            pair_copy(step).wait_send()
            for e in range(2):
                line_all(step, e).wait_send()
            alone = mine_first if step == 0 else jnp.logical_not(mine_first)

            @pl.when(alone)
            def _():
                val_all(step, 0, 0, plane - 1).wait_send()

            @pl.when(jnp.logical_not(alone))
            def _():
                val_all(step, 0, 0, plane).wait_send()


def run(coefficients, rotation, potential, index_map, counts, consts, box, window, radix):
    bands, groups = lax.axis_size("band"), lax.axis_size("ga")
    depth, _, slots = coefficients.shape
    cols = rotation.shape[2]
    assert (bands, groups, cols) == (8, 32, 8)
    lines, plane = bands // 2, groups // 2
    rot = rotation.transpose(0, 2, 1).reshape(1, 2 * cols, depth)
    hbm = pl.BlockSpec(memory_space=pl.ANY)
    dma = pltpu.SemaphoreType.DMA
    rows, wide = radix * window, window // radix * window
    blocks = (2, lines, 2, 2, 8, slots)
    return pl.pallas_call(
        functools.partial(whole_kernel, box, window, radix),
        out_shape=jax.ShapeDtypeStruct((1, 2, window, window * window), F32),
        in_specs=[hbm] * 9,
        out_specs=hbm,
        scratch_shapes=[
            pltpu.VMEM((2, depth, slots), F32),
            pltpu.VMEM((4, depth, slots), BF16),
            pltpu.VMEM((2 * cols, depth), F32),
            pltpu.VMEM((2, cols, depth), F32),
            pltpu.VMEM((2, plane, 2, cols, depth), F32),
            pltpu.VMEM((2,) + blocks, F32),
            pltpu.VMEM(blocks, F32),
            pltpu.VMEM(blocks, F32),
            pltpu.VMEM((4, 8, 2, slots), F32),
            pltpu.VMEM((2, plane, 2, slots), F32),
            pltpu.VMEM((2, rows, plane * slots), BF16),
            pltpu.VMEM((2, wide, plane * slots), BF16),
            pltpu.VMEM((rows, 2 * wide), F32),
            pltpu.VMEM((1, groups * slots), jnp.int32),
            pltpu.SMEM((groups,), jnp.int32),
            pltpu.VMEM((groups,) + potential.shape, F32),
            *[pltpu.VMEM(table.shape, table.dtype) for table in consts],
            pltpu.VMEM((2, 2 * wide, 2 * radix * box), BF16),
            pltpu.VMEM((rows, 2 * radix * box), F32),
            pltpu.VMEM((2, radix, 2 * window, radix * box), BF16),
            pltpu.VMEM((radix, 2 * window, radix * box), F32),
            pltpu.VMEM((2, rows, 2 * radix * box), BF16),
            pltpu.VMEM((rows, wide), F32),
            pltpu.VMEM((2, window, window * window), F32),
            dma((10,)),
            dma((3,)),
            dma((3,)),
            dma((4,)),
            dma((4,)),
            dma((2,)),
            dma((2,)),
            dma((2, 2)),
            dma((2, 2)),
            dma((2,)),
            dma((2, 4)),
            dma((2,)),
        ],
        compiler_params=pltpu.CompilerParams(
            collective_id=0, has_side_effects=True, vmem_limit_bytes=60 * 1024 * 1024
        ),
    )(coefficients, rot, potential, index_map[None], counts, *consts)


def kinetic_factors(box, window, radix):
    rows, cols = radix * window, window // radix * window
    half = window // 2
    row_at = lax.broadcasted_iota(jnp.int32, (rows, cols), 0)
    col_at = lax.broadcasted_iota(jnp.int32, (rows, cols), 1)
    n_x = (row_at % window - half).astype(F32)
    n_y = (col_at // window * radix + row_at // window - half).astype(F32)
    n_z = (col_at % window - half).astype(F32)
    return (8.0 / (box * box)) * (n_x * n_x + n_y * n_y + n_z * n_z)


def apply_kernel(
    box, window, radix, apart, pot_ready, grid_field, pot_ref, right_ref, left_ref, back_ref, twist_ref,
    field_ref, mixed_ref, unmixed_ref, turned_ref, kinetic_ref, out_ref, ship
):
    coarse = window // radix
    rows = radix * window
    cols = coarse * window
    wide = radix * box
    lanes = 128
    per = wide // pot_ref.shape[2]

    with jax.named_scope("fwd_right"):
        field_ref[...] = dot3(split_parts(grid_field), [right_ref[0], right_ref[1]])

    def mix(tile, carry):
        at = pl.ds(pl.multiple_of(tile * lanes, lanes), lanes)
        imag_at = pl.ds(pl.multiple_of(wide + tile * lanes, lanes), lanes)
        values = []
        for low in range(radix):
            real = field_ref[low * window : (low + 1) * window, at]
            imag = field_ref[low * window : (low + 1) * window, imag_at]
            cos, sin = twist_ref[0, low : low + 1, at], twist_ref[1, low : low + 1, at]
            values.append((real * cos - imag * sin, real * sin + imag * cos))
        for k, pair in enumerate(fft8(values, 1)):
            for c in range(2):
                high, low = split_parts(pair[c])
                mixed_ref[0, k, c * window : (c + 1) * window, at] = high
                mixed_ref[1, k, c * window : (c + 1) * window, at] = low
        return carry

    with jax.named_scope("mix"):
        lax.fori_loop(0, wide // lanes, mix, 0)
    with jax.named_scope("wait_pot"):
        pot_ready()

    with jax.named_scope("left"):
        @pl.when(apart)
        def _():
            for k in range(radix):
                for n in range(2):
                    at = slice(n * 2 * lanes, (n + 1) * 2 * lanes)
                    high, low = mixed_ref[0, k, :, at], mixed_ref[1, k, :, at]
                    space = jnp.dot(
                        left_ref[...], jnp.concatenate([high, high, low, low], axis=0), preferred_element_type=F32
                    )
                    pot = jnp.concatenate([pot_ref[k * per + 2 * n + i] for i in range(2)], axis=1)
                    high, low = split_parts(space * jnp.concatenate([pot, pot], axis=0))
                    both = jnp.dot(back_ref[...], jnp.concatenate([high, low], axis=0), preferred_element_type=F32)
                    unmixed_ref[k, :, at] = both[: 2 * window] + both[2 * window :]

    def unmix(tile, carry):
        at = pl.ds(pl.multiple_of(tile * lanes, lanes), lanes)
        imag_at = pl.ds(pl.multiple_of(wide + tile * lanes, lanes), lanes)
        values = [
            (unmixed_ref[k, :window, at], unmixed_ref[k, window:, at]) for k in range(radix)
        ]
        for low, (real, imag) in enumerate(fft8(values, -1)):
            cos, sin = twist_ref[0, low : low + 1, at], twist_ref[1, low : low + 1, at]
            turned = (real * cos + imag * sin, imag * cos - real * sin)
            for value, to in zip(turned, (at, imag_at)):
                for i, part in enumerate(split_parts(value)):
                    turned_ref[i, low * window : (low + 1) * window, to] = part
        return carry

    with jax.named_scope("unmix"):
        lax.fori_loop(0, wide // lanes, unmix, 0)
    with jax.named_scope("back_right"):
        applied = dot3([turned_ref[0], turned_ref[1]], [right_ref[0], right_ref[1]], ((1,), (1,)))

    kinetic = kinetic_ref[...]
    applied = applied + jnp.concatenate([kinetic, kinetic], axis=1) * grid_field
    for c in range(2):
        pieces = [
            applied[lo * window : (lo + 1) * window, c * cols + hi * window : c * cols + (hi + 1) * window]
            for hi in range(coarse)
            for lo in range(radix)
        ]
        out_ref[c] = jnp.concatenate(pieces, axis=1)
        ship(c)


def per_device(coefficients, rotation, potential, index_map, counts):
    box = potential.shape[0]
    window = box // 2
    radix = math.isqrt(box)
    assert radix * radix == box
    consts = [jnp.asarray(t) for t in tables(box, window, radix)]
    return run(coefficients, rotation, potential, index_map, counts, consts, box, window, radix)


def solution(mesh):
    placed = (P("band", None, "ga"), P(None, "band", "ga"), P(None, "ga"), P(), P())
    return jax.shard_map(
        per_device,
        mesh=mesh,
        in_specs=placed,
        out_specs=P(("band", "ga"), None, None, None),
        check_vma=False,
    )
```

```python
import functools
import math

import jax
import jax.numpy as jnp
import numpy as np
from jax import lax
from jax.experimental import pallas as pl
from jax.experimental.pallas import tpu as pltpu
from jax.sharding import PartitionSpec as P

F32 = jnp.float32
BF16 = jnp.bfloat16


def split_parts(values):
    high = values.astype(BF16)
    return high, (values - high.astype(F32)).astype(BF16)


def two_parts(table):
    high = table.astype(BF16)
    low = (table - high.astype(np.float32)).astype(BF16)
    return np.stack([high, low])


def tables(box, window, radix):
    half = window // 2
    coarse = window // radix
    k_all = np.arange(box)
    n_signed = np.arange(window) - half
    low = np.arange(radix)
    y_phase = (radix * np.arange(coarse) - half)[:, None] * low[None, :]
    z_phase = n_signed[:, None] * k_all[None, :]
    right = y_phase[:, None, :, None] + z_phase[None, :, None, :]
    right = right.reshape(coarse * window, radix * box) % box
    x_phase = k_all[:, None] * n_signed[None, :] % box
    twist = np.repeat(low[:, None] * low[None, :], box, axis=1) % box

    def pair(phase, scale=1.0):
        angle = phase * (2.0 * math.pi / box)
        return (np.stack([np.cos(angle), np.sin(angle)]) * scale).astype(np.float32)

    right_tab = two_parts(pair(right))
    cos, sin = pair(x_phase)
    left_high, left_low = two_parts(np.block([[cos, -sin], [sin, cos]]) / np.float32(box**3))
    left_tab = np.concatenate([left_high, left_low, left_high, left_low], axis=1)
    back_high, back_low = two_parts(np.block([[cos.T, sin.T], [-sin.T, cos.T]]))
    back_tab = np.block([[back_high, back_high], [back_low, back_low]])
    return right_tab, left_tab, back_tab, pair(twist)


def fft8(values, sign):
    root = math.sqrt(0.5)

    def add(a, b):
        return a[0] + b[0], a[1] + b[1]

    def sub(a, b):
        return a[0] - b[0], a[1] - b[1]

    def turn(a):
        return (-a[1], a[0]) if sign > 0 else (a[1], -a[0])

    def fft4(a, b, c, d):
        total, diff = add(a, c), sub(a, c)
        other, cross = add(b, d), turn(sub(b, d))
        return add(total, other), add(diff, cross), sub(total, other), sub(diff, cross)

    even = fft4(*values[0::2])
    odd = list(fft4(*values[1::2]))
    one, three = odd[1], odd[3]
    one_turn, three_turn = turn(one), turn(three)
    odd[1] = ((one[0] + one_turn[0]) * root, (one[1] + one_turn[1]) * root)
    odd[2] = turn(odd[2])
    odd[3] = ((three_turn[0] - three[0]) * root, (three_turn[1] - three[1]) * root)
    return [add(a, b) for a, b in zip(even, odd)] + [sub(a, b) for a, b in zip(even, odd)]


def dot3(lhs, rhs, dims=((1,), (0,))):
    def one(a, b):
        return lax.dot_general(a, b, (dims, ((), ())), preferred_element_type=F32)

    return one(lhs[0], rhs[0]) + (one(lhs[0], rhs[1]) + one(lhs[1], rhs[0]))


def block(cos, sin):
    upper = jnp.concatenate([cos, sin], axis=1)
    lower = jnp.concatenate([-sin, cos], axis=1)
    return jnp.concatenate([upper, lower], axis=0)


def whole_kernel(
    box, window, radix, coef_hbm, rot_hbm, pot_hbm, idx_hbm, cnt_hbm, right_hbm, left_hbm, back_hbm, twist_hbm,
    out_ref, coef, coef_parts, rot_raw, rot_own, rots, prod, drecv, zrecv, tout, land, onehot, hits, acc, idx, cnt,
    pot_out, right_tab, left_tab, back_tab, twist, right_blk, field, mixed, unmixed, turned, kinetic, out_buf,
    load_sem, rot_send, rot_recv, pot_send, pot_recv, pair_send, pair_recv, line_send, line_recv, val_send, val_recv,
    out_sem
):
    band = lax.axis_index("band")
    me = lax.axis_index("ga")
    groups = 2 * rots.shape[1]
    plane = groups // 2
    lines = zrecv.shape[1]
    line, core = band // 2, lax.rem(band, 2)
    cell, side = me // 2, lax.rem(me, 2)
    across = cell * 2 + (1 - side)
    sibling = line * 2 + (1 - core)
    mirror = (lines - 1 - line) * 2 + core
    half_rows = pot_hbm.shape[0] // 2
    share = pl.ds(pl.multiple_of(core * half_rows, half_rows), half_rows)
    slots = coef.shape[2]

    def local(src, dst, i):
        copy = pltpu.make_async_copy(src, dst, load_sem.at[i])
        copy.start()
        return copy

    barrier = pltpu.get_barrier_semaphore()

    def greet(to_band, to):
        pl.semaphore_signal(
            barrier, inc=1, device_id={"band": to_band, "ga": to}, device_id_type=pl.DeviceIdType.MESH
        )

    def peers(act):
        def body(step, code):
            shift = lax.rem(code, 16)
            act(lax.rem(cell // 4 + shift // 4, 4) * 4 + lax.rem(cell + shift, 4))
            return code // 16

        lax.fori_loop(0, 8, body, jnp.int32(0x528E6B9A))
        lax.fori_loop(0, 7, body, jnp.int32(0xC431FD7))

    def lines_other(act):
        low = 1 - line // 2
        for step in range(lines):
            l = low * (lines - 1 - step) + (1 - low) * step

            @pl.when(l != line)
            def _(l=l):
                act(l)

    def remote(src, dst, send, recv, to_band, to):
        return pltpu.make_async_remote_copy(
            src_ref=src, dst_ref=dst, send_sem=send, recv_sem=recv,
            device_id={"band": to_band, "ga": to}, device_id_type=pl.DeviceIdType.MESH,
        )

    with jax.named_scope("barrier"):
        greet(band, across)
        greet(mirror, across)
        peers(lambda q: greet(band, q * 2 + side))
        lines_other(lambda l: greet(l * 2 + core, me))
        greet(sibling, me)

    rot_load = local(rot_hbm.at[0], rot_raw, 0)
    idx_load = local(idx_hbm, idx, 1)
    cnt_load = local(cnt_hbm, cnt, 2)
    coef_loads = [local(coef_hbm.at[:, c, :], coef.at[c], 3 + c) for c in range(2)]
    pot_load = local(pot_hbm, pot_out.at[me], 5)
    tab_loads = [
        local(src, dst, 6 + i)
        for i, (src, dst) in enumerate(
            ((right_hbm, right_tab), (left_hbm, left_tab), (back_hbm, back_tab), (twist_hbm, twist))
        )
    ]

    def split_coef():
        for c in range(2):
            coef_loads[c].wait()
            high, low = split_parts(coef[c])
            coef_parts[2 * c] = high
            coef_parts[2 * c + 1] = low
        rot_load.wait()
        for e in range(2):
            for c in range(2):
                for x in range(4):
                    rot_own[e, 4 * c + x] = rot_raw[8 * c + 2 * x + e]

    with jax.named_scope("barrier_wait"):
        split_coef()
        pl.semaphore_wait(barrier, plane - 1 + 3 + lines - 1)

    def rot_swap():
        return remote(rot_own, rots.at[side, cell], rot_send.at[0], rot_recv.at[0], band, across)

    def rot_copy(which, held, q):
        slot = rots.at[held, cell]
        src = rot_own if which == 1 else slot
        return remote(src, slot, rot_send.at[which], rot_recv.at[which], band, q * 2 + side)

    def rot_all(which):
        part = rots.at[0, pl.ds(0, plane - 1)]
        return remote(part, part, rot_send.at[which], rot_recv.at[which], band, across)

    def pot_swap():
        part = pot_out.at[me, share]
        return remote(part, part, pot_send.at[0], pot_recv.at[0], mirror, across)

    def pot_copy(which, piece, q):
        part = pot_out.at[piece, share]
        return remote(part, part, pot_send.at[which], pot_recv.at[which], band, q * 2 + side)

    def pot_all(which):
        part = pot_out.at[pl.ds(0, plane - 1), pl.ds(0, half_rows)]
        return remote(part, part, pot_send.at[which], pot_recv.at[which], band, across)

    def pot_pair():
        part = pot_out.at[:, share]
        return remote(part, part, pot_send.at[3], pot_recv.at[3], sibling, me)

    def pair_copy(step):
        return remote(prod.at[step, 0], drecv.at[step], pair_send.at[step], pair_recv.at[step], sibling, me)

    def line_copy(step, e, l):
        return remote(
            prod.at[step, 1, l, e], zrecv.at[step, line, e], line_send.at[step, e], line_recv.at[step, e],
            l * 2 + core, me,
        )

    def line_all(step, e):
        part = zrecv.at[step, pl.ds(0, lines - 1), 0]
        return remote(part, part, line_send.at[step, e], line_recv.at[step, e], sibling, me)

    def val_copy(step, turn, i, to_band, to):
        return remote(
            tout.at[turn, i], land.at[side, cell], val_send.at[step], val_recv.at[step, cell // 4], to_band, to
        )

    def val_all(step, batch, row, count):
        part = land.at[0, pl.ds(0, count)]
        return remote(part, part, val_send.at[step], val_recv.at[batch, row], band, across)

    with jax.named_scope("send_rot"):
        rot_swap().start()
        pot_load.wait()
        pot_swap().start()
        peers(lambda q: rot_copy(1, side, q).start())
        rots[side, cell] = rot_own[...]

    def mark(src, carry):
        at = pl.ds(pl.multiple_of(src * slots, slots), slots)
        to = pl.ds(pl.multiple_of(src // 2 * slots, slots), slots)
        half = window // 2
        cells = idx[:, at]
        cell_x = (cells // (box * box) + half) % box
        cell_y = (cells // box % box + half) % box
        cell_z = (cells % box + half) % box
        inside = (cell_x < window) & (cell_y < window) & (cell_z < window)
        live = lax.broadcasted_iota(jnp.int32, (1, slots), 1) < cnt[src]
        row_id = jnp.where(live & inside, cell_y % radix * window + cell_x, -1)
        col_id = cell_y // radix * window + cell_z
        rows, cols = onehot.shape[1], hits.shape[1]
        picks = lax.broadcasted_iota(jnp.int32, (rows, slots), 0) == row_id
        onehot[lax.rem(src, 2), :, to] = jnp.where(picks, 1.0, 0.0).astype(BF16)
        found = lax.broadcasted_iota(jnp.int32, (cols, slots), 0) == col_id
        hits[lax.rem(src, 2), :, to] = jnp.where(found, 1.0, 0.0).astype(BF16)
        return carry

    with jax.named_scope("mark0"):
        idx_load.wait()
        cnt_load.wait()
        lax.fori_loop(0, 4, mark, 0)

    with jax.named_scope("relay_rot"):
        rot_swap().wait_recv()
        pot_swap().wait_recv()
        peers(lambda q: rot_copy(2, 1 - side, q).start())
        lax.fori_loop(4, 8, mark, 0)

    def rotate(held, to_core):
        blocks = []
        for l in range(lines):
            for l_of, e in ((l, side), (lines - 1 - l, 1 - side)):
                for r in range(2):
                    blocks.append(rots[held, l_of * 4 + to_core * 2 + r, e])
        a = jnp.concatenate(blocks, axis=0)
        b = jnp.concatenate([piece for blk in blocks for piece in (-blk[4:], blk[:4])], axis=0)
        a_high, a_low = split_parts(a)
        b_high, b_low = split_parts(b)
        lhs = jnp.concatenate([a_high, a_low, a_high, b_high, b_low, b_high], axis=1)
        rhs = jnp.concatenate(
            [coef_parts[0], coef_parts[0], coef_parts[1], coef_parts[2], coef_parts[2], coef_parts[3]], axis=0
        )
        return jnp.dot(lhs, rhs, preferred_element_type=F32).reshape(lines, 2, 2, 8, slots)

    def first_half(step, carry):
        with jax.named_scope("wait_rot"):
            rot_all(1 + step).wait_recv()

        def part(i, carry):
            with jax.named_scope("rotate"):
                prod[step, i] = rotate(lax.rem(side + step, 2), lax.rem(core + 1 + i, 2))

            @pl.when(i == 0)
            def _():
                pair_copy(step).start()

            return carry

        lax.fori_loop(0, 2, part, 0)

        with jax.named_scope("pair"):
            pair_copy(step).wait_recv()
            prod[step, 1] = prod[step, 1] + drecv[step]
            for e in (1, 0):
                lines_other(lambda l: line_copy(step, e, l).start())

        @pl.when(step == 1)
        def _():
            with jax.named_scope("relay_pot"):
                peers(lambda q: pot_copy(1, me, q).start())
                peers(lambda q: pot_copy(2, across, q).start())

        return carry

    lax.fori_loop(0, 2, first_half, 0)
    with jax.named_scope("blocks"):
        for tab in tab_loads:
            tab.wait()
        for i in range(2):
            right_blk[i] = block(right_tab[i, 0], right_tab[i, 1])
        kinetic[...] = kinetic_factors(box, window, radix)

    early = lax.rem(me // 8, 2)
    mine_first = early == side
    acc[...] = jnp.zeros_like(acc)

    def collect(step, carry):
        batch, near = step // 4, lax.rem(step, 4)
        parity = lax.rem(early + batch, 2)
        row = lax.rem(cell // 4 + near + near // 2 - 2 * (near // 3), 4)
        alone = (parity == side) & (row == cell // 4)

        @pl.when(alone)
        def _():
            val_all(0, batch, row, 3).wait_recv()

        @pl.when(jnp.logical_not(alone))
        def _():
            val_all(0, batch, row, 4).wait_recv()

        deep = 4 * slots
        span = pl.ds(pl.multiple_of(row * deep, deep), deep)
        cols = hits.shape[1]
        placed = [[], []]
        for u in range(4):
            to = pl.ds(pl.multiple_of(row * deep + u * slots, slots), slots)
            mask = hits[parity, :, to]
            for n, part in enumerate(split_parts(land[parity, row * 4 + u])):
                part = part.astype(F32)
                pieces = []
                for c in range(2):
                    line_of = jnp.broadcast_to(part[c : c + 1, :], (16, slots)).astype(BF16)
                    pieces.append(mask * jnp.concatenate([line_of] * (cols // 16), axis=0))
                placed[n].append(jnp.concatenate(pieces, axis=0))
        picked = onehot[parity, :, span]
        high, low = (
            lax.dot_general(
                picked, jnp.concatenate(part, axis=1), (((1,), (1,)), ((), ())), preferred_element_type=F32
            )
            for part in placed
        )
        acc[...] += high + low
        return carry

    def second_half(turn, carry):
        step, e = turn // 2, 1 - lax.rem(turn, 2)
        with jax.named_scope("mark1"):
            before = jnp.where(turn == 0, 8, jnp.where(turn == 1, 20, jnp.where(turn == 2, 30, groups)))
            lax.fori_loop(jnp.where(turn == 0, 8, jnp.where(turn == 1, 8, jnp.where(turn == 2, 20, 30))), before, mark, 0)
        @pl.when(turn == 3)
        def _():
            with jax.named_scope("collect0"):
                lax.fori_loop(0, 1, collect, 0)

        with jax.named_scope("wait_line"):
            line_all(step, e).wait_recv()
        with jax.named_scope("send_val"):
            total = prod[step, 1, line, e]
            for other in range(1, lines):
                total = total + zrecv[step, lax.rem(line + other, lines), e]
            for r in range(2):
                for c in range(2):
                    tout[turn, r * 4 : r * 4 + 4, c, :] = total[r, c * 4 : c * 4 + 4]

            def send(n, carry):
                r = lax.rem(cell // 8 + 1 + n // 4, 2)
                m = lax.rem(n, 4)
                x = lax.rem(cell + jnp.where(m == 0, 2, jnp.where(m == 1, 1, jnp.where(m == 2, 3, 0))), 4)
                to = (r * 8 + lax.rem(side + step, 2) * 4 + x) * 2 + lax.rem(side + e, 2)
                i = r * 4 + x

                @pl.when(to != me)
                def _():
                    val_copy(step, turn, i, (1 - e) * band + e * mirror, to).start()

                @pl.when(to == me)
                def _():
                    land[side, cell] = tout[turn, i]

                return carry

            lax.fori_loop(0, 8, send, 0)
        return carry

    lax.fori_loop(0, 4, second_half, 0)
    with jax.named_scope("pair_pot"):
        pot_all(1).wait_recv()
        pot_all(2).wait_recv()
        pot_pair().start()

    with jax.named_scope("collect"):
        lax.fori_loop(1, 8, collect, 0)
    grid_field = acc[...]

    def pot_ready():
        pot_pair().wait_recv()

    def out_copy(c):
        return pltpu.make_async_copy(out_buf.at[c], out_ref.at[0, c], out_sem.at[c])

    apply_kernel(
        box, window, radix, band >= 0, pot_ready, grid_field, pot_out, right_blk, left_tab, back_tab, twist,
        field, mixed, unmixed, turned, kinetic, out_buf, lambda c: out_copy(c).start()
    )
    with jax.named_scope("wait_sends"):
        for c in range(2):
            out_copy(c).wait()
        rot_swap().wait_send()
        rot_all(1).wait_send()
        rot_all(2).wait_send()
        pot_swap().wait_send()
        pot_all(1).wait_send()
        pot_all(2).wait_send()
        pot_pair().wait_send()
        for step in range(2):
            pair_copy(step).wait_send()
            for e in range(2):
                line_all(step, e).wait_send()
            alone = mine_first if step == 0 else jnp.logical_not(mine_first)

            @pl.when(alone)
            def _():
                val_all(step, 0, 0, plane - 1).wait_send()

            @pl.when(jnp.logical_not(alone))
            def _():
                val_all(step, 0, 0, plane).wait_send()


def run(coefficients, rotation, potential, index_map, counts, consts, box, window, radix):
    bands, groups = lax.axis_size("band"), lax.axis_size("ga")
    depth, _, slots = coefficients.shape
    cols = rotation.shape[2]
    assert (bands, groups, cols) == (8, 32, 8)
    lines, plane = bands // 2, groups // 2
    rot = rotation.transpose(0, 2, 1).reshape(1, 2 * cols, depth)
    hbm = pl.BlockSpec(memory_space=pl.ANY)
    dma = pltpu.SemaphoreType.DMA
    rows, wide = radix * window, window // radix * window
    blocks = (2, lines, 2, 2, 8, slots)
    return pl.pallas_call(
        functools.partial(whole_kernel, box, window, radix),
        out_shape=jax.ShapeDtypeStruct((1, 2, window, window * window), F32),
        in_specs=[hbm] * 9,
        out_specs=hbm,
        scratch_shapes=[
            pltpu.VMEM((2, depth, slots), F32),
            pltpu.VMEM((4, depth, slots), BF16),
            pltpu.VMEM((2 * cols, depth), F32),
            pltpu.VMEM((2, cols, depth), F32),
            pltpu.VMEM((2, plane, 2, cols, depth), F32),
            pltpu.VMEM((2,) + blocks, F32),
            pltpu.VMEM(blocks, F32),
            pltpu.VMEM(blocks, F32),
            pltpu.VMEM((4, 8, 2, slots), F32),
            pltpu.VMEM((2, plane, 2, slots), F32),
            pltpu.VMEM((2, rows, plane * slots), BF16),
            pltpu.VMEM((2, wide, plane * slots), BF16),
            pltpu.VMEM((rows, 2 * wide), F32),
            pltpu.VMEM((1, groups * slots), jnp.int32),
            pltpu.SMEM((groups,), jnp.int32),
            pltpu.VMEM((groups,) + potential.shape, F32),
            *[pltpu.VMEM(table.shape, table.dtype) for table in consts],
            pltpu.VMEM((2, 2 * wide, 2 * radix * box), BF16),
            pltpu.VMEM((rows, 2 * radix * box), F32),
            pltpu.VMEM((2, radix, 2 * window, radix * box), BF16),
            pltpu.VMEM((radix, 2 * window, radix * box), F32),
            pltpu.VMEM((2, rows, 2 * radix * box), BF16),
            pltpu.VMEM((rows, wide), F32),
            pltpu.VMEM((2, window, window * window), F32),
            dma((10,)),
            dma((3,)),
            dma((3,)),
            dma((4,)),
            dma((4,)),
            dma((2,)),
            dma((2,)),
            dma((2, 2)),
            dma((2, 2)),
            dma((2,)),
            dma((2, 4)),
            dma((2,)),
        ],
        compiler_params=pltpu.CompilerParams(
            collective_id=0, has_side_effects=True, vmem_limit_bytes=60 * 1024 * 1024
        ),
    )(coefficients, rot, potential, index_map[None], counts, *consts)


def kinetic_factors(box, window, radix):
    rows, cols = radix * window, window // radix * window
    half = window // 2
    row_at = lax.broadcasted_iota(jnp.int32, (rows, cols), 0)
    col_at = lax.broadcasted_iota(jnp.int32, (rows, cols), 1)
    n_x = (row_at % window - half).astype(F32)
    n_y = (col_at // window * radix + row_at // window - half).astype(F32)
    n_z = (col_at % window - half).astype(F32)
    return (8.0 / (box * box)) * (n_x * n_x + n_y * n_y + n_z * n_z)


def apply_kernel(
    box, window, radix, apart, pot_ready, grid_field, pot_ref, right_ref, left_ref, back_ref, twist_ref,
    field_ref, mixed_ref, unmixed_ref, turned_ref, kinetic_ref, out_ref, ship
):
    coarse = window // radix
    rows = radix * window
    cols = coarse * window
    wide = radix * box
    lanes = 128
    per = wide // pot_ref.shape[2]

    with jax.named_scope("fwd_right"):
        field_ref[...] = dot3(split_parts(grid_field), [right_ref[0], right_ref[1]])

    def mix(tile, carry):
        at = pl.ds(pl.multiple_of(tile * lanes, lanes), lanes)
        imag_at = pl.ds(pl.multiple_of(wide + tile * lanes, lanes), lanes)
        values = []
        for low in range(radix):
            real = field_ref[low * window : (low + 1) * window, at]
            imag = field_ref[low * window : (low + 1) * window, imag_at]
            cos, sin = twist_ref[0, low : low + 1, at], twist_ref[1, low : low + 1, at]
            values.append((real * cos - imag * sin, real * sin + imag * cos))
        for k, pair in enumerate(fft8(values, 1)):
            for c in range(2):
                high, low = split_parts(pair[c])
                mixed_ref[0, k, c * window : (c + 1) * window, at] = high
                mixed_ref[1, k, c * window : (c + 1) * window, at] = low
        return carry

    with jax.named_scope("mix"):
        lax.fori_loop(0, wide // lanes, mix, 0)
    with jax.named_scope("wait_pot"):
        pot_ready()

    with jax.named_scope("left"):
        @pl.when(apart)
        def _():
            for k in range(radix):
                for n in range(2):
                    at = slice(n * 2 * lanes, (n + 1) * 2 * lanes)
                    high, low = mixed_ref[0, k, :, at], mixed_ref[1, k, :, at]
                    space = jnp.dot(
                        left_ref[...], jnp.concatenate([high, high, low, low], axis=0), preferred_element_type=F32
                    )
                    pot = jnp.concatenate([pot_ref[k * per + 2 * n + i] for i in range(2)], axis=1)
                    high, low = split_parts(space * jnp.concatenate([pot, pot], axis=0))
                    both = jnp.dot(back_ref[...], jnp.concatenate([high, low], axis=0), preferred_element_type=F32)
                    unmixed_ref[k, :, at] = both[: 2 * window] + both[2 * window :]

    def unmix(tile, carry):
        at = pl.ds(pl.multiple_of(tile * lanes, lanes), lanes)
        imag_at = pl.ds(pl.multiple_of(wide + tile * lanes, lanes), lanes)
        values = [
            (unmixed_ref[k, :window, at], unmixed_ref[k, window:, at]) for k in range(radix)
        ]
        for low, (real, imag) in enumerate(fft8(values, -1)):
            cos, sin = twist_ref[0, low : low + 1, at], twist_ref[1, low : low + 1, at]
            turned = (real * cos + imag * sin, imag * cos - real * sin)
            for value, to in zip(turned, (at, imag_at)):
                for i, part in enumerate(split_parts(value)):
                    turned_ref[i, low * window : (low + 1) * window, to] = part
        return carry

    with jax.named_scope("unmix"):
        lax.fori_loop(0, wide // lanes, unmix, 0)
    with jax.named_scope("back_right"):
        applied = dot3([turned_ref[0], turned_ref[1]], [right_ref[0], right_ref[1]], ((1,), (1,)))

    kinetic = kinetic_ref[...]
    applied = applied + jnp.concatenate([kinetic, kinetic], axis=1) * grid_field
    for c in range(2):
        pieces = [
            applied[lo * window : (lo + 1) * window, c * cols + hi * window : c * cols + (hi + 1) * window]
            for hi in range(coarse)
            for lo in range(radix)
        ]
        out_ref[c] = jnp.concatenate(pieces, axis=1)
        ship(c)


def per_device(coefficients, rotation, potential, index_map, counts):
    box = potential.shape[0]
    window = box // 2
    radix = math.isqrt(box)
    assert radix * radix == box
    consts = [jnp.asarray(t) for t in tables(box, window, radix)]
    return run(coefficients, rotation, potential, index_map, counts, consts, box, window, radix)


def solution(mesh):
    placed = (P("band", None, "ga"), P(None, "band", "ga"), P(None, "ga"), P(), P())
    return jax.shard_map(
        per_device,
        mesh=mesh,
        in_specs=placed,
        out_specs=P(("band", "ga"), None, None, None),
        check_vma=False,
    )
```

```python
import functools
import math

import jax
import jax.numpy as jnp
import numpy as np
from jax import lax
from jax.experimental import pallas as pl
from jax.experimental.pallas import tpu as pltpu
from jax.sharding import PartitionSpec as P

F32 = jnp.float32
BF16 = jnp.bfloat16


def split_parts(values):
    high = values.astype(BF16)
    return high, (values - high.astype(F32)).astype(BF16)


def two_parts(table):
    high = table.astype(BF16)
    low = (table - high.astype(np.float32)).astype(BF16)
    return np.stack([high, low])


def tables(box, window, radix):
    half = window // 2
    coarse = window // radix
    k_all = np.arange(box)
    n_signed = np.arange(window) - half
    low = np.arange(radix)
    y_phase = (radix * np.arange(coarse) - half)[:, None] * low[None, :]
    z_phase = n_signed[:, None] * k_all[None, :]
    right = y_phase[:, None, :, None] + z_phase[None, :, None, :]
    right = right.reshape(coarse * window, radix * box) % box
    x_phase = k_all[:, None] * n_signed[None, :] % box
    twist = np.repeat(low[:, None] * low[None, :], box, axis=1) % box

    def pair(phase, scale=1.0):
        angle = phase * (2.0 * math.pi / box)
        return (np.stack([np.cos(angle), np.sin(angle)]) * scale).astype(np.float32)

    right_tab = two_parts(pair(right))
    cos, sin = pair(x_phase)
    left_high, left_low = two_parts(np.block([[cos, -sin], [sin, cos]]) / np.float32(box**3))
    left_tab = np.concatenate([left_high, left_low, left_high, left_low], axis=1)
    back_high, back_low = two_parts(np.block([[cos.T, sin.T], [-sin.T, cos.T]]))
    back_tab = np.block([[back_high, back_high], [back_low, back_low]])
    return right_tab, left_tab, back_tab, pair(twist)


def fft8(values, sign):
    root = math.sqrt(0.5)

    def add(a, b):
        return a[0] + b[0], a[1] + b[1]

    def sub(a, b):
        return a[0] - b[0], a[1] - b[1]

    def turn(a):
        return (-a[1], a[0]) if sign > 0 else (a[1], -a[0])

    def fft4(a, b, c, d):
        total, diff = add(a, c), sub(a, c)
        other, cross = add(b, d), turn(sub(b, d))
        return add(total, other), add(diff, cross), sub(total, other), sub(diff, cross)

    even = fft4(*values[0::2])
    odd = list(fft4(*values[1::2]))
    one, three = odd[1], odd[3]
    one_turn, three_turn = turn(one), turn(three)
    odd[1] = ((one[0] + one_turn[0]) * root, (one[1] + one_turn[1]) * root)
    odd[2] = turn(odd[2])
    odd[3] = ((three_turn[0] - three[0]) * root, (three_turn[1] - three[1]) * root)
    return [add(a, b) for a, b in zip(even, odd)] + [sub(a, b) for a, b in zip(even, odd)]


def dot3(lhs, rhs, dims=((1,), (0,))):
    def one(a, b):
        return lax.dot_general(a, b, (dims, ((), ())), preferred_element_type=F32)

    return one(lhs[0], rhs[0]) + (one(lhs[0], rhs[1]) + one(lhs[1], rhs[0]))


def block(cos, sin):
    upper = jnp.concatenate([cos, sin], axis=1)
    lower = jnp.concatenate([-sin, cos], axis=1)
    return jnp.concatenate([upper, lower], axis=0)


def whole_kernel(
    box, window, radix, coef_hbm, rot_hbm, pot_hbm, idx_hbm, cnt_hbm, right_hbm, left_hbm, back_hbm, twist_hbm,
    out_ref, coef, coef_parts, rot_raw, rot_own, rots, prod, drecv, zrecv, tout, land, onehot, hits, acc, idx, cnt,
    pot_out, right_tab, left_tab, back_tab, twist, right_blk, mixed, unmixed, kinetic, out_buf,
    load_sem, rot_send, rot_recv, pot_send, pot_recv, pair_send, pair_recv, line_send, line_recv, val_send, val_recv,
    out_sem
):
    band = lax.axis_index("band")
    me = lax.axis_index("ga")
    groups = 2 * rots.shape[1]
    plane = groups // 2
    lines = zrecv.shape[1]
    line, core = band // 2, lax.rem(band, 2)
    cell, side = me // 2, lax.rem(me, 2)
    across = cell * 2 + (1 - side)
    sibling = line * 2 + (1 - core)
    mirror = (lines - 1 - line) * 2 + core
    half_rows = pot_hbm.shape[0] // 2
    share = pl.ds(pl.multiple_of(core * half_rows, half_rows), half_rows)
    slots = coef.shape[2]

    def local(src, dst, i):
        copy = pltpu.make_async_copy(src, dst, load_sem.at[i])
        copy.start()
        return copy

    barrier = pltpu.get_barrier_semaphore()

    def greet(to_band, to):
        pl.semaphore_signal(
            barrier, inc=1, device_id={"band": to_band, "ga": to}, device_id_type=pl.DeviceIdType.MESH
        )

    def peers(act):
        def body(step, code):
            shift = lax.rem(code, 16)
            act(lax.rem(cell // 4 + shift // 4, 4) * 4 + lax.rem(cell + shift, 4))
            return code // 16

        lax.fori_loop(0, 8, body, jnp.int32(0x528E6B9A))
        lax.fori_loop(0, 7, body, jnp.int32(0xC431FD7))

    def lines_other(act):
        low = 1 - line // 2
        for step in range(lines):
            l = low * (lines - 1 - step) + (1 - low) * step

            @pl.when(l != line)
            def _(l=l):
                act(l)

    def remote(src, dst, send, recv, to_band, to):
        return pltpu.make_async_remote_copy(
            src_ref=src, dst_ref=dst, send_sem=send, recv_sem=recv,
            device_id={"band": to_band, "ga": to}, device_id_type=pl.DeviceIdType.MESH,
        )

    with jax.named_scope("barrier"):
        greet(band, across)
        greet(mirror, across)
        peers(lambda q: greet(band, q * 2 + side))
        lines_other(lambda l: greet(l * 2 + core, me))
        greet(sibling, me)

    rot_load = local(rot_hbm.at[0], rot_raw, 0)
    idx_load = local(idx_hbm, idx, 1)
    cnt_load = local(cnt_hbm, cnt, 2)
    coef_loads = [local(coef_hbm.at[:, c, :], coef.at[c], 3 + c) for c in range(2)]
    pot_load = local(pot_hbm, pot_out.at[me], 5)
    tab_loads = [
        local(src, dst, 6 + i)
        for i, (src, dst) in enumerate(
            ((right_hbm, right_tab), (left_hbm, left_tab), (back_hbm, back_tab), (twist_hbm, twist))
        )
    ]

    def split_coef():
        for c in range(2):
            coef_loads[c].wait()
            high, low = split_parts(coef[c])
            coef_parts[2 * c] = high
            coef_parts[2 * c + 1] = low
        rot_load.wait()
        for e in range(2):
            for c in range(2):
                for x in range(4):
                    rot_own[e, 4 * c + x] = rot_raw[8 * c + 2 * x + e]

    with jax.named_scope("barrier_wait"):
        split_coef()
        pl.semaphore_wait(barrier, plane - 1 + 3 + lines - 1)

    def rot_swap():
        return remote(rot_own, rots.at[side, cell], rot_send.at[0], rot_recv.at[0], band, across)

    def rot_copy(which, held, q):
        slot = rots.at[held, cell]
        src = rot_own if which == 1 else slot
        return remote(src, slot, rot_send.at[which], rot_recv.at[which], band, q * 2 + side)

    def rot_all(which):
        part = rots.at[0, pl.ds(0, plane - 1)]
        return remote(part, part, rot_send.at[which], rot_recv.at[which], band, across)

    def pot_swap():
        part = pot_out.at[me, share]
        return remote(part, part, pot_send.at[0], pot_recv.at[0], mirror, across)

    def pot_copy(which, piece, q):
        part = pot_out.at[piece, share]
        return remote(part, part, pot_send.at[which], pot_recv.at[which], band, q * 2 + side)

    def pot_all(which):
        part = pot_out.at[pl.ds(0, plane - 1), pl.ds(0, half_rows)]
        return remote(part, part, pot_send.at[which], pot_recv.at[which], band, across)

    def pot_pair():
        part = pot_out.at[:, share]
        return remote(part, part, pot_send.at[3], pot_recv.at[3], sibling, me)

    def pair_copy(step):
        return remote(prod.at[step, 0], drecv.at[step], pair_send.at[step], pair_recv.at[step], sibling, me)

    def line_copy(step, e, l):
        return remote(
            prod.at[step, 1, l, e], zrecv.at[step, line, e], line_send.at[step, e], line_recv.at[step, e],
            l * 2 + core, me,
        )

    def line_all(step, e):
        part = zrecv.at[step, pl.ds(0, lines - 1), 0]
        return remote(part, part, line_send.at[step, e], line_recv.at[step, e], sibling, me)

    def val_copy(step, turn, i, to_band, to):
        return remote(
            tout.at[turn, i], land.at[side, cell], val_send.at[step], val_recv.at[step, cell // 4], to_band, to
        )

    def val_all(step, batch, row, count):
        part = land.at[0, pl.ds(0, count)]
        return remote(part, part, val_send.at[step], val_recv.at[batch, row], band, across)

    with jax.named_scope("send_rot"):
        rot_swap().start()
        pot_load.wait()
        pot_swap().start()
        peers(lambda q: rot_copy(1, side, q).start())
        rots[side, cell] = rot_own[...]

    def mark(src, carry):
        at = pl.ds(pl.multiple_of(src * slots, slots), slots)
        to = pl.ds(pl.multiple_of(src // 2 * slots, slots), slots)
        half = window // 2
        cells = idx[:, at]
        cell_x = (cells // (box * box) + half) % box
        cell_y = (cells // box % box + half) % box
        cell_z = (cells % box + half) % box
        inside = (cell_x < window) & (cell_y < window) & (cell_z < window)
        live = lax.broadcasted_iota(jnp.int32, (1, slots), 1) < cnt[src]
        row_id = jnp.where(live & inside, cell_y % radix * window + cell_x, -1)
        col_id = cell_y // radix * window + cell_z
        rows, cols = onehot.shape[1], hits.shape[1]
        picks = lax.broadcasted_iota(jnp.int32, (rows, slots), 0) == row_id
        onehot[lax.rem(src, 2), :, to] = jnp.where(picks, 1.0, 0.0).astype(BF16)
        found = lax.broadcasted_iota(jnp.int32, (cols, slots), 0) == col_id
        hits[lax.rem(src, 2), :, to] = jnp.where(found, 1.0, 0.0).astype(BF16)
        return carry

    with jax.named_scope("mark0"):
        idx_load.wait()
        cnt_load.wait()
        lax.fori_loop(0, 4, mark, 0)

    with jax.named_scope("relay_rot"):
        rot_swap().wait_recv()
        pot_swap().wait_recv()
        peers(lambda q: rot_copy(2, 1 - side, q).start())
        lax.fori_loop(4, 8, mark, 0)

    def rotate(held, to_core):
        blocks = []
        for l in range(lines):
            for l_of, e in ((l, side), (lines - 1 - l, 1 - side)):
                for r in range(2):
                    blocks.append(rots[held, l_of * 4 + to_core * 2 + r, e])
        a = jnp.concatenate(blocks, axis=0)
        b = jnp.concatenate([piece for blk in blocks for piece in (-blk[4:], blk[:4])], axis=0)
        a_high, a_low = split_parts(a)
        b_high, b_low = split_parts(b)
        lhs = jnp.concatenate([a_high, a_low, a_high, b_high, b_low, b_high], axis=1)
        rhs = jnp.concatenate(
            [coef_parts[0], coef_parts[0], coef_parts[1], coef_parts[2], coef_parts[2], coef_parts[3]], axis=0
        )
        return jnp.dot(lhs, rhs, preferred_element_type=F32).reshape(lines, 2, 2, 8, slots)

    def first_half(step, carry):
        with jax.named_scope("wait_rot"):
            rot_all(1 + step).wait_recv()

        def part(i, carry):
            with jax.named_scope("rotate"):
                prod[step, i] = rotate(lax.rem(side + step, 2), lax.rem(core + 1 + i, 2))

            @pl.when(i == 0)
            def _():
                pair_copy(step).start()

            return carry

        lax.fori_loop(0, 2, part, 0)

        with jax.named_scope("pair"):
            pair_copy(step).wait_recv()
            prod[step, 1] = prod[step, 1] + drecv[step]
            for e in (1, 0):
                lines_other(lambda l: line_copy(step, e, l).start())

        @pl.when(step == 1)
        def _():
            with jax.named_scope("relay_pot"):
                peers(lambda q: pot_copy(1, me, q).start())
                peers(lambda q: pot_copy(2, across, q).start())

        return carry

    lax.fori_loop(0, 2, first_half, 0)
    with jax.named_scope("blocks"):
        for tab in tab_loads:
            tab.wait()
        for i in range(2):
            right_blk[i] = block(right_tab[i, 0], right_tab[i, 1])
        kinetic[...] = kinetic_factors(box, window, radix)

    early = lax.rem(me // 8, 2)
    mine_first = early == side
    acc[...] = jnp.zeros_like(acc)

    def row_part(batch, near):
        parity = lax.rem(early + batch, 2)
        row = lax.rem(cell // 4 + near + near // 2 - 2 * (near // 3), 4)
        alone = (parity == side) & (row == cell // 4)

        @pl.when(alone)
        def _():
            val_all(0, batch, row, 3).wait_recv()

        @pl.when(jnp.logical_not(alone))
        def _():
            val_all(0, batch, row, 4).wait_recv()

        return parity, row

    def row_sum(parity, row):
        deep = 4 * slots
        cols = hits.shape[1]
        placed = [[], []]
        for u in range(4):
            to = pl.ds(pl.multiple_of(row * deep + u * slots, slots), slots)
            mask = hits[parity, :, to]
            for n, part in enumerate(split_parts(land[parity, row * 4 + u])):
                part = part.astype(F32)
                pieces = []
                for c in range(2):
                    line_of = jnp.broadcast_to(part[c : c + 1, :], (16, slots)).astype(BF16)
                    pieces.append(mask * jnp.concatenate([line_of] * (cols // 16), axis=0))
                placed[n].append(jnp.concatenate(pieces, axis=0))
        picked = onehot[parity, :, pl.ds(pl.multiple_of(row * deep, deep), deep)]
        high, low = (
            lax.dot_general(
                picked, jnp.concatenate(part, axis=1), (((1,), (1,)), ((), ())), preferred_element_type=F32
            )
            for part in placed
        )
        return high + low

    def collect_pair(pair, carry):
        batch, near = pair // 2, 2 * lax.rem(pair, 2)
        first, second = row_part(batch, near), row_part(batch, near + 1)
        acc[...] += row_sum(*first) + row_sum(*second)
        return carry

    def collect(step, carry):
        acc[...] += row_sum(*row_part(step // 4, lax.rem(step, 4)))
        return carry

    def second_half(turn, carry):
        step, e = turn // 2, 1 - lax.rem(turn, 2)
        with jax.named_scope("mark1"):
            before = jnp.where(turn == 0, 8, jnp.where(turn == 1, 20, jnp.where(turn == 2, 30, groups)))
            lax.fori_loop(jnp.where(turn == 0, 8, jnp.where(turn == 1, 8, jnp.where(turn == 2, 20, 30))), before, mark, 0)
        @pl.when(turn == 3)
        def _():
            with jax.named_scope("collect0"):
                collect(0, 0)

        with jax.named_scope("wait_line"):
            line_all(step, e).wait_recv()
        with jax.named_scope("send_val"):
            total = prod[step, 1, line, e]
            for other in range(1, lines):
                total = total + zrecv[step, lax.rem(line + other, lines), e]
            for r in range(2):
                for c in range(2):
                    tout[turn, r * 4 : r * 4 + 4, c, :] = total[r, c * 4 : c * 4 + 4]

            def send(n, carry):
                r = lax.rem(cell // 8 + 1 + n // 4, 2)
                m = lax.rem(n, 4)
                x = lax.rem(cell + jnp.where(m == 0, 2, jnp.where(m == 1, 1, jnp.where(m == 2, 3, 0))), 4)
                to = (r * 8 + lax.rem(side + step, 2) * 4 + x) * 2 + lax.rem(side + e, 2)
                i = r * 4 + x

                @pl.when(to != me)
                def _():
                    val_copy(step, turn, i, (1 - e) * band + e * mirror, to).start()

                @pl.when(to == me)
                def _():
                    land[side, cell] = tout[turn, i]

                return carry

            lax.fori_loop(0, 8, send, 0)
        return carry

    lax.fori_loop(0, 4, second_half, 0)
    with jax.named_scope("pair_pot"):
        pot_all(1).wait_recv()
        pot_all(2).wait_recv()
        pot_pair().start()

    with jax.named_scope("collect"):
        lax.fori_loop(1, 4, collect, 0)
        lax.fori_loop(2, 4, collect_pair, 0)
    grid_field = acc[...]

    def pot_ready():
        pot_pair().wait_recv()

    def out_copy(c):
        return pltpu.make_async_copy(out_buf.at[c], out_ref.at[0, c], out_sem.at[c])

    apply_kernel(
        box, window, radix, band >= 0, pot_ready, grid_field, pot_out, right_blk, left_tab, back_tab, twist,
        mixed, unmixed, kinetic, out_buf, lambda c: out_copy(c).start()
    )
    with jax.named_scope("wait_sends"):
        for c in range(2):
            out_copy(c).wait()
        rot_swap().wait_send()
        rot_all(1).wait_send()
        rot_all(2).wait_send()
        pot_swap().wait_send()
        pot_all(1).wait_send()
        pot_all(2).wait_send()
        pot_pair().wait_send()
        for step in range(2):
            pair_copy(step).wait_send()
            for e in range(2):
                line_all(step, e).wait_send()
            alone = mine_first if step == 0 else jnp.logical_not(mine_first)

            @pl.when(alone)
            def _():
                val_all(step, 0, 0, plane - 1).wait_send()

            @pl.when(jnp.logical_not(alone))
            def _():
                val_all(step, 0, 0, plane).wait_send()


def run(coefficients, rotation, potential, index_map, counts, consts, box, window, radix):
    bands, groups = lax.axis_size("band"), lax.axis_size("ga")
    depth, _, slots = coefficients.shape
    cols = rotation.shape[2]
    assert (bands, groups, cols) == (8, 32, 8)
    lines, plane = bands // 2, groups // 2
    rot = rotation.transpose(0, 2, 1).reshape(1, 2 * cols, depth)
    hbm = pl.BlockSpec(memory_space=pl.ANY)
    dma = pltpu.SemaphoreType.DMA
    rows, wide = radix * window, window // radix * window
    blocks = (2, lines, 2, 2, 8, slots)
    return pl.pallas_call(
        functools.partial(whole_kernel, box, window, radix),
        out_shape=jax.ShapeDtypeStruct((1, 2, window, window * window), F32),
        in_specs=[hbm] * 9,
        out_specs=hbm,
        scratch_shapes=[
            pltpu.VMEM((2, depth, slots), F32),
            pltpu.VMEM((4, depth, slots), BF16),
            pltpu.VMEM((2 * cols, depth), F32),
            pltpu.VMEM((2, cols, depth), F32),
            pltpu.VMEM((2, plane, 2, cols, depth), F32),
            pltpu.VMEM((2,) + blocks, F32),
            pltpu.VMEM(blocks, F32),
            pltpu.VMEM(blocks, F32),
            pltpu.VMEM((4, 8, 2, slots), F32),
            pltpu.VMEM((2, plane, 2, slots), F32),
            pltpu.VMEM((2, rows, plane * slots), BF16),
            pltpu.VMEM((2, wide, plane * slots), BF16),
            pltpu.VMEM((rows, 2 * wide), F32),
            pltpu.VMEM((1, groups * slots), jnp.int32),
            pltpu.SMEM((groups,), jnp.int32),
            pltpu.VMEM((groups,) + potential.shape, F32),
            *[pltpu.VMEM(table.shape, table.dtype) for table in consts],
            pltpu.VMEM((2, 2 * wide, 2 * radix * box), BF16),
            pltpu.VMEM((2, radix, 2 * window, radix * box), BF16),
            pltpu.VMEM((radix, 2 * window, radix * box), F32),
            pltpu.VMEM((rows, wide), F32),
            pltpu.VMEM((2, window, window * window), F32),
            dma((10,)),
            dma((3,)),
            dma((3,)),
            dma((4,)),
            dma((4,)),
            dma((2,)),
            dma((2,)),
            dma((2, 2)),
            dma((2, 2)),
            dma((2,)),
            dma((2, 4)),
            dma((2,)),
        ],
        compiler_params=pltpu.CompilerParams(
            collective_id=0, has_side_effects=True, vmem_limit_bytes=60 * 1024 * 1024
        ),
    )(coefficients, rot, potential, index_map[None], counts, *consts)


def kinetic_factors(box, window, radix):
    rows, cols = radix * window, window // radix * window
    half = window // 2
    row_at = lax.broadcasted_iota(jnp.int32, (rows, cols), 0)
    col_at = lax.broadcasted_iota(jnp.int32, (rows, cols), 1)
    n_x = (row_at % window - half).astype(F32)
    n_y = (col_at // window * radix + row_at // window - half).astype(F32)
    n_z = (col_at % window - half).astype(F32)
    return (8.0 / (box * box)) * (n_x * n_x + n_y * n_y + n_z * n_z)


def apply_kernel(
    box, window, radix, apart, pot_ready, grid_field, pot_ref, right_ref, left_ref, back_ref, twist_ref,
    mixed_ref, unmixed_ref, kinetic_ref, out_ref, ship
):
    coarse = window // radix
    rows = radix * window
    cols = coarse * window
    wide = radix * box
    lanes = 128
    per = wide // pot_ref.shape[2]

    def columns(tile):
        return slice(tile * lanes, (tile + 1) * lanes), slice(wide + tile * lanes, wide + (tile + 1) * lanes)

    def right_of(tile):
        return [jnp.concatenate([right_ref[i, :, at] for at in columns(tile)], axis=1) for i in range(2)]

    def twist_of(low, at):
        return twist_ref[0, low : low + 1, at], twist_ref[1, low : low + 1, at]

    with jax.named_scope("fwd_mix"):
        parts = split_parts(grid_field)
        for tile in range(wide // lanes):
            at = columns(tile)[0]
            both = dot3(parts, right_of(tile))
            values = []
            for low in range(radix):
                real = both[low * window : (low + 1) * window, :lanes]
                imag = both[low * window : (low + 1) * window, lanes:]
                if low:
                    cos, sin = twist_of(low, at)
                    real, imag = real * cos - imag * sin, real * sin + imag * cos
                values.append((real, imag))
            for k, pair in enumerate(fft8(values, 1)):
                for c in range(2):
                    high, low = split_parts(pair[c])
                    mixed_ref[0, k, c * window : (c + 1) * window, at] = high
                    mixed_ref[1, k, c * window : (c + 1) * window, at] = low
    with jax.named_scope("wait_pot"):
        pot_ready()

    with jax.named_scope("left"):
        @pl.when(apart)
        def _():
            for k in range(radix):
                for n in range(2):
                    at = slice(n * 2 * lanes, (n + 1) * 2 * lanes)
                    high, low = mixed_ref[0, k, :, at], mixed_ref[1, k, :, at]
                    space = jnp.dot(
                        left_ref[...], jnp.concatenate([high, high, low, low], axis=0), preferred_element_type=F32
                    )
                    pot = jnp.concatenate([pot_ref[k * per + 2 * n + i] for i in range(2)], axis=1)
                    high, low = split_parts(space * jnp.concatenate([pot, pot], axis=0))
                    both = jnp.dot(back_ref[...], jnp.concatenate([high, low], axis=0), preferred_element_type=F32)
                    unmixed_ref[k, :, at] = both[: 2 * window] + both[2 * window :]

    def unmix(tile):
        at = columns(tile)[0]
        values = [(unmixed_ref[k, :window, at], unmixed_ref[k, window:, at]) for k in range(radix)]
        halves = [[], []]
        for low, (real, imag) in enumerate(fft8(values, -1)):
            if low:
                cos, sin = twist_of(low, at)
                real, imag = real * cos + imag * sin, imag * cos - real * sin
            split = [split_parts(real), split_parts(imag)]
            for i in range(2):
                halves[i].append(jnp.concatenate([split[0][i], split[1][i]], axis=1))
        turned = [jnp.concatenate(half, axis=0) for half in halves]
        return dot3(turned, right_of(tile), ((1,), (1,)))

    with jax.named_scope("unmix_back"):
        applied = unmix(0)
        for tile in range(1, wide // lanes):
            applied = applied + unmix(tile)

    kinetic = kinetic_ref[...]
    applied = applied + jnp.concatenate([kinetic, kinetic], axis=1) * grid_field
    for c in range(2):
        pieces = [
            applied[lo * window : (lo + 1) * window, c * cols + hi * window : c * cols + (hi + 1) * window]
            for hi in range(coarse)
            for lo in range(radix)
        ]
        out_ref[c] = jnp.concatenate(pieces, axis=1)
        ship(c)


def per_device(coefficients, rotation, potential, index_map, counts):
    box = potential.shape[0]
    window = box // 2
    radix = math.isqrt(box)
    assert radix * radix == box
    consts = [jnp.asarray(t) for t in tables(box, window, radix)]
    return run(coefficients, rotation, potential, index_map, counts, consts, box, window, radix)


def solution(mesh):
    placed = (P("band", None, "ga"), P(None, "band", "ga"), P(None, "ga"), P(), P())
    return jax.shard_map(
        per_device,
        mesh=mesh,
        in_specs=placed,
        out_specs=P(("band", "ga"), None, None, None),
        check_vma=False,
    )
```

```python
import functools
import math

import jax
import jax.numpy as jnp
import numpy as np
from jax import lax
from jax.experimental import pallas as pl
from jax.experimental.pallas import tpu as pltpu
from jax.sharding import PartitionSpec as P

F32 = jnp.float32
BF16 = jnp.bfloat16


def split_parts(values):
    high = values.astype(BF16)
    return high, (values - high.astype(F32)).astype(BF16)


def two_parts(table):
    high = table.astype(BF16)
    low = (table - high.astype(np.float32)).astype(BF16)
    return np.stack([high, low])


def tables(box, window, radix):
    half = window // 2
    coarse = window // radix
    k_all = np.arange(box)
    n_signed = np.arange(window) - half
    low = np.arange(radix)
    y_phase = (radix * np.arange(coarse) - half)[:, None] * low[None, :]
    z_phase = n_signed[:, None] * k_all[None, :]
    right = y_phase[:, None, :, None] + z_phase[None, :, None, :]
    right = right.reshape(coarse * window, radix * box) % box
    x_phase = k_all[:, None] * n_signed[None, :] % box
    twist = np.repeat(low[:, None] * low[None, :], box, axis=1) % box

    def pair(phase, scale=1.0):
        angle = phase * (2.0 * math.pi / box)
        return (np.stack([np.cos(angle), np.sin(angle)]) * scale).astype(np.float32)

    right_tab = two_parts(pair(right))
    cos, sin = pair(x_phase)
    left_high, left_low = two_parts(np.block([[cos, -sin], [sin, cos]]) / np.float32(box**3))
    left_tab = np.concatenate([left_high, left_low, left_high, left_low], axis=1)
    back_high, back_low = two_parts(np.block([[cos.T, sin.T], [-sin.T, cos.T]]))
    back_tab = np.block([[back_high, back_high], [back_low, back_low]])
    return right_tab, left_tab, back_tab, pair(twist)


def fft8(values, sign):
    root = math.sqrt(0.5)

    def add(a, b):
        return a[0] + b[0], a[1] + b[1]

    def sub(a, b):
        return a[0] - b[0], a[1] - b[1]

    def turn(a):
        return (-a[1], a[0]) if sign > 0 else (a[1], -a[0])

    def fft4(a, b, c, d):
        total, diff = add(a, c), sub(a, c)
        other, cross = add(b, d), turn(sub(b, d))
        return add(total, other), add(diff, cross), sub(total, other), sub(diff, cross)

    even = fft4(*values[0::2])
    odd = list(fft4(*values[1::2]))
    one, three = odd[1], odd[3]
    one_turn, three_turn = turn(one), turn(three)
    odd[1] = ((one[0] + one_turn[0]) * root, (one[1] + one_turn[1]) * root)
    odd[2] = turn(odd[2])
    odd[3] = ((three_turn[0] - three[0]) * root, (three_turn[1] - three[1]) * root)
    return [add(a, b) for a, b in zip(even, odd)] + [sub(a, b) for a, b in zip(even, odd)]


def dot3(lhs, rhs, dims=((1,), (0,))):
    def one(a, b):
        return lax.dot_general(a, b, (dims, ((), ())), preferred_element_type=F32)

    return one(lhs[0], rhs[0]) + (one(lhs[0], rhs[1]) + one(lhs[1], rhs[0]))


def block(cos, sin):
    upper = jnp.concatenate([cos, sin], axis=1)
    lower = jnp.concatenate([-sin, cos], axis=1)
    return jnp.concatenate([upper, lower], axis=0)


def whole_kernel(
    box, window, radix, coef_hbm, rot_hbm, pot_hbm, idx_hbm, cnt_hbm, right_hbm, left_hbm, back_hbm, twist_hbm,
    out_ref, coef, coef_parts, rot_raw, rot_own, rots, prod, drecv, zrecv, tout, land, onehot, hits, acc, idx, cnt,
    pot_out, right_tab, left_tab, back_tab, twist, right_blk, mixed, unmixed, kinetic, out_buf,
    load_sem, rot_send, rot_recv, pot_send, pot_recv, pair_send, pair_recv, line_send, line_recv, val_send, val_recv,
    out_sem
):
    band = lax.axis_index("band")
    me = lax.axis_index("ga")
    groups = 2 * rots.shape[1]
    plane = groups // 2
    lines = zrecv.shape[1]
    line, core = band // 2, lax.rem(band, 2)
    cell, side = me // 2, lax.rem(me, 2)
    across = cell * 2 + (1 - side)
    sibling = line * 2 + (1 - core)
    mirror = (lines - 1 - line) * 2 + core
    half_rows = pot_hbm.shape[0] // 2
    share = pl.ds(pl.multiple_of(core * half_rows, half_rows), half_rows)
    slots = coef.shape[2]

    def local(src, dst, i):
        copy = pltpu.make_async_copy(src, dst, load_sem.at[i])
        copy.start()
        return copy

    barrier = pltpu.get_barrier_semaphore()

    def greet(to_band, to):
        pl.semaphore_signal(
            barrier, inc=1, device_id={"band": to_band, "ga": to}, device_id_type=pl.DeviceIdType.MESH
        )

    def peers(act):
        def body(step, code):
            shift = lax.rem(code, 16)
            act(lax.rem(cell // 4 + shift // 4, 4) * 4 + lax.rem(cell + shift, 4))
            return code // 16

        lax.fori_loop(0, 8, body, jnp.int32(0x528E6B9A))
        lax.fori_loop(0, 7, body, jnp.int32(0xC431FD7))

    def lines_other(act):
        for step in range(lines):
            l = side * (lines - 1 - step) + (1 - side) * step

            @pl.when(l != line)
            def _(l=l):
                act(l)

    def remote(src, dst, send, recv, to_band, to):
        return pltpu.make_async_remote_copy(
            src_ref=src, dst_ref=dst, send_sem=send, recv_sem=recv,
            device_id={"band": to_band, "ga": to}, device_id_type=pl.DeviceIdType.MESH,
        )

    with jax.named_scope("barrier"):
        greet(band, across)
        greet(mirror, across)
        peers(lambda q: greet(band, q * 2 + side))
        lines_other(lambda l: greet(l * 2 + core, me))
        greet(sibling, me)

    rot_load = local(rot_hbm.at[0], rot_raw, 0)
    idx_load = local(idx_hbm, idx, 1)
    cnt_load = local(cnt_hbm, cnt, 2)
    coef_loads = [local(coef_hbm.at[:, c, :], coef.at[c], 3 + c) for c in range(2)]
    pot_load = local(pot_hbm, pot_out.at[me], 5)
    tab_loads = [
        local(src, dst, 6 + i)
        for i, (src, dst) in enumerate(
            ((right_hbm, right_tab), (left_hbm, left_tab), (back_hbm, back_tab), (twist_hbm, twist))
        )
    ]

    def split_coef():
        for c in range(2):
            coef_loads[c].wait()
            high, low = split_parts(coef[c])
            coef_parts[2 * c] = high
            coef_parts[2 * c + 1] = low
        rot_load.wait()
        for e in range(2):
            for c in range(2):
                for x in range(4):
                    rot_own[e, 4 * c + x] = rot_raw[8 * c + 2 * x + e]

    with jax.named_scope("barrier_wait"):
        split_coef()
        pl.semaphore_wait(barrier, plane - 1 + 3 + lines - 1)

    def rot_swap():
        return remote(rot_own, rots.at[side, cell], rot_send.at[0], rot_recv.at[0], band, across)

    def rot_copy(which, held, q):
        slot = rots.at[held, cell]
        src = rot_own if which == 1 else slot
        return remote(src, slot, rot_send.at[which], rot_recv.at[which], band, q * 2 + side)

    def rot_all(which):
        part = rots.at[0, pl.ds(0, plane - 1)]
        return remote(part, part, rot_send.at[which], rot_recv.at[which], band, across)

    def pot_swap():
        part = pot_out.at[me, share]
        return remote(part, part, pot_send.at[0], pot_recv.at[0], mirror, across)

    def pot_copy(which, piece, q):
        part = pot_out.at[piece, share]
        return remote(part, part, pot_send.at[which], pot_recv.at[which], band, q * 2 + side)

    def pot_all(which):
        part = pot_out.at[pl.ds(0, plane - 1), pl.ds(0, half_rows)]
        return remote(part, part, pot_send.at[which], pot_recv.at[which], band, across)

    def pot_pair():
        part = pot_out.at[:, share]
        return remote(part, part, pot_send.at[3], pot_recv.at[3], sibling, me)

    def pair_copy(step):
        return remote(prod.at[step, 0], drecv.at[step], pair_send.at[step], pair_recv.at[step], sibling, me)

    def line_copy(step, e, l):
        return remote(
            prod.at[step, 1, l, e], zrecv.at[step, line, e], line_send.at[step, e], line_recv.at[step, e],
            l * 2 + core, me,
        )

    def line_all(step, e):
        part = zrecv.at[step, pl.ds(0, lines - 1), 0]
        return remote(part, part, line_send.at[step, e], line_recv.at[step, e], sibling, me)

    def val_copy(step, turn, i, to_band, to):
        return remote(
            tout.at[turn, i], land.at[side, cell], val_send.at[step], val_recv.at[step, cell // 4], to_band, to
        )

    def val_all(step, batch, row, count):
        part = land.at[0, pl.ds(0, count)]
        return remote(part, part, val_send.at[step], val_recv.at[batch, row], band, across)

    with jax.named_scope("send_rot"):
        rot_swap().start()
        pot_load.wait()
        pot_swap().start()
        peers(lambda q: rot_copy(1, side, q).start())
        rots[side, cell] = rot_own[...]

    def mark(src, carry):
        at = pl.ds(pl.multiple_of(src * slots, slots), slots)
        to = pl.ds(pl.multiple_of(src // 2 * slots, slots), slots)
        half = window // 2
        cells = idx[:, at]
        cell_x = (cells // (box * box) + half) % box
        cell_y = (cells // box % box + half) % box
        cell_z = (cells % box + half) % box
        inside = (cell_x < window) & (cell_y < window) & (cell_z < window)
        live = lax.broadcasted_iota(jnp.int32, (1, slots), 1) < cnt[src]
        row_id = jnp.where(live & inside, cell_y % radix * window + cell_x, -1)
        col_id = cell_y // radix * window + cell_z
        rows, cols = onehot.shape[1], hits.shape[1]
        picks = lax.broadcasted_iota(jnp.int32, (rows, slots), 0) == row_id
        onehot[lax.rem(src, 2), :, to] = jnp.where(picks, 1.0, 0.0).astype(BF16)
        found = lax.broadcasted_iota(jnp.int32, (cols, slots), 0) == col_id
        hits[lax.rem(src, 2), :, to] = jnp.where(found, 1.0, 0.0).astype(BF16)
        return carry

    with jax.named_scope("mark0"):
        idx_load.wait()
        cnt_load.wait()
        lax.fori_loop(0, 4, mark, 0)

    with jax.named_scope("relay_rot"):
        rot_swap().wait_recv()
        pot_swap().wait_recv()
        peers(lambda q: rot_copy(2, 1 - side, q).start())
        lax.fori_loop(4, 8, mark, 0)

    def rotate(held, to_core):
        blocks = []
        for l in range(lines):
            for l_of, e in ((l, side), (lines - 1 - l, 1 - side)):
                for r in range(2):
                    blocks.append(rots[held, l_of * 4 + to_core * 2 + r, e])
        a = jnp.concatenate(blocks, axis=0)
        b = jnp.concatenate([piece for blk in blocks for piece in (-blk[4:], blk[:4])], axis=0)
        a_high, a_low = split_parts(a)
        b_high, b_low = split_parts(b)
        lhs = jnp.concatenate([a_high, a_low, a_high, b_high, b_low, b_high], axis=1)
        rhs = jnp.concatenate(
            [coef_parts[0], coef_parts[0], coef_parts[1], coef_parts[2], coef_parts[2], coef_parts[3]], axis=0
        )
        return jnp.dot(lhs, rhs, preferred_element_type=F32).reshape(lines, 2, 2, 8, slots)

    def first_half(step, carry):
        with jax.named_scope("wait_rot"):
            rot_all(1 + step).wait_recv()

        def part(i, carry):
            with jax.named_scope("rotate"):
                prod[step, i] = rotate(lax.rem(side + step, 2), lax.rem(core + 1 + i, 2))

            @pl.when(i == 0)
            def _():
                pair_copy(step).start()

            return carry

        lax.fori_loop(0, 2, part, 0)

        with jax.named_scope("pair"):
            pair_copy(step).wait_recv()
            prod[step, 1] = prod[step, 1] + drecv[step]
            for e in (side, 1 - side):
                lines_other(lambda l: line_copy(step, e, l).start())

        @pl.when(step == 1)
        def _():
            with jax.named_scope("relay_pot"):
                peers(lambda q: pot_copy(1, me, q).start())
                peers(lambda q: pot_copy(2, across, q).start())

        return carry

    lax.fori_loop(0, 2, first_half, 0)
    with jax.named_scope("blocks"):
        for tab in tab_loads:
            tab.wait()
        for i in range(2):
            right_blk[i] = block(right_tab[i, 0], right_tab[i, 1])
        kinetic[...] = kinetic_factors(box, window, radix)

    early = lax.rem(me // 8, 2)
    mine_first = early == side
    acc[...] = jnp.zeros_like(acc)

    def row_part(batch, near):
        parity = lax.rem(early + batch, 2)
        row = lax.rem(cell // 4 + near + near // 2 - 2 * (near // 3), 4)
        alone = (parity == side) & (row == cell // 4)

        @pl.when(alone)
        def _():
            val_all(0, batch, row, 3).wait_recv()

        @pl.when(jnp.logical_not(alone))
        def _():
            val_all(0, batch, row, 4).wait_recv()

        return parity, row

    def row_sum(parity, row):
        deep = 4 * slots
        cols = hits.shape[1]
        placed = [[], []]
        for u in range(4):
            to = pl.ds(pl.multiple_of(row * deep + u * slots, slots), slots)
            mask = hits[parity, :, to]
            for n, part in enumerate(split_parts(land[parity, row * 4 + u])):
                part = part.astype(F32)
                pieces = []
                for c in range(2):
                    line_of = jnp.broadcast_to(part[c : c + 1, :], (16, slots)).astype(BF16)
                    pieces.append(mask * jnp.concatenate([line_of] * (cols // 16), axis=0))
                placed[n].append(jnp.concatenate(pieces, axis=0))
        picked = onehot[parity, :, pl.ds(pl.multiple_of(row * deep, deep), deep)]
        high, low = (
            lax.dot_general(
                picked, jnp.concatenate(part, axis=1), (((1,), (1,)), ((), ())), preferred_element_type=F32
            )
            for part in placed
        )
        return high + low

    def collect_pair(pair, carry):
        batch, near = pair // 2, 2 * lax.rem(pair, 2)
        first, second = row_part(batch, near), row_part(batch, near + 1)
        acc[...] += row_sum(*first) + row_sum(*second)
        return carry

    def collect(step, carry):
        acc[...] += row_sum(*row_part(step // 4, lax.rem(step, 4)))
        return carry

    def second_half(turn, carry):
        step, e = turn // 2, lax.rem(side + turn, 2)
        with jax.named_scope("mark1"):
            before = jnp.where(turn == 0, 8, jnp.where(turn == 1, 20, jnp.where(turn == 2, 30, groups)))
            lax.fori_loop(jnp.where(turn == 0, 8, jnp.where(turn == 1, 8, jnp.where(turn == 2, 20, 30))), before, mark, 0)
        @pl.when(turn == 3)
        def _():
            with jax.named_scope("collect0"):
                lax.fori_loop(0, 2 - side, collect, 0)

        with jax.named_scope("wait_line"):
            line_all(step, e).wait_recv()
        with jax.named_scope("send_val"):
            total = prod[step, 1, line, e]
            for other in range(1, lines):
                total = total + zrecv[step, lax.rem(line + other, lines), e]
            for r in range(2):
                for c in range(2):
                    tout[turn, r * 4 : r * 4 + 4, c, :] = total[r, c * 4 : c * 4 + 4]

            def send(n, carry):
                r = lax.rem(cell // 8 + 1 + n // 4, 2)
                m = lax.rem(n, 4)
                x = lax.rem(cell + jnp.where(m == 0, 2, jnp.where(m == 1, 1, jnp.where(m == 2, 3, 0))), 4)
                to = (r * 8 + lax.rem(side + step, 2) * 4 + x) * 2 + lax.rem(side + e, 2)
                i = r * 4 + x

                @pl.when(to != me)
                def _():
                    val_copy(step, turn, i, (1 - e) * band + e * mirror, to).start()

                @pl.when(to == me)
                def _():
                    land[side, cell] = tout[turn, i]

                return carry

            lax.fori_loop(0, 8, send, 0)
        return carry

    lax.fori_loop(0, 4, second_half, 0)
    with jax.named_scope("pair_pot"):
        pot_all(1).wait_recv()
        pot_all(2).wait_recv()
        pot_pair().start()

    with jax.named_scope("collect"):
        lax.fori_loop(2 - side, 4, collect, 0)
        lax.fori_loop(2, 4, collect_pair, 0)
    grid_field = acc[...]

    def pot_ready():
        pot_pair().wait_recv()

    def out_copy(c):
        return pltpu.make_async_copy(out_buf.at[c], out_ref.at[0, c], out_sem.at[c])

    apply_kernel(
        box, window, radix, band >= 0, pot_ready, grid_field, pot_out, right_blk, left_tab, back_tab, twist,
        mixed, unmixed, kinetic, out_buf, lambda c: out_copy(c).start()
    )
    with jax.named_scope("wait_sends"):
        for c in range(2):
            out_copy(c).wait()
        rot_swap().wait_send()
        rot_all(1).wait_send()
        rot_all(2).wait_send()
        pot_swap().wait_send()
        pot_all(1).wait_send()
        pot_all(2).wait_send()
        pot_pair().wait_send()
        for step in range(2):
            pair_copy(step).wait_send()
            for e in range(2):
                line_all(step, e).wait_send()
            alone = mine_first if step == 0 else jnp.logical_not(mine_first)

            @pl.when(alone)
            def _():
                val_all(step, 0, 0, plane - 1).wait_send()

            @pl.when(jnp.logical_not(alone))
            def _():
                val_all(step, 0, 0, plane).wait_send()


def run(coefficients, rotation, potential, index_map, counts, consts, box, window, radix):
    bands, groups = lax.axis_size("band"), lax.axis_size("ga")
    depth, _, slots = coefficients.shape
    cols = rotation.shape[2]
    assert (bands, groups, cols) == (8, 32, 8)
    lines, plane = bands // 2, groups // 2
    rot = rotation.transpose(0, 2, 1).reshape(1, 2 * cols, depth)
    hbm = pl.BlockSpec(memory_space=pl.ANY)
    dma = pltpu.SemaphoreType.DMA
    rows, wide = radix * window, window // radix * window
    blocks = (2, lines, 2, 2, 8, slots)
    return pl.pallas_call(
        functools.partial(whole_kernel, box, window, radix),
        out_shape=jax.ShapeDtypeStruct((1, 2, window, window * window), F32),
        in_specs=[hbm] * 9,
        out_specs=hbm,
        scratch_shapes=[
            pltpu.VMEM((2, depth, slots), F32),
            pltpu.VMEM((4, depth, slots), BF16),
            pltpu.VMEM((2 * cols, depth), F32),
            pltpu.VMEM((2, cols, depth), F32),
            pltpu.VMEM((2, plane, 2, cols, depth), F32),
            pltpu.VMEM((2,) + blocks, F32),
            pltpu.VMEM(blocks, F32),
            pltpu.VMEM(blocks, F32),
            pltpu.VMEM((4, 8, 2, slots), F32),
            pltpu.VMEM((2, plane, 2, slots), F32),
            pltpu.VMEM((2, rows, plane * slots), BF16),
            pltpu.VMEM((2, wide, plane * slots), BF16),
            pltpu.VMEM((rows, 2 * wide), F32),
            pltpu.VMEM((1, groups * slots), jnp.int32),
            pltpu.SMEM((groups,), jnp.int32),
            pltpu.VMEM((groups,) + potential.shape, F32),
            *[pltpu.VMEM(table.shape, table.dtype) for table in consts],
            pltpu.VMEM((2, 2 * wide, 2 * radix * box), BF16),
            pltpu.VMEM((2, radix, 2 * window, radix * box), BF16),
            pltpu.VMEM((radix, 2 * window, radix * box), F32),
            pltpu.VMEM((rows, wide), F32),
            pltpu.VMEM((2, window, window * window), F32),
            dma((10,)),
            dma((3,)),
            dma((3,)),
            dma((4,)),
            dma((4,)),
            dma((2,)),
            dma((2,)),
            dma((2, 2)),
            dma((2, 2)),
            dma((2,)),
            dma((2, 4)),
            dma((2,)),
        ],
        compiler_params=pltpu.CompilerParams(
            collective_id=0, has_side_effects=True, vmem_limit_bytes=60 * 1024 * 1024
        ),
    )(coefficients, rot, potential, index_map[None], counts, *consts)


def kinetic_factors(box, window, radix):
    rows, cols = radix * window, window // radix * window
    half = window // 2
    row_at = lax.broadcasted_iota(jnp.int32, (rows, cols), 0)
    col_at = lax.broadcasted_iota(jnp.int32, (rows, cols), 1)
    n_x = (row_at % window - half).astype(F32)
    n_y = (col_at // window * radix + row_at // window - half).astype(F32)
    n_z = (col_at % window - half).astype(F32)
    return (8.0 / (box * box)) * (n_x * n_x + n_y * n_y + n_z * n_z)


def apply_kernel(
    box, window, radix, apart, pot_ready, grid_field, pot_ref, right_ref, left_ref, back_ref, twist_ref,
    mixed_ref, unmixed_ref, kinetic_ref, out_ref, ship
):
    coarse = window // radix
    rows = radix * window
    cols = coarse * window
    wide = radix * box
    lanes = 128
    per = wide // pot_ref.shape[2]

    def columns(tile):
        return slice(tile * lanes, (tile + 1) * lanes), slice(wide + tile * lanes, wide + (tile + 1) * lanes)

    def right_of(tile):
        return [jnp.concatenate([right_ref[i, :, at] for at in columns(tile)], axis=1) for i in range(2)]

    def twist_of(low, at):
        return twist_ref[0, low : low + 1, at], twist_ref[1, low : low + 1, at]

    with jax.named_scope("fwd_mix"):
        parts = split_parts(grid_field)
        for tile in range(wide // lanes):
            at = columns(tile)[0]
            both = dot3(parts, right_of(tile))
            values = []
            for low in range(radix):
                real = both[low * window : (low + 1) * window, :lanes]
                imag = both[low * window : (low + 1) * window, lanes:]
                if low:
                    cos, sin = twist_of(low, at)
                    real, imag = real * cos - imag * sin, real * sin + imag * cos
                values.append((real, imag))
            for k, pair in enumerate(fft8(values, 1)):
                for c in range(2):
                    high, low = split_parts(pair[c])
                    mixed_ref[0, k, c * window : (c + 1) * window, at] = high
                    mixed_ref[1, k, c * window : (c + 1) * window, at] = low
    with jax.named_scope("wait_pot"):
        pot_ready()

    with jax.named_scope("left"):
        @pl.when(apart)
        def _():
            for k in range(radix):
                for n in range(2):
                    at = slice(n * 2 * lanes, (n + 1) * 2 * lanes)
                    high, low = mixed_ref[0, k, :, at], mixed_ref[1, k, :, at]
                    space = jnp.dot(
                        left_ref[...], jnp.concatenate([high, high, low, low], axis=0), preferred_element_type=F32
                    )
                    pot = jnp.concatenate([pot_ref[k * per + 2 * n + i] for i in range(2)], axis=1)
                    high, low = split_parts(space * jnp.concatenate([pot, pot], axis=0))
                    both = jnp.dot(back_ref[...], jnp.concatenate([high, low], axis=0), preferred_element_type=F32)
                    unmixed_ref[k, :, at] = both[: 2 * window] + both[2 * window :]

    def unmix(tile):
        at = columns(tile)[0]
        values = [(unmixed_ref[k, :window, at], unmixed_ref[k, window:, at]) for k in range(radix)]
        halves = [[], []]
        for low, (real, imag) in enumerate(fft8(values, -1)):
            if low:
                cos, sin = twist_of(low, at)
                real, imag = real * cos + imag * sin, imag * cos - real * sin
            split = [split_parts(real), split_parts(imag)]
            for i in range(2):
                halves[i].append(jnp.concatenate([split[0][i], split[1][i]], axis=1))
        turned = [jnp.concatenate(half, axis=0) for half in halves]
        return dot3(turned, right_of(tile), ((1,), (1,)))

    with jax.named_scope("unmix_back"):
        applied = unmix(0)
        for tile in range(1, wide // lanes):
            applied = applied + unmix(tile)

    kinetic = kinetic_ref[...]
    applied = applied + jnp.concatenate([kinetic, kinetic], axis=1) * grid_field
    for c in range(2):
        pieces = [
            applied[lo * window : (lo + 1) * window, c * cols + hi * window : c * cols + (hi + 1) * window]
            for hi in range(coarse)
            for lo in range(radix)
        ]
        out_ref[c] = jnp.concatenate(pieces, axis=1)
        ship(c)


def per_device(coefficients, rotation, potential, index_map, counts):
    box = potential.shape[0]
    window = box // 2
    radix = math.isqrt(box)
    assert radix * radix == box
    consts = [jnp.asarray(t) for t in tables(box, window, radix)]
    return run(coefficients, rotation, potential, index_map, counts, consts, box, window, radix)


def solution(mesh):
    placed = (P("band", None, "ga"), P(None, "band", "ga"), P(None, "ga"), P(), P())
    return jax.shard_map(
        per_device,
        mesh=mesh,
        in_specs=placed,
        out_specs=P(("band", "ga"), None, None, None),
        check_vma=False,
    )
```

```python
import functools
import math

import jax
import jax.numpy as jnp
import numpy as np
from jax import lax
from jax.experimental import pallas as pl
from jax.experimental.pallas import tpu as pltpu
from jax.sharding import PartitionSpec as P

F32 = jnp.float32
BF16 = jnp.bfloat16


def split_parts(values):
    high = values.astype(BF16)
    return high, (values - high.astype(F32)).astype(BF16)


def two_parts(table):
    high = table.astype(BF16)
    low = (table - high.astype(np.float32)).astype(BF16)
    return np.stack([high, low])


def tables(box, window, radix):
    half = window // 2
    coarse = window // radix
    k_all = np.arange(box)
    n_signed = np.arange(window) - half
    low = np.arange(radix)
    y_phase = (radix * np.arange(coarse) - half)[:, None] * low[None, :]
    z_phase = n_signed[:, None] * k_all[None, :]
    right = y_phase[:, None, :, None] + z_phase[None, :, None, :]
    right = right.reshape(coarse * window, radix * box) % box
    x_phase = k_all[:, None] * n_signed[None, :] % box
    twist = np.repeat(low[:, None] * low[None, :], box, axis=1) % box

    def pair(phase, scale=1.0):
        angle = phase * (2.0 * math.pi / box)
        return (np.stack([np.cos(angle), np.sin(angle)]) * scale).astype(np.float32)

    right_tab = two_parts(pair(right))
    cos, sin = pair(x_phase)
    left_high, left_low = two_parts(np.block([[cos, -sin], [sin, cos]]) / np.float32(box**3))
    left_tab = np.concatenate([left_high, left_low, left_high, left_low], axis=1)
    back_high, back_low = two_parts(np.block([[cos.T, sin.T], [-sin.T, cos.T]]))
    back_tab = np.block([[back_high, back_high], [back_low, back_low]])
    return right_tab, left_tab, back_tab, pair(twist)


def fft8(values, sign):
    root = math.sqrt(0.5)

    def add(a, b):
        return a[0] + b[0], a[1] + b[1]

    def sub(a, b):
        return a[0] - b[0], a[1] - b[1]

    def turn(a):
        return (-a[1], a[0]) if sign > 0 else (a[1], -a[0])

    def fft4(a, b, c, d):
        total, diff = add(a, c), sub(a, c)
        other, cross = add(b, d), turn(sub(b, d))
        return add(total, other), add(diff, cross), sub(total, other), sub(diff, cross)

    even = fft4(*values[0::2])
    odd = list(fft4(*values[1::2]))
    one, three = odd[1], odd[3]
    one_turn, three_turn = turn(one), turn(three)
    odd[1] = ((one[0] + one_turn[0]) * root, (one[1] + one_turn[1]) * root)
    odd[2] = turn(odd[2])
    odd[3] = ((three_turn[0] - three[0]) * root, (three_turn[1] - three[1]) * root)
    return [add(a, b) for a, b in zip(even, odd)] + [sub(a, b) for a, b in zip(even, odd)]


def dot3(lhs, rhs, dims=((1,), (0,))):
    def one(a, b):
        return lax.dot_general(a, b, (dims, ((), ())), preferred_element_type=F32)

    return one(lhs[0], rhs[0]) + (one(lhs[0], rhs[1]) + one(lhs[1], rhs[0]))


def block(cos, sin):
    upper = jnp.concatenate([cos, sin], axis=1)
    lower = jnp.concatenate([-sin, cos], axis=1)
    return jnp.concatenate([upper, lower], axis=0)


def whole_kernel(
    box, window, radix, coef_hbm, rot_hbm, pot_hbm, idx_hbm, cnt_hbm, right_hbm, left_hbm, back_hbm, twist_hbm,
    out_ref, coef, coef_parts, rot_raw, rot_own, rots, prod, drecv, zrecv, tout, land, onehot, hits, acc, idx, cnt,
    pot_out, right_tab, left_tab, back_tab, twist, right_blk, mixed, unmixed, kinetic, out_buf,
    load_sem, rot_send, rot_recv, pot_send, pot_recv, pair_send, pair_recv, line_send, line_recv, val_send, val_recv,
    out_sem
):
    band = lax.axis_index("band")
    me = lax.axis_index("ga")
    groups = 2 * rots.shape[1]
    plane = groups // 2
    lines = zrecv.shape[1]
    line, core = band // 2, lax.rem(band, 2)
    cell, side = me // 2, lax.rem(me, 2)
    across = cell * 2 + (1 - side)
    sibling = line * 2 + (1 - core)
    mirror = (lines - 1 - line) * 2 + core
    half_rows = pot_hbm.shape[0] // 2
    share = pl.ds(pl.multiple_of(core * half_rows, half_rows), half_rows)
    slots = coef.shape[2]

    def local(src, dst, i):
        copy = pltpu.make_async_copy(src, dst, load_sem.at[i])
        copy.start()
        return copy

    barrier = pltpu.get_barrier_semaphore()

    def greet(to_band, to):
        pl.semaphore_signal(
            barrier, inc=1, device_id={"band": to_band, "ga": to}, device_id_type=pl.DeviceIdType.MESH
        )

    def peers(act):
        def body(step, code):
            shift = lax.rem(code, 16)
            act(lax.rem(cell // 4 + shift // 4, 4) * 4 + lax.rem(cell + shift, 4))
            return code // 16

        lax.fori_loop(0, 8, body, jnp.int32(0x528E6B9A))
        lax.fori_loop(0, 7, body, jnp.int32(0xC431FD7))

    def lines_other(act):
        for step in range(lines):
            l = side * (lines - 1 - step) + (1 - side) * step

            @pl.when(l != line)
            def _(l=l):
                act(l)

    def remote(src, dst, send, recv, to_band, to):
        return pltpu.make_async_remote_copy(
            src_ref=src, dst_ref=dst, send_sem=send, recv_sem=recv,
            device_id={"band": to_band, "ga": to}, device_id_type=pl.DeviceIdType.MESH,
        )

    with jax.named_scope("barrier"):
        greet(band, across)
        greet(mirror, across)
        peers(lambda q: greet(band, q * 2 + side))
        lines_other(lambda l: greet(l * 2 + core, me))
        greet(sibling, me)

    rot_load = local(rot_hbm.at[0], rot_raw, 0)
    idx_load = local(idx_hbm, idx, 1)
    cnt_load = local(cnt_hbm, cnt, 2)
    coef_loads = [local(coef_hbm.at[:, c, :], coef.at[c], 3 + c) for c in range(2)]
    pot_load = local(pot_hbm, pot_out.at[me], 5)
    tab_loads = [
        local(src, dst, 6 + i)
        for i, (src, dst) in enumerate(
            ((right_hbm, right_tab), (left_hbm, left_tab), (back_hbm, back_tab), (twist_hbm, twist))
        )
    ]

    def split_coef():
        for c in range(2):
            coef_loads[c].wait()
            high, low = split_parts(coef[c])
            coef_parts[2 * c] = high
            coef_parts[2 * c + 1] = low
        rot_load.wait()
        for e in range(2):
            for c in range(2):
                for x in range(4):
                    rot_own[e, 4 * c + x] = rot_raw[8 * c + 2 * x + e]

    with jax.named_scope("barrier_wait"):
        split_coef()
        pl.semaphore_wait(barrier, plane - 1 + 3 + lines - 1)

    def rot_swap():
        return remote(rot_own, rots.at[side, cell], rot_send.at[0], rot_recv.at[0], band, across)

    def rot_copy(which, held, q):
        slot = rots.at[held, cell]
        src = rot_own if which == 1 else slot
        return remote(src, slot, rot_send.at[which], rot_recv.at[which], band, q * 2 + side)

    def rot_all(which):
        part = rots.at[0, pl.ds(0, plane - 1)]
        return remote(part, part, rot_send.at[which], rot_recv.at[which], band, across)

    def pot_swap():
        part = pot_out.at[me, share]
        return remote(part, part, pot_send.at[0], pot_recv.at[0], mirror, across)

    def pot_copy(q):
        part = pot_out.at[pl.ds(2 * cell, 2), share]
        return remote(part, part, pot_send.at[1], pot_recv.at[1], band, q * 2 + side)

    def pot_all():
        part = pot_out.at[pl.ds(0, 2 * (plane - 1)), pl.ds(0, half_rows)]
        return remote(part, part, pot_send.at[1], pot_recv.at[1], band, across)

    def pot_pair():
        part = pot_out.at[:, share]
        return remote(part, part, pot_send.at[3], pot_recv.at[3], sibling, me)

    def pair_copy(step):
        return remote(prod.at[step, 0], drecv.at[step], pair_send.at[step], pair_recv.at[step], sibling, me)

    def line_copy(step, e, l):
        return remote(
            prod.at[step, 1, l, e], zrecv.at[step, line, e], line_send.at[step, e], line_recv.at[step, e],
            l * 2 + core, me,
        )

    def line_all(step, e):
        part = zrecv.at[step, pl.ds(0, lines - 1), 0]
        return remote(part, part, line_send.at[step, e], line_recv.at[step, e], sibling, me)

    def val_copy(step, turn, i, to_band, to):
        return remote(
            tout.at[turn, i], land.at[side, cell], val_send.at[step], val_recv.at[step, cell // 4], to_band, to
        )

    def val_all(step, batch, row, count):
        part = land.at[0, pl.ds(0, count)]
        return remote(part, part, val_send.at[step], val_recv.at[batch, row], band, across)

    with jax.named_scope("send_rot"):
        rot_swap().start()
        pot_load.wait()
        pot_swap().start()
        peers(lambda q: rot_copy(1, side, q).start())
        rots[side, cell] = rot_own[...]

    def mark(src, carry):
        at = pl.ds(pl.multiple_of(src * slots, slots), slots)
        to = pl.ds(pl.multiple_of(src // 2 * slots, slots), slots)
        half = window // 2
        cells = idx[:, at]
        cell_x = (cells // (box * box) + half) % box
        cell_y = (cells // box % box + half) % box
        cell_z = (cells % box + half) % box
        inside = (cell_x < window) & (cell_y < window) & (cell_z < window)
        live = lax.broadcasted_iota(jnp.int32, (1, slots), 1) < cnt[src]
        row_id = jnp.where(live & inside, cell_y % radix * window + cell_x, -1)
        col_id = cell_y // radix * window + cell_z
        rows, cols = onehot.shape[1], hits.shape[1]
        picks = lax.broadcasted_iota(jnp.int32, (rows, slots), 0) == row_id
        onehot[lax.rem(src, 2), :, to] = jnp.where(picks, 1.0, 0.0).astype(BF16)
        found = lax.broadcasted_iota(jnp.int32, (cols, slots), 0) == col_id
        hits[lax.rem(src, 2), :, to] = jnp.where(found, 1.0, 0.0).astype(BF16)
        return carry

    with jax.named_scope("mark0"):
        idx_load.wait()
        cnt_load.wait()
        lax.fori_loop(0, 4, mark, 0)

    with jax.named_scope("relay_rot"):
        rot_swap().wait_recv()
        pot_swap().wait_recv()
        peers(lambda q: rot_copy(2, 1 - side, q).start())
        lax.fori_loop(4, 8, mark, 0)

    def rotate(held, to_core):
        blocks = []
        for l in range(lines):
            for l_of, e in ((l, side), (lines - 1 - l, 1 - side)):
                for r in range(2):
                    blocks.append(rots[held, l_of * 4 + to_core * 2 + r, e])
        a = jnp.concatenate(blocks, axis=0)
        b = jnp.concatenate([piece for blk in blocks for piece in (-blk[4:], blk[:4])], axis=0)
        a_high, a_low = split_parts(a)
        b_high, b_low = split_parts(b)
        lhs = jnp.concatenate([a_high, a_low, a_high, b_high, b_low, b_high], axis=1)
        rhs = jnp.concatenate(
            [coef_parts[0], coef_parts[0], coef_parts[1], coef_parts[2], coef_parts[2], coef_parts[3]], axis=0
        )
        return jnp.dot(lhs, rhs, preferred_element_type=F32).reshape(lines, 2, 2, 8, slots)

    def first_half(step, carry):
        with jax.named_scope("wait_rot"):
            rot_all(1 + step).wait_recv()

        def part(i, carry):
            with jax.named_scope("rotate"):
                prod[step, i] = rotate(lax.rem(side + step, 2), lax.rem(core + 1 + i, 2))

            @pl.when(i == 0)
            def _():
                pair_copy(step).start()

            return carry

        lax.fori_loop(0, 2, part, 0)

        with jax.named_scope("pair"):
            pair_copy(step).wait_recv()
            prod[step, 1] = prod[step, 1] + drecv[step]
            for e in (side, 1 - side):
                lines_other(lambda l: line_copy(step, e, l).start())

        @pl.when(step == 1)
        def _():
            with jax.named_scope("relay_pot"):
                peers(lambda q: pot_copy(q).start())

        return carry

    lax.fori_loop(0, 2, first_half, 0)
    with jax.named_scope("blocks"):
        for tab in tab_loads:
            tab.wait()
        for i in range(2):
            right_blk[i] = block(right_tab[i, 0], right_tab[i, 1])
        kinetic[...] = kinetic_factors(box, window, radix)

    early = lax.rem(me // 8, 2)
    mine_first = early == side
    acc[...] = jnp.zeros_like(acc)

    def row_part(batch, near):
        parity = lax.rem(early + batch, 2)
        row = lax.rem(cell // 4 + near + near // 2 - 2 * (near // 3), 4)
        alone = (parity == side) & (row == cell // 4)

        @pl.when(alone)
        def _():
            val_all(0, batch, row, 3).wait_recv()

        @pl.when(jnp.logical_not(alone))
        def _():
            val_all(0, batch, row, 4).wait_recv()

        return parity, row

    def row_sum(parity, row):
        deep = 4 * slots
        cols = hits.shape[1]
        placed = [[], []]
        for u in range(4):
            to = pl.ds(pl.multiple_of(row * deep + u * slots, slots), slots)
            mask = hits[parity, :, to]
            for n, part in enumerate(split_parts(land[parity, row * 4 + u])):
                part = part.astype(F32)
                pieces = []
                for c in range(2):
                    line_of = jnp.broadcast_to(part[c : c + 1, :], (16, slots)).astype(BF16)
                    pieces.append(mask * jnp.concatenate([line_of] * (cols // 16), axis=0))
                placed[n].append(jnp.concatenate(pieces, axis=0))
        picked = onehot[parity, :, pl.ds(pl.multiple_of(row * deep, deep), deep)]
        high, low = (
            lax.dot_general(
                picked, jnp.concatenate(part, axis=1), (((1,), (1,)), ((), ())), preferred_element_type=F32
            )
            for part in placed
        )
        return high + low

    def collect_pair(pair, carry):
        batch, near = pair // 2, 2 * lax.rem(pair, 2)
        first, second = row_part(batch, near), row_part(batch, near + 1)
        acc[...] += row_sum(*first) + row_sum(*second)
        return carry

    def collect(step, carry):
        acc[...] += row_sum(*row_part(step // 4, lax.rem(step, 4)))
        return carry

    def second_half(turn, carry):
        step, e = turn // 2, lax.rem(side + turn, 2)
        with jax.named_scope("mark1"):
            before = jnp.where(turn == 0, 8, jnp.where(turn == 1, 20, jnp.where(turn == 2, 30, groups)))
            lax.fori_loop(jnp.where(turn == 0, 8, jnp.where(turn == 1, 8, jnp.where(turn == 2, 20, 30))), before, mark, 0)
        @pl.when(turn == 3)
        def _():
            with jax.named_scope("collect0"):
                lax.fori_loop(0, 2 - side, collect, 0)

        with jax.named_scope("wait_line"):
            line_all(step, e).wait_recv()
        with jax.named_scope("send_val"):
            total = prod[step, 1, line, e]
            for other in range(1, lines):
                total = total + zrecv[step, lax.rem(line + other, lines), e]
            for r in range(2):
                for c in range(2):
                    tout[turn, r * 4 : r * 4 + 4, c, :] = total[r, c * 4 : c * 4 + 4]

            def send(n, carry):
                r = lax.rem(cell // 8 + 1 + n // 4, 2)
                m = lax.rem(n, 4)
                x = lax.rem(cell + jnp.where(m == 0, 2, jnp.where(m == 1, 1, jnp.where(m == 2, 3, 0))), 4)
                to = (r * 8 + lax.rem(side + step, 2) * 4 + x) * 2 + lax.rem(side + e, 2)
                i = r * 4 + x

                @pl.when(to != me)
                def _():
                    val_copy(step, turn, i, (1 - e) * band + e * mirror, to).start()

                @pl.when(to == me)
                def _():
                    land[side, cell] = tout[turn, i]

                return carry

            lax.fori_loop(0, 8, send, 0)
        return carry

    lax.fori_loop(0, 4, second_half, 0)
    with jax.named_scope("pair_pot"):
        pot_all().wait_recv()
        pot_pair().start()

    with jax.named_scope("collect"):
        lax.fori_loop(2 - side, 4, collect, 0)
        lax.fori_loop(2, 4, collect_pair, 0)
    grid_field = acc[...]

    def pot_ready():
        pot_pair().wait_recv()

    def out_copy(c):
        return pltpu.make_async_copy(out_buf.at[c], out_ref.at[0, c], out_sem.at[c])

    apply_kernel(
        box, window, radix, band >= 0, pot_ready, grid_field, pot_out, right_blk, left_tab, back_tab, twist,
        mixed, unmixed, kinetic, out_buf, lambda c: out_copy(c).start()
    )
    with jax.named_scope("wait_sends"):
        for c in range(2):
            out_copy(c).wait()
        rot_swap().wait_send()
        rot_all(1).wait_send()
        rot_all(2).wait_send()
        pot_swap().wait_send()
        pot_all().wait_send()
        pot_pair().wait_send()
        for step in range(2):
            pair_copy(step).wait_send()
            for e in range(2):
                line_all(step, e).wait_send()
            alone = mine_first if step == 0 else jnp.logical_not(mine_first)

            @pl.when(alone)
            def _():
                val_all(step, 0, 0, plane - 1).wait_send()

            @pl.when(jnp.logical_not(alone))
            def _():
                val_all(step, 0, 0, plane).wait_send()


def run(coefficients, rotation, potential, index_map, counts, consts, box, window, radix):
    bands, groups = lax.axis_size("band"), lax.axis_size("ga")
    depth, _, slots = coefficients.shape
    cols = rotation.shape[2]
    assert (bands, groups, cols) == (8, 32, 8)
    lines, plane = bands // 2, groups // 2
    rot = rotation.transpose(0, 2, 1).reshape(1, 2 * cols, depth)
    hbm = pl.BlockSpec(memory_space=pl.ANY)
    dma = pltpu.SemaphoreType.DMA
    rows, wide = radix * window, window // radix * window
    blocks = (2, lines, 2, 2, 8, slots)
    return pl.pallas_call(
        functools.partial(whole_kernel, box, window, radix),
        out_shape=jax.ShapeDtypeStruct((1, 2, window, window * window), F32),
        in_specs=[hbm] * 9,
        out_specs=hbm,
        scratch_shapes=[
            pltpu.VMEM((2, depth, slots), F32),
            pltpu.VMEM((4, depth, slots), BF16),
            pltpu.VMEM((2 * cols, depth), F32),
            pltpu.VMEM((2, cols, depth), F32),
            pltpu.VMEM((2, plane, 2, cols, depth), F32),
            pltpu.VMEM((2,) + blocks, F32),
            pltpu.VMEM(blocks, F32),
            pltpu.VMEM(blocks, F32),
            pltpu.VMEM((4, 8, 2, slots), F32),
            pltpu.VMEM((2, plane, 2, slots), F32),
            pltpu.VMEM((2, rows, plane * slots), BF16),
            pltpu.VMEM((2, wide, plane * slots), BF16),
            pltpu.VMEM((rows, 2 * wide), F32),
            pltpu.VMEM((1, groups * slots), jnp.int32),
            pltpu.SMEM((groups,), jnp.int32),
            pltpu.VMEM((groups,) + potential.shape, F32),
            *[pltpu.VMEM(table.shape, table.dtype) for table in consts],
            pltpu.VMEM((2, 2 * wide, 2 * radix * box), BF16),
            pltpu.VMEM((2, radix, 2 * window, radix * box), BF16),
            pltpu.VMEM((radix, 2 * window, radix * box), F32),
            pltpu.VMEM((rows, wide), F32),
            pltpu.VMEM((2, window, window * window), F32),
            dma((10,)),
            dma((3,)),
            dma((3,)),
            dma((4,)),
            dma((4,)),
            dma((2,)),
            dma((2,)),
            dma((2, 2)),
            dma((2, 2)),
            dma((2,)),
            dma((2, 4)),
            dma((2,)),
        ],
        compiler_params=pltpu.CompilerParams(
            collective_id=0, has_side_effects=True, vmem_limit_bytes=60 * 1024 * 1024
        ),
    )(coefficients, rot, potential, index_map[None], counts, *consts)


def kinetic_factors(box, window, radix):
    rows, cols = radix * window, window // radix * window
    half = window // 2
    row_at = lax.broadcasted_iota(jnp.int32, (rows, cols), 0)
    col_at = lax.broadcasted_iota(jnp.int32, (rows, cols), 1)
    n_x = (row_at % window - half).astype(F32)
    n_y = (col_at // window * radix + row_at // window - half).astype(F32)
    n_z = (col_at % window - half).astype(F32)
    return (8.0 / (box * box)) * (n_x * n_x + n_y * n_y + n_z * n_z)


def apply_kernel(
    box, window, radix, apart, pot_ready, grid_field, pot_ref, right_ref, left_ref, back_ref, twist_ref,
    mixed_ref, unmixed_ref, kinetic_ref, out_ref, ship
):
    coarse = window // radix
    rows = radix * window
    cols = coarse * window
    wide = radix * box
    lanes = 128
    per = wide // pot_ref.shape[2]

    def columns(tile):
        return slice(tile * lanes, (tile + 1) * lanes), slice(wide + tile * lanes, wide + (tile + 1) * lanes)

    def right_of(tile):
        return [jnp.concatenate([right_ref[i, :, at] for at in columns(tile)], axis=1) for i in range(2)]

    def twist_of(low, at):
        return twist_ref[0, low : low + 1, at], twist_ref[1, low : low + 1, at]

    with jax.named_scope("fwd_mix"):
        parts = split_parts(grid_field)
        for tile in range(wide // lanes):
            at = columns(tile)[0]
            both = dot3(parts, right_of(tile))
            values = []
            for low in range(radix):
                real = both[low * window : (low + 1) * window, :lanes]
                imag = both[low * window : (low + 1) * window, lanes:]
                if low:
                    cos, sin = twist_of(low, at)
                    real, imag = real * cos - imag * sin, real * sin + imag * cos
                values.append((real, imag))
            for k, pair in enumerate(fft8(values, 1)):
                for c in range(2):
                    high, low = split_parts(pair[c])
                    mixed_ref[0, k, c * window : (c + 1) * window, at] = high
                    mixed_ref[1, k, c * window : (c + 1) * window, at] = low
    with jax.named_scope("wait_pot"):
        pot_ready()

    with jax.named_scope("left"):
        @pl.when(apart)
        def _():
            for k in range(radix):
                for n in range(2):
                    at = slice(n * 2 * lanes, (n + 1) * 2 * lanes)
                    high, low = mixed_ref[0, k, :, at], mixed_ref[1, k, :, at]
                    space = jnp.dot(
                        left_ref[...], jnp.concatenate([high, high, low, low], axis=0), preferred_element_type=F32
                    )
                    pot = jnp.concatenate([pot_ref[k * per + 2 * n + i] for i in range(2)], axis=1)
                    high, low = split_parts(space * jnp.concatenate([pot, pot], axis=0))
                    both = jnp.dot(back_ref[...], jnp.concatenate([high, low], axis=0), preferred_element_type=F32)
                    unmixed_ref[k, :, at] = both[: 2 * window] + both[2 * window :]

    def unmix(tile):
        at = columns(tile)[0]
        values = [(unmixed_ref[k, :window, at], unmixed_ref[k, window:, at]) for k in range(radix)]
        halves = [[], []]
        for low, (real, imag) in enumerate(fft8(values, -1)):
            if low:
                cos, sin = twist_of(low, at)
                real, imag = real * cos + imag * sin, imag * cos - real * sin
            split = [split_parts(real), split_parts(imag)]
            for i in range(2):
                halves[i].append(jnp.concatenate([split[0][i], split[1][i]], axis=1))
        turned = [jnp.concatenate(half, axis=0) for half in halves]
        return dot3(turned, right_of(tile), ((1,), (1,)))

    with jax.named_scope("unmix_back"):
        applied = unmix(0)
        for tile in range(1, wide // lanes):
            applied = applied + unmix(tile)

    kinetic = kinetic_ref[...]
    applied = applied + jnp.concatenate([kinetic, kinetic], axis=1) * grid_field
    for c in range(2):
        pieces = [
            applied[lo * window : (lo + 1) * window, c * cols + hi * window : c * cols + (hi + 1) * window]
            for hi in range(coarse)
            for lo in range(radix)
        ]
        out_ref[c] = jnp.concatenate(pieces, axis=1)
        ship(c)


def per_device(coefficients, rotation, potential, index_map, counts):
    box = potential.shape[0]
    window = box // 2
    radix = math.isqrt(box)
    assert radix * radix == box
    consts = [jnp.asarray(t) for t in tables(box, window, radix)]
    return run(coefficients, rotation, potential, index_map, counts, consts, box, window, radix)


def solution(mesh):
    placed = (P("band", None, "ga"), P(None, "band", "ga"), P(None, "ga"), P(), P())
    return jax.shard_map(
        per_device,
        mesh=mesh,
        in_specs=placed,
        out_specs=P(("band", "ga"), None, None, None),
        check_vma=False,
    )
```

```python
import functools
import math

import jax
import jax.numpy as jnp
import numpy as np
from jax import lax
from jax.experimental import pallas as pl
from jax.experimental.pallas import tpu as pltpu
from jax.sharding import PartitionSpec as P

F32 = jnp.float32
BF16 = jnp.bfloat16


def split_parts(values):
    high = values.astype(BF16)
    return high, (values - high.astype(F32)).astype(BF16)


def two_parts(table):
    high = table.astype(BF16)
    low = (table - high.astype(np.float32)).astype(BF16)
    return np.stack([high, low])


def tables(box, window, radix):
    half = window // 2
    coarse = window // radix
    k_all = np.arange(box)
    n_signed = np.arange(window) - half
    low = np.arange(radix)
    y_phase = (radix * np.arange(coarse) - half)[:, None] * low[None, :]
    z_phase = n_signed[:, None] * k_all[None, :]
    right = y_phase[:, None, :, None] + z_phase[None, :, None, :]
    right = right.reshape(coarse * window, radix * box) % box
    x_phase = k_all[:, None] * n_signed[None, :] % box
    twist = np.repeat(low[:, None] * low[None, :], box, axis=1) % box

    def pair(phase, scale=1.0):
        angle = phase * (2.0 * math.pi / box)
        return (np.stack([np.cos(angle), np.sin(angle)]) * scale).astype(np.float32)

    right_tab = two_parts(pair(right))
    cos, sin = pair(x_phase)
    left_high, left_low = two_parts(np.block([[cos, -sin], [sin, cos]]) / np.float32(box**3))
    left_tab = np.concatenate([left_high, left_low, left_high, left_low], axis=1)
    back_high, back_low = two_parts(np.block([[cos.T, sin.T], [-sin.T, cos.T]]))
    back_tab = np.block([[back_high, back_high], [back_low, back_low]])
    return right_tab, left_tab, back_tab, pair(twist)


def fft8(values, sign):
    root = math.sqrt(0.5)

    def add(a, b):
        return a[0] + b[0], a[1] + b[1]

    def sub(a, b):
        return a[0] - b[0], a[1] - b[1]

    def turn(a):
        return (-a[1], a[0]) if sign > 0 else (a[1], -a[0])

    def fft4(a, b, c, d):
        total, diff = add(a, c), sub(a, c)
        other, cross = add(b, d), turn(sub(b, d))
        return add(total, other), add(diff, cross), sub(total, other), sub(diff, cross)

    even = fft4(*values[0::2])
    odd = list(fft4(*values[1::2]))
    one, three = odd[1], odd[3]
    one_turn, three_turn = turn(one), turn(three)
    odd[1] = ((one[0] + one_turn[0]) * root, (one[1] + one_turn[1]) * root)
    odd[2] = turn(odd[2])
    odd[3] = ((three_turn[0] - three[0]) * root, (three_turn[1] - three[1]) * root)
    return [add(a, b) for a, b in zip(even, odd)] + [sub(a, b) for a, b in zip(even, odd)]


def dot3(lhs, rhs, dims=((1,), (0,))):
    def one(a, b):
        return lax.dot_general(a, b, (dims, ((), ())), preferred_element_type=F32)

    return one(lhs[0], rhs[0]) + (one(lhs[0], rhs[1]) + one(lhs[1], rhs[0]))


def block(cos, sin):
    upper = jnp.concatenate([cos, sin], axis=1)
    lower = jnp.concatenate([-sin, cos], axis=1)
    return jnp.concatenate([upper, lower], axis=0)


def whole_kernel(
    box, window, radix, coef_hbm, rot_hbm, pot_hbm, idx_hbm, cnt_hbm, right_hbm, left_hbm, back_hbm, twist_hbm,
    out_ref, coef, coef_parts, rot_raw, rot_own, rots, prod, drecv, zrecv, tout, land, onehot, hits, acc, idx, cnt,
    pot_out, right_tab, left_tab, back_tab, twist, right_blk, mixed, unmixed, kinetic, out_buf,
    load_sem, rot_send, rot_recv, pot_send, pot_recv, pair_send, pair_recv, line_send, line_recv, val_send, val_recv,
    out_sem
):
    band = lax.axis_index("band")
    me = lax.axis_index("ga")
    groups = 2 * rots.shape[1]
    plane = groups // 2
    lines = zrecv.shape[1]
    line, core = band // 2, lax.rem(band, 2)
    cell, side = me // 2, lax.rem(me, 2)
    across = cell * 2 + (1 - side)
    sibling = line * 2 + (1 - core)
    mirror = (lines - 1 - line) * 2 + core
    half_rows = pot_hbm.shape[0] // 2
    share = pl.ds(pl.multiple_of(core * half_rows, half_rows), half_rows)
    slots = coef.shape[2]

    def local(src, dst, i):
        copy = pltpu.make_async_copy(src, dst, load_sem.at[i])
        copy.start()
        return copy

    barrier = pltpu.get_barrier_semaphore()

    def greet(to_band, to):
        pl.semaphore_signal(
            barrier, inc=1, device_id={"band": to_band, "ga": to}, device_id_type=pl.DeviceIdType.MESH
        )

    def peers(act):
        def body(step, code):
            shift = lax.rem(code, 16)
            act(lax.rem(cell // 4 + shift // 4, 4) * 4 + lax.rem(cell + shift, 4))
            return code // 16

        lax.fori_loop(0, 8, body, jnp.int32(0x528E6B9A))
        lax.fori_loop(0, 7, body, jnp.int32(0xC431FD7))

    def lines_other(act):
        for step in range(lines):
            l = side * (lines - 1 - step) + (1 - side) * step

            @pl.when(l != line)
            def _(l=l):
                act(l)

    def remote(src, dst, send, recv, to_band, to):
        return pltpu.make_async_remote_copy(
            src_ref=src, dst_ref=dst, send_sem=send, recv_sem=recv,
            device_id={"band": to_band, "ga": to}, device_id_type=pl.DeviceIdType.MESH,
        )

    with jax.named_scope("barrier"):
        greet(band, across)
        greet(mirror, across)
        peers(lambda q: greet(band, q * 2 + side))
        lines_other(lambda l: greet(l * 2 + core, me))
        greet(sibling, me)

    rot_load = local(rot_hbm.at[0], rot_raw, 0)
    idx_load = local(idx_hbm, idx, 1)
    cnt_load = local(cnt_hbm, cnt, 2)
    coef_loads = [local(coef_hbm.at[:, c, :], coef.at[c], 3 + c) for c in range(2)]
    pot_load = local(pot_hbm, pot_out.at[me], 5)
    tab_loads = [
        local(src, dst, 6 + i)
        for i, (src, dst) in enumerate(
            ((right_hbm, right_tab), (left_hbm, left_tab), (back_hbm, back_tab), (twist_hbm, twist))
        )
    ]

    def split_coef():
        for c in range(2):
            coef_loads[c].wait()
            high, low = split_parts(coef[c])
            coef_parts[2 * c] = high
            coef_parts[2 * c + 1] = low
        rot_load.wait()
        for e in range(2):
            for c in range(2):
                for x in range(4):
                    rot_own[e, 4 * c + x] = rot_raw[8 * c + 2 * x + e]

    with jax.named_scope("barrier_wait"):
        split_coef()
        pl.semaphore_wait(barrier, plane - 1 + 3 + lines - 1)

    def rot_swap():
        return remote(rot_own, rots.at[side, cell], rot_send.at[0], rot_recv.at[0], band, across)

    def rot_copy(which, held, q):
        slot = rots.at[held, cell]
        src = rot_own if which == 1 else slot
        return remote(src, slot, rot_send.at[which], rot_recv.at[which], band, q * 2 + side)

    def rot_all(which):
        part = rots.at[0, pl.ds(0, plane - 1)]
        return remote(part, part, rot_send.at[which], rot_recv.at[which], band, across)

    def pot_swap():
        part = pot_out.at[me, share]
        return remote(part, part, pot_send.at[0], pot_recv.at[0], mirror, across)

    def pot_copy(q):
        part = pot_out.at[pl.ds(2 * cell, 2), share]
        return remote(part, part, pot_send.at[1], pot_recv.at[1], band, q * 2 + side)

    def pot_all():
        part = pot_out.at[pl.ds(0, 2 * (plane - 1)), pl.ds(0, half_rows)]
        return remote(part, part, pot_send.at[1], pot_recv.at[1], band, across)

    def pot_pair():
        part = pot_out.at[:, share]
        return remote(part, part, pot_send.at[3], pot_recv.at[3], sibling, me)

    def pair_copy(step):
        return remote(prod.at[step, 0], drecv.at[step], pair_send.at[step], pair_recv.at[step], sibling, me)

    def line_copy(step, e, l):
        return remote(
            prod.at[step, 1, l, e], zrecv.at[step, line, e], line_send.at[step, e], line_recv.at[step, e],
            l * 2 + core, me,
        )

    def line_all(step, e):
        part = zrecv.at[step, pl.ds(0, lines - 1), 0]
        return remote(part, part, line_send.at[step, e], line_recv.at[step, e], sibling, me)

    def val_copy(step, turn, i, to_band, to):
        return remote(
            tout.at[turn, i], land.at[side, cell], val_send.at[step], val_recv.at[step, cell // 4], to_band, to
        )

    def val_all(step, batch, row, count):
        part = land.at[0, pl.ds(0, count)]
        return remote(part, part, val_send.at[step], val_recv.at[batch, row], band, across)

    with jax.named_scope("send_rot"):
        rot_swap().start()
        pot_load.wait()
        pot_swap().start()
        peers(lambda q: rot_copy(1, side, q).start())
        rots[side, cell] = rot_own[...]

    def mark(src, carry):
        at = pl.ds(pl.multiple_of(src * slots, slots), slots)
        to = pl.ds(pl.multiple_of(src // 2 * slots, slots), slots)
        half = window // 2
        cells = idx[:, at]
        cell_x = (cells // (box * box) + half) % box
        cell_y = (cells // box % box + half) % box
        cell_z = (cells % box + half) % box
        inside = (cell_x < window) & (cell_y < window) & (cell_z < window)
        live = lax.broadcasted_iota(jnp.int32, (1, slots), 1) < cnt[src]
        row_id = jnp.where(live & inside, cell_y % radix * window + cell_x, -1)
        col_id = cell_y // radix * window + cell_z
        rows, cols = onehot.shape[1], hits.shape[1]
        picks = lax.broadcasted_iota(jnp.int32, (rows, slots), 0) == row_id
        onehot[lax.rem(src, 2), :, to] = jnp.where(picks, 1.0, 0.0).astype(BF16)
        found = lax.broadcasted_iota(jnp.int32, (cols, slots), 0) == col_id
        hits[lax.rem(src, 2), :, to] = jnp.where(found, 1.0, 0.0).astype(BF16)
        return carry

    with jax.named_scope("mark0"):
        idx_load.wait()
        cnt_load.wait()
        lax.fori_loop(0, 4, mark, 0)

    with jax.named_scope("relay_rot"):
        rot_swap().wait_recv()
        pot_swap().wait_recv()
        peers(lambda q: rot_copy(2, 1 - side, q).start())
        lax.fori_loop(4, 8, mark, 0)

    def rotate(held, to_core):
        blocks = []
        for l in range(lines):
            for l_of, e in ((l, side), (lines - 1 - l, 1 - side)):
                for r in range(2):
                    blocks.append(rots[held, l_of * 4 + to_core * 2 + r, e])
        a = jnp.concatenate(blocks, axis=0)
        b = jnp.concatenate([piece for blk in blocks for piece in (-blk[4:], blk[:4])], axis=0)
        a_high, a_low = split_parts(a)
        b_high, b_low = split_parts(b)
        lhs = jnp.concatenate([a_high, a_low, a_high, b_high, b_low, b_high], axis=1)
        rhs = jnp.concatenate(
            [coef_parts[0], coef_parts[0], coef_parts[1], coef_parts[2], coef_parts[2], coef_parts[3]], axis=0
        )
        return jnp.dot(lhs, rhs, preferred_element_type=F32).reshape(lines, 2, 2, 8, slots)

    def first_half(step, carry):
        with jax.named_scope("wait_rot"):
            rot_all(1 + step).wait_recv()

        def part(i, carry):
            with jax.named_scope("rotate"):
                prod[step, i] = rotate(lax.rem(side + step, 2), lax.rem(core + 1 + i, 2))

            @pl.when(i == 0)
            def _():
                pair_copy(step).start()

            return carry

        lax.fori_loop(0, 2, part, 0)

        with jax.named_scope("pair"):
            pair_copy(step).wait_recv()
            for e in (side, 1 - side):
                prod[step, 1, :, e] = prod[step, 1, :, e] + drecv[step, :, e]
                lines_other(lambda l: line_copy(step, e, l).start())

        @pl.when(step == 1)
        def _():
            with jax.named_scope("relay_pot"):
                peers(lambda q: pot_copy(q).start())

        return carry

    lax.fori_loop(0, 2, first_half, 0)
    with jax.named_scope("blocks"):
        for tab in tab_loads:
            tab.wait()
        for i in range(2):
            right_blk[i] = block(right_tab[i, 0], right_tab[i, 1])
        kinetic[...] = kinetic_factors(box, window, radix)

    early = lax.rem(me // 8, 2)
    mine_first = early == side
    acc[...] = jnp.zeros_like(acc)

    def row_part(batch, near):
        parity = lax.rem(early + batch, 2)
        row = lax.rem(cell // 4 + near + near // 2 - 2 * (near // 3), 4)
        alone = (parity == side) & (row == cell // 4)

        @pl.when(alone)
        def _():
            val_all(0, batch, row, 3).wait_recv()

        @pl.when(jnp.logical_not(alone))
        def _():
            val_all(0, batch, row, 4).wait_recv()

        return parity, row

    def row_sum(parity, row):
        deep = 4 * slots
        cols = hits.shape[1]
        placed = [[], []]
        for u in range(4):
            to = pl.ds(pl.multiple_of(row * deep + u * slots, slots), slots)
            mask = hits[parity, :, to]
            for n, part in enumerate(split_parts(land[parity, row * 4 + u])):
                part = part.astype(F32)
                pieces = []
                for c in range(2):
                    line_of = jnp.broadcast_to(part[c : c + 1, :], (16, slots)).astype(BF16)
                    pieces.append(mask * jnp.concatenate([line_of] * (cols // 16), axis=0))
                placed[n].append(jnp.concatenate(pieces, axis=0))
        picked = onehot[parity, :, pl.ds(pl.multiple_of(row * deep, deep), deep)]
        high, low = (
            lax.dot_general(
                picked, jnp.concatenate(part, axis=1), (((1,), (1,)), ((), ())), preferred_element_type=F32
            )
            for part in placed
        )
        return high + low

    def collect_pair(pair, carry):
        batch, near = pair // 2, 2 * lax.rem(pair, 2)
        first, second = row_part(batch, near), row_part(batch, near + 1)
        acc[...] += row_sum(*first) + row_sum(*second)
        return carry

    def collect(step, carry):
        acc[...] += row_sum(*row_part(step // 4, lax.rem(step, 4)))
        return carry

    def second_half(turn, carry):
        step, e = turn // 2, lax.rem(side + turn, 2)
        with jax.named_scope("mark1"):
            before = jnp.where(turn == 0, 8, jnp.where(turn == 1, 20, jnp.where(turn == 2, 30, groups)))
            lax.fori_loop(jnp.where(turn == 0, 8, jnp.where(turn == 1, 8, jnp.where(turn == 2, 20, 30))), before, mark, 0)
        @pl.when(turn == 3)
        def _():
            with jax.named_scope("collect0"):
                lax.fori_loop(0, 2 - side, collect, 0)

        with jax.named_scope("wait_line"):
            line_all(step, e).wait_recv()
        with jax.named_scope("send_val"):
            total = prod[step, 1, line, e]
            for other in range(1, lines):
                total = total + zrecv[step, lax.rem(line + other, lines), e]
            for r in range(2):
                for c in range(2):
                    tout[turn, r * 4 : r * 4 + 4, c, :] = total[r, c * 4 : c * 4 + 4]

            def send(n, carry):
                r = lax.rem(cell // 8 + 1 + n // 4, 2)
                m = lax.rem(n, 4)
                x = lax.rem(cell + jnp.where(m == 0, 2, jnp.where(m == 1, 1, jnp.where(m == 2, 3, 0))), 4)
                to = (r * 8 + lax.rem(side + step, 2) * 4 + x) * 2 + lax.rem(side + e, 2)
                i = r * 4 + x

                @pl.when(to != me)
                def _():
                    val_copy(step, turn, i, (1 - e) * band + e * mirror, to).start()

                @pl.when(to == me)
                def _():
                    land[side, cell] = tout[turn, i]

                return carry

            lax.fori_loop(0, 8, send, 0)
        return carry

    lax.fori_loop(0, 4, second_half, 0)
    with jax.named_scope("pair_pot"):
        pot_all().wait_recv()
        pot_pair().start()

    with jax.named_scope("collect"):
        lax.fori_loop(2 - side, 4, collect, 0)
        lax.fori_loop(2, 3, collect_pair, 0)
        lax.fori_loop(6, 8, collect, 0)
    grid_field = acc[...]

    def pot_ready():
        pot_pair().wait_recv()

    def out_copy(c):
        return pltpu.make_async_copy(out_buf.at[c], out_ref.at[0, c], out_sem.at[c])

    apply_kernel(
        box, window, radix, band >= 0, pot_ready, grid_field, pot_out, right_blk, left_tab, back_tab, twist,
        mixed, unmixed, kinetic, out_buf, lambda c: out_copy(c).start()
    )
    with jax.named_scope("wait_sends"):
        for c in range(2):
            out_copy(c).wait()
        rot_swap().wait_send()
        rot_all(1).wait_send()
        rot_all(2).wait_send()
        pot_swap().wait_send()
        pot_all().wait_send()
        pot_pair().wait_send()
        for step in range(2):
            pair_copy(step).wait_send()
            for e in range(2):
                line_all(step, e).wait_send()
            alone = mine_first if step == 0 else jnp.logical_not(mine_first)

            @pl.when(alone)
            def _():
                val_all(step, 0, 0, plane - 1).wait_send()

            @pl.when(jnp.logical_not(alone))
            def _():
                val_all(step, 0, 0, plane).wait_send()


def run(coefficients, rotation, potential, index_map, counts, consts, box, window, radix):
    bands, groups = lax.axis_size("band"), lax.axis_size("ga")
    depth, _, slots = coefficients.shape
    cols = rotation.shape[2]
    assert (bands, groups, cols) == (8, 32, 8)
    lines, plane = bands // 2, groups // 2
    rot = rotation.transpose(0, 2, 1).reshape(1, 2 * cols, depth)
    hbm = pl.BlockSpec(memory_space=pl.ANY)
    dma = pltpu.SemaphoreType.DMA
    rows, wide = radix * window, window // radix * window
    blocks = (2, lines, 2, 2, 8, slots)
    return pl.pallas_call(
        functools.partial(whole_kernel, box, window, radix),
        out_shape=jax.ShapeDtypeStruct((1, 2, window, window * window), F32),
        in_specs=[hbm] * 9,
        out_specs=hbm,
        scratch_shapes=[
            pltpu.VMEM((2, depth, slots), F32),
            pltpu.VMEM((4, depth, slots), BF16),
            pltpu.VMEM((2 * cols, depth), F32),
            pltpu.VMEM((2, cols, depth), F32),
            pltpu.VMEM((2, plane, 2, cols, depth), F32),
            pltpu.VMEM((2,) + blocks, F32),
            pltpu.VMEM(blocks, F32),
            pltpu.VMEM(blocks, F32),
            pltpu.VMEM((4, 8, 2, slots), F32),
            pltpu.VMEM((2, plane, 2, slots), F32),
            pltpu.VMEM((2, rows, plane * slots), BF16),
            pltpu.VMEM((2, wide, plane * slots), BF16),
            pltpu.VMEM((rows, 2 * wide), F32),
            pltpu.VMEM((1, groups * slots), jnp.int32),
            pltpu.SMEM((groups,), jnp.int32),
            pltpu.VMEM((groups,) + potential.shape, F32),
            *[pltpu.VMEM(table.shape, table.dtype) for table in consts],
            pltpu.VMEM((2, 2 * wide, 2 * radix * box), BF16),
            pltpu.VMEM((2, radix, 2 * window, radix * box), BF16),
            pltpu.VMEM((radix, 2 * window, radix * box), F32),
            pltpu.VMEM((rows, wide), F32),
            pltpu.VMEM((2, window, window * window), F32),
            dma((10,)),
            dma((3,)),
            dma((3,)),
            dma((4,)),
            dma((4,)),
            dma((2,)),
            dma((2,)),
            dma((2, 2)),
            dma((2, 2)),
            dma((2,)),
            dma((2, 4)),
            dma((2,)),
        ],
        compiler_params=pltpu.CompilerParams(
            collective_id=0, has_side_effects=True, vmem_limit_bytes=60 * 1024 * 1024
        ),
    )(coefficients, rot, potential, index_map[None], counts, *consts)


def kinetic_factors(box, window, radix):
    rows, cols = radix * window, window // radix * window
    half = window // 2
    row_at = lax.broadcasted_iota(jnp.int32, (rows, cols), 0)
    col_at = lax.broadcasted_iota(jnp.int32, (rows, cols), 1)
    n_x = (row_at % window - half).astype(F32)
    n_y = (col_at // window * radix + row_at // window - half).astype(F32)
    n_z = (col_at % window - half).astype(F32)
    return (8.0 / (box * box)) * (n_x * n_x + n_y * n_y + n_z * n_z)


def apply_kernel(
    box, window, radix, apart, pot_ready, grid_field, pot_ref, right_ref, left_ref, back_ref, twist_ref,
    mixed_ref, unmixed_ref, kinetic_ref, out_ref, ship
):
    coarse = window // radix
    rows = radix * window
    cols = coarse * window
    wide = radix * box
    lanes = 128
    per = wide // pot_ref.shape[2]

    def columns(tile):
        return slice(tile * lanes, (tile + 1) * lanes), slice(wide + tile * lanes, wide + (tile + 1) * lanes)

    def right_of(tile):
        return [jnp.concatenate([right_ref[i, :, at] for at in columns(tile)], axis=1) for i in range(2)]

    def twist_of(low, at):
        return twist_ref[0, low : low + 1, at], twist_ref[1, low : low + 1, at]

    with jax.named_scope("fwd_mix"):
        parts = split_parts(grid_field)
        for tile in range(wide // lanes):
            at = columns(tile)[0]
            both = dot3(parts, right_of(tile))
            values = []
            for low in range(radix):
                real = both[low * window : (low + 1) * window, :lanes]
                imag = both[low * window : (low + 1) * window, lanes:]
                if low:
                    cos, sin = twist_of(low, at)
                    real, imag = real * cos - imag * sin, real * sin + imag * cos
                values.append((real, imag))
            for k, pair in enumerate(fft8(values, 1)):
                for c in range(2):
                    high, low = split_parts(pair[c])
                    mixed_ref[0, k, c * window : (c + 1) * window, at] = high
                    mixed_ref[1, k, c * window : (c + 1) * window, at] = low
    with jax.named_scope("wait_pot"):
        pot_ready()

    with jax.named_scope("left"):
        @pl.when(apart)
        def _():
            for k in range(radix):
                for n in range(2):
                    at = slice(n * 2 * lanes, (n + 1) * 2 * lanes)
                    high, low = mixed_ref[0, k, :, at], mixed_ref[1, k, :, at]
                    space = jnp.dot(
                        left_ref[...], jnp.concatenate([high, high, low, low], axis=0), preferred_element_type=F32
                    )
                    pot = jnp.concatenate([pot_ref[k * per + 2 * n + i] for i in range(2)], axis=1)
                    high, low = split_parts(space * jnp.concatenate([pot, pot], axis=0))
                    both = jnp.dot(back_ref[...], jnp.concatenate([high, low], axis=0), preferred_element_type=F32)
                    unmixed_ref[k, :, at] = both[: 2 * window] + both[2 * window :]

    def unmix(tile):
        at = columns(tile)[0]
        values = [(unmixed_ref[k, :window, at], unmixed_ref[k, window:, at]) for k in range(radix)]
        halves = [[], []]
        for low, (real, imag) in enumerate(fft8(values, -1)):
            if low:
                cos, sin = twist_of(low, at)
                real, imag = real * cos + imag * sin, imag * cos - real * sin
            split = [split_parts(real), split_parts(imag)]
            for i in range(2):
                halves[i].append(jnp.concatenate([split[0][i], split[1][i]], axis=1))
        turned = [jnp.concatenate(half, axis=0) for half in halves]
        return dot3(turned, right_of(tile), ((1,), (1,)))

    with jax.named_scope("unmix_back"):
        applied = unmix(0)
        for tile in range(1, wide // lanes):
            applied = applied + unmix(tile)

    kinetic = kinetic_ref[...]
    applied = applied + jnp.concatenate([kinetic, kinetic], axis=1) * grid_field
    for c in range(2):
        pieces = [
            applied[lo * window : (lo + 1) * window, c * cols + hi * window : c * cols + (hi + 1) * window]
            for hi in range(coarse)
            for lo in range(radix)
        ]
        out_ref[c] = jnp.concatenate(pieces, axis=1)
        ship(c)


def per_device(coefficients, rotation, potential, index_map, counts):
    box = potential.shape[0]
    window = box // 2
    radix = math.isqrt(box)
    assert radix * radix == box
    consts = [jnp.asarray(t) for t in tables(box, window, radix)]
    return run(coefficients, rotation, potential, index_map, counts, consts, box, window, radix)


def solution(mesh):
    placed = (P("band", None, "ga"), P(None, "band", "ga"), P(None, "ga"), P(), P())
    return jax.shard_map(
        per_device,
        mesh=mesh,
        in_specs=placed,
        out_specs=P(("band", "ga"), None, None, None),
        check_vma=False,
    )
```

```python
import functools
import math

import jax
import jax.numpy as jnp
import numpy as np
from jax import lax
from jax.experimental import pallas as pl
from jax.experimental.pallas import tpu as pltpu
from jax.sharding import PartitionSpec as P

F32 = jnp.float32
BF16 = jnp.bfloat16


def split_parts(values):
    high = values.astype(BF16)
    return high, (values - high.astype(F32)).astype(BF16)


def two_parts(table):
    high = table.astype(BF16)
    low = (table - high.astype(np.float32)).astype(BF16)
    return np.stack([high, low])


def tables(box, window, radix):
    half = window // 2
    coarse = window // radix
    k_all = np.arange(box)
    n_signed = np.arange(window) - half
    low = np.arange(radix)
    y_phase = (radix * np.arange(coarse) - half)[:, None] * low[None, :]
    z_phase = n_signed[:, None] * k_all[None, :]
    right = y_phase[:, None, :, None] + z_phase[None, :, None, :]
    right = right.reshape(coarse * window, radix * box) % box
    x_phase = k_all[:, None] * n_signed[None, :] % box
    twist = np.repeat(low[:, None] * low[None, :], box, axis=1) % box

    def pair(phase, scale=1.0):
        angle = phase * (2.0 * math.pi / box)
        return (np.stack([np.cos(angle), np.sin(angle)]) * scale).astype(np.float32)

    right_tab = two_parts(pair(right))
    cos, sin = pair(x_phase)
    left_high, left_low = two_parts(np.block([[cos, -sin], [sin, cos]]) / np.float32(box**3))
    left_tab = np.concatenate([left_high, left_low, left_high, left_low], axis=1)
    back_high, back_low = two_parts(np.block([[cos.T, sin.T], [-sin.T, cos.T]]))
    back_tab = np.block([[back_high, back_high], [back_low, back_low]])
    return right_tab, left_tab, back_tab, pair(twist)


def fft8(values, sign):
    root = math.sqrt(0.5)

    def add(a, b):
        return a[0] + b[0], a[1] + b[1]

    def sub(a, b):
        return a[0] - b[0], a[1] - b[1]

    def turn(a):
        return (-a[1], a[0]) if sign > 0 else (a[1], -a[0])

    def fft4(a, b, c, d):
        total, diff = add(a, c), sub(a, c)
        other, cross = add(b, d), turn(sub(b, d))
        return add(total, other), add(diff, cross), sub(total, other), sub(diff, cross)

    even = fft4(*values[0::2])
    odd = list(fft4(*values[1::2]))
    one, three = odd[1], odd[3]
    one_turn, three_turn = turn(one), turn(three)
    odd[1] = ((one[0] + one_turn[0]) * root, (one[1] + one_turn[1]) * root)
    odd[2] = turn(odd[2])
    odd[3] = ((three_turn[0] - three[0]) * root, (three_turn[1] - three[1]) * root)
    return [add(a, b) for a, b in zip(even, odd)] + [sub(a, b) for a, b in zip(even, odd)]


def dot3(lhs, rhs, dims=((1,), (0,))):
    def one(a, b):
        return lax.dot_general(a, b, (dims, ((), ())), preferred_element_type=F32)

    return one(lhs[0], rhs[0]) + (one(lhs[0], rhs[1]) + one(lhs[1], rhs[0]))


def block(cos, sin):
    upper = jnp.concatenate([cos, sin], axis=1)
    lower = jnp.concatenate([-sin, cos], axis=1)
    return jnp.concatenate([upper, lower], axis=0)


def whole_kernel(
    box, window, radix, coef_hbm, rot_hbm, pot_hbm, idx_hbm, cnt_hbm, right_hbm, left_hbm, back_hbm, twist_hbm,
    out_ref, coef, coef_parts, rot_raw, rot_own, rots, prod, drecv, zrecv, tout, land, onehot, hits, acc, idx, cnt,
    pot_out, right_tab, left_tab, back_tab, twist, right_blk, mixed, unmixed, kinetic, out_buf,
    load_sem, rot_send, rot_recv, pot_send, pot_recv, pair_send, pair_recv, line_send, line_recv, val_send, val_recv,
    out_sem
):
    band = lax.axis_index("band")
    me = lax.axis_index("ga")
    groups = 2 * rots.shape[1]
    plane = groups // 2
    lines = zrecv.shape[1]
    line, core = band // 2, lax.rem(band, 2)
    cell, side = me // 2, lax.rem(me, 2)
    across = cell * 2 + (1 - side)
    sibling = line * 2 + (1 - core)
    mirror = (lines - 1 - line) * 2 + core
    half_rows = pot_hbm.shape[0] // 2
    share = pl.ds(pl.multiple_of(core * half_rows, half_rows), half_rows)
    slots = coef.shape[2]

    def local(src, dst, i):
        copy = pltpu.make_async_copy(src, dst, load_sem.at[i])
        copy.start()
        return copy

    barrier = pltpu.get_barrier_semaphore()

    def greet(to_band, to):
        pl.semaphore_signal(
            barrier, inc=1, device_id={"band": to_band, "ga": to}, device_id_type=pl.DeviceIdType.MESH
        )

    def peers(act):
        def body(step, code):
            shift = lax.rem(code, 16)
            act(lax.rem(cell // 4 + shift // 4, 4) * 4 + lax.rem(cell + shift, 4))
            return code // 16

        lax.fori_loop(0, 8, body, jnp.int32(0x528E6B9A))
        lax.fori_loop(0, 7, body, jnp.int32(0xC431FD7))

    def lines_other(act):
        for step in range(lines):
            l = side * (lines - 1 - step) + (1 - side) * step

            @pl.when(l != line)
            def _(l=l):
                act(l)

    def remote(src, dst, send, recv, to_band, to):
        return pltpu.make_async_remote_copy(
            src_ref=src, dst_ref=dst, send_sem=send, recv_sem=recv,
            device_id={"band": to_band, "ga": to}, device_id_type=pl.DeviceIdType.MESH,
        )

    with jax.named_scope("barrier"):
        greet(band, across)
        greet(mirror, across)
        peers(lambda q: greet(band, q * 2 + side))
        lines_other(lambda l: greet(l * 2 + core, me))
        greet(sibling, me)

    rot_load = local(rot_hbm.at[0], rot_raw, 0)
    idx_load = local(idx_hbm, idx, 1)
    cnt_load = local(cnt_hbm, cnt, 2)
    coef_loads = [local(coef_hbm.at[:, c, :], coef.at[c], 3 + c) for c in range(2)]
    pot_load = local(pot_hbm, pot_out.at[me], 5)
    tab_loads = [
        local(src, dst, 6 + i)
        for i, (src, dst) in enumerate(
            ((right_hbm, right_tab), (left_hbm, left_tab), (back_hbm, back_tab), (twist_hbm, twist))
        )
    ]

    def split_coef():
        for c in range(2):
            coef_loads[c].wait()
            high, low = split_parts(coef[c])
            coef_parts[2 * c] = high
            coef_parts[2 * c + 1] = low
        rot_load.wait()
        for e in range(2):
            for c in range(2):
                for x in range(4):
                    rot_own[e, 4 * c + x] = rot_raw[8 * c + 2 * x + e]

    with jax.named_scope("barrier_wait"):
        split_coef()
        pl.semaphore_wait(barrier, plane - 1 + 3 + lines - 1)

    def rot_swap():
        return remote(rot_own, rots.at[side, cell], rot_send.at[0], rot_recv.at[0], band, across)

    def rot_copy(which, held, q):
        slot = rots.at[held, cell]
        src = rot_own if which == 1 else slot
        return remote(src, slot, rot_send.at[which], rot_recv.at[which], band, q * 2 + side)

    def rot_all(which):
        part = rots.at[0, pl.ds(0, plane - 1)]
        return remote(part, part, rot_send.at[which], rot_recv.at[which], band, across)

    def pot_swap():
        part = pot_out.at[me, share]
        return remote(part, part, pot_send.at[0], pot_recv.at[0], mirror, across)

    def pot_copy(q):
        part = pot_out.at[pl.ds(2 * cell, 2), share]
        return remote(part, part, pot_send.at[1], pot_recv.at[1], band, q * 2 + side)

    def pot_all():
        part = pot_out.at[pl.ds(0, 2 * (plane - 1)), pl.ds(0, half_rows)]
        return remote(part, part, pot_send.at[1], pot_recv.at[1], band, across)

    def pot_pair():
        part = pot_out.at[:, share]
        return remote(part, part, pot_send.at[3], pot_recv.at[3], sibling, me)

    def pair_copy(step):
        return remote(prod.at[step, 0], drecv.at[step], pair_send.at[step], pair_recv.at[step], sibling, me)

    def line_copy(step, e, l):
        return remote(
            prod.at[step, 1, l, e], zrecv.at[step, line, e], line_send.at[step, e], line_recv.at[step, e],
            l * 2 + core, me,
        )

    def line_all(step, e):
        part = zrecv.at[step, pl.ds(0, lines - 1), 0]
        return remote(part, part, line_send.at[step, e], line_recv.at[step, e], sibling, me)

    def val_copy(step, turn, i, to_band, to):
        return remote(
            tout.at[turn, i], land.at[side, cell], val_send.at[step], val_recv.at[step, cell // 4], to_band, to
        )

    def val_all(step, batch, row, count):
        part = land.at[0, pl.ds(0, count)]
        return remote(part, part, val_send.at[step], val_recv.at[batch, row], band, across)

    with jax.named_scope("send_rot"):
        rot_swap().start()
        pot_load.wait()
        pot_swap().start()
        peers(lambda q: rot_copy(1, side, q).start())
        rots[side, cell] = rot_own[...]

    def mark(src, carry):
        at = pl.ds(pl.multiple_of(src * slots, slots), slots)
        to = pl.ds(pl.multiple_of(src // 2 * slots, slots), slots)
        half = window // 2
        cells = idx[:, at]
        cell_x = (cells // (box * box) + half) % box
        cell_y = (cells // box % box + half) % box
        cell_z = (cells % box + half) % box
        inside = (cell_x < window) & (cell_y < window) & (cell_z < window)
        live = lax.broadcasted_iota(jnp.int32, (1, slots), 1) < cnt[src]
        row_id = jnp.where(live & inside, cell_y % radix * window + cell_x, -1)
        col_id = cell_y // radix * window + cell_z
        rows, cols = onehot.shape[1], hits.shape[1]
        picks = lax.broadcasted_iota(jnp.int32, (rows, slots), 0) == row_id
        onehot[lax.rem(src, 2), :, to] = jnp.where(picks, 1.0, 0.0).astype(BF16)
        found = lax.broadcasted_iota(jnp.int32, (cols, slots), 0) == col_id
        hits[lax.rem(src, 2), :, to] = jnp.where(found, 1.0, 0.0).astype(BF16)
        return carry

    with jax.named_scope("mark0"):
        idx_load.wait()
        cnt_load.wait()
        lax.fori_loop(0, 4, mark, 0)

    with jax.named_scope("relay_rot"):
        rot_swap().wait_recv()
        pot_swap().wait_recv()
        peers(lambda q: rot_copy(2, 1 - side, q).start())
        lax.fori_loop(4, 8, mark, 0)

    def rotate(held, to_core):
        blocks = []
        for l in range(lines):
            for l_of, e in ((l, side), (lines - 1 - l, 1 - side)):
                for r in range(2):
                    blocks.append(rots[held, l_of * 4 + to_core * 2 + r, e])
        a = jnp.concatenate(blocks, axis=0)
        b = jnp.concatenate([piece for blk in blocks for piece in (-blk[4:], blk[:4])], axis=0)
        a_high, a_low = split_parts(a)
        b_high, b_low = split_parts(b)
        lhs = jnp.concatenate([a_high, a_low, a_high, b_high, b_low, b_high], axis=1)
        rhs = jnp.concatenate(
            [coef_parts[0], coef_parts[0], coef_parts[1], coef_parts[2], coef_parts[2], coef_parts[3]], axis=0
        )
        return jnp.dot(lhs, rhs, preferred_element_type=F32).reshape(lines, 2, 2, 8, slots)

    def first_half(step, carry):
        with jax.named_scope("wait_rot"):
            rot_all(1 + step).wait_recv()

        def part(i, carry):
            with jax.named_scope("rotate"):
                prod[step, i] = rotate(lax.rem(side + step, 2), lax.rem(core + 1 + i, 2))

            @pl.when(i == 0)
            def _():
                pair_copy(step).start()

            return carry

        lax.fori_loop(0, 2, part, 0)

        with jax.named_scope("pair"):
            pair_copy(step).wait_recv()
            prod[step, 1] = prod[step, 1] + drecv[step]
            for e in (side, 1 - side):
                lines_other(lambda l: line_copy(step, e, l).start())

        @pl.when(step == 1)
        def _():
            with jax.named_scope("relay_pot"):
                peers(lambda q: pot_copy(q).start())

        return carry

    lax.fori_loop(0, 2, first_half, 0)
    with jax.named_scope("blocks"):
        for tab in tab_loads:
            tab.wait()
        for i in range(2):
            right_blk[i] = block(right_tab[i, 0], right_tab[i, 1])
        kinetic[...] = kinetic_factors(box, window, radix)

    early = lax.rem(me // 8, 2)
    mine_first = early == side
    acc[...] = jnp.zeros_like(acc)

    def row_part(batch, near):
        parity = lax.rem(early + batch, 2)
        row = lax.rem(cell // 4 + near + near // 2 - 2 * (near // 3), 4)
        alone = (parity == side) & (row == cell // 4)

        @pl.when(alone)
        def _():
            val_all(0, batch, row, 3).wait_recv()

        @pl.when(jnp.logical_not(alone))
        def _():
            val_all(0, batch, row, 4).wait_recv()

        return parity, row

    def row_sum(parity, row):
        deep = 4 * slots
        cols = hits.shape[1]
        placed = [[], []]
        for u in range(4):
            to = pl.ds(pl.multiple_of(row * deep + u * slots, slots), slots)
            mask = hits[parity, :, to]
            for n, part in enumerate(split_parts(land[parity, row * 4 + u])):
                part = part.astype(F32)
                pieces = []
                for c in range(2):
                    line_of = jnp.broadcast_to(part[c : c + 1, :], (16, slots)).astype(BF16)
                    pieces.append(mask * jnp.concatenate([line_of] * (cols // 16), axis=0))
                placed[n].append(jnp.concatenate(pieces, axis=0))
        picked = onehot[parity, :, pl.ds(pl.multiple_of(row * deep, deep), deep)]
        high, low = (
            lax.dot_general(
                picked, jnp.concatenate(part, axis=1), (((1,), (1,)), ((), ())), preferred_element_type=F32
            )
            for part in placed
        )
        return high + low

    def collect_pair(pair, carry):
        batch, near = pair // 2, 2 * lax.rem(pair, 2)
        first, second = row_part(batch, near), row_part(batch, near + 1)
        acc[...] += row_sum(*first) + row_sum(*second)
        return carry

    def collect(step, carry):
        acc[...] += row_sum(*row_part(step // 4, lax.rem(step, 4)))
        return carry

    def second_half(turn, carry):
        step, e = turn // 2, lax.rem(side + turn, 2)
        with jax.named_scope("mark1"):
            before = jnp.where(turn == 0, 8, jnp.where(turn == 1, 20, jnp.where(turn == 2, 30, groups)))
            lax.fori_loop(jnp.where(turn == 0, 8, jnp.where(turn == 1, 8, jnp.where(turn == 2, 20, 30))), before, mark, 0)
        @pl.when(turn == 3)
        def _():
            with jax.named_scope("collect0"):
                lax.fori_loop(0, 3 - 2 * side, collect, 0)

        with jax.named_scope("wait_line"):
            line_all(step, e).wait_recv()
        with jax.named_scope("send_val"):
            total = prod[step, 1, line, e]
            for other in range(1, lines):
                total = total + zrecv[step, lax.rem(line + other, lines), e]
            for r in range(2):
                for c in range(2):
                    tout[turn, r * 4 : r * 4 + 4, c, :] = total[r, c * 4 : c * 4 + 4]

            def send(n, carry):
                r = lax.rem(cell // 8 + 1 + n // 4, 2)
                m = lax.rem(n, 4)
                x = lax.rem(cell + jnp.where(m == 0, 2, jnp.where(m == 1, 1, jnp.where(m == 2, 3, 0))), 4)
                to = (r * 8 + lax.rem(side + step, 2) * 4 + x) * 2 + lax.rem(side + e, 2)
                i = r * 4 + x

                @pl.when(to != me)
                def _():
                    val_copy(step, turn, i, (1 - e) * band + e * mirror, to).start()

                @pl.when(to == me)
                def _():
                    land[side, cell] = tout[turn, i]

                return carry

            lax.fori_loop(0, 8, send, 0)
        return carry

    lax.fori_loop(0, 4, second_half, 0)
    with jax.named_scope("pair_pot"):
        pot_all().wait_recv()
        pot_pair().start()

    with jax.named_scope("collect"):
        lax.fori_loop(3 - 2 * side, 4, collect, 0)
        lax.fori_loop(2, 4, collect_pair, 0)
    grid_field = acc[...]

    def pot_ready():
        pot_pair().wait_recv()

    def out_copy(c):
        return pltpu.make_async_copy(out_buf.at[c], out_ref.at[0, c], out_sem.at[c])

    apply_kernel(
        box, window, radix, band >= 0, pot_ready, grid_field, pot_out, right_blk, left_tab, back_tab, twist,
        mixed, unmixed, kinetic, out_buf, lambda c: out_copy(c).start()
    )
    with jax.named_scope("wait_sends"):
        for c in range(2):
            out_copy(c).wait()
        rot_swap().wait_send()
        rot_all(1).wait_send()
        rot_all(2).wait_send()
        pot_swap().wait_send()
        pot_all().wait_send()
        pot_pair().wait_send()
        for step in range(2):
            pair_copy(step).wait_send()
            for e in range(2):
                line_all(step, e).wait_send()
            alone = mine_first if step == 0 else jnp.logical_not(mine_first)

            @pl.when(alone)
            def _():
                val_all(step, 0, 0, plane - 1).wait_send()

            @pl.when(jnp.logical_not(alone))
            def _():
                val_all(step, 0, 0, plane).wait_send()


def run(coefficients, rotation, potential, index_map, counts, consts, box, window, radix):
    bands, groups = lax.axis_size("band"), lax.axis_size("ga")
    depth, _, slots = coefficients.shape
    cols = rotation.shape[2]
    assert (bands, groups, cols) == (8, 32, 8)
    lines, plane = bands // 2, groups // 2
    rot = rotation.transpose(0, 2, 1).reshape(1, 2 * cols, depth)
    hbm = pl.BlockSpec(memory_space=pl.ANY)
    dma = pltpu.SemaphoreType.DMA
    rows, wide = radix * window, window // radix * window
    blocks = (2, lines, 2, 2, 8, slots)
    return pl.pallas_call(
        functools.partial(whole_kernel, box, window, radix),
        out_shape=jax.ShapeDtypeStruct((1, 2, window, window * window), F32),
        in_specs=[hbm] * 9,
        out_specs=hbm,
        scratch_shapes=[
            pltpu.VMEM((2, depth, slots), F32),
            pltpu.VMEM((4, depth, slots), BF16),
            pltpu.VMEM((2 * cols, depth), F32),
            pltpu.VMEM((2, cols, depth), F32),
            pltpu.VMEM((2, plane, 2, cols, depth), F32),
            pltpu.VMEM((2,) + blocks, F32),
            pltpu.VMEM(blocks, F32),
            pltpu.VMEM(blocks, F32),
            pltpu.VMEM((4, 8, 2, slots), F32),
            pltpu.VMEM((2, plane, 2, slots), F32),
            pltpu.VMEM((2, rows, plane * slots), BF16),
            pltpu.VMEM((2, wide, plane * slots), BF16),
            pltpu.VMEM((rows, 2 * wide), F32),
            pltpu.VMEM((1, groups * slots), jnp.int32),
            pltpu.SMEM((groups,), jnp.int32),
            pltpu.VMEM((groups,) + potential.shape, F32),
            *[pltpu.VMEM(table.shape, table.dtype) for table in consts],
            pltpu.VMEM((2, 2 * wide, 2 * radix * box), BF16),
            pltpu.VMEM((2, radix, 2 * window, radix * box), BF16),
            pltpu.VMEM((radix, 2 * window, radix * box), F32),
            pltpu.VMEM((rows, wide), F32),
            pltpu.VMEM((2, window, window * window), F32),
            dma((10,)),
            dma((3,)),
            dma((3,)),
            dma((4,)),
            dma((4,)),
            dma((2,)),
            dma((2,)),
            dma((2, 2)),
            dma((2, 2)),
            dma((2,)),
            dma((2, 4)),
            dma((2,)),
        ],
        compiler_params=pltpu.CompilerParams(
            collective_id=0, has_side_effects=True, vmem_limit_bytes=60 * 1024 * 1024
        ),
    )(coefficients, rot, potential, index_map[None], counts, *consts)


def kinetic_factors(box, window, radix):
    rows, cols = radix * window, window // radix * window
    half = window // 2
    row_at = lax.broadcasted_iota(jnp.int32, (rows, cols), 0)
    col_at = lax.broadcasted_iota(jnp.int32, (rows, cols), 1)
    n_x = (row_at % window - half).astype(F32)
    n_y = (col_at // window * radix + row_at // window - half).astype(F32)
    n_z = (col_at % window - half).astype(F32)
    return (8.0 / (box * box)) * (n_x * n_x + n_y * n_y + n_z * n_z)


def apply_kernel(
    box, window, radix, apart, pot_ready, grid_field, pot_ref, right_ref, left_ref, back_ref, twist_ref,
    mixed_ref, unmixed_ref, kinetic_ref, out_ref, ship
):
    coarse = window // radix
    rows = radix * window
    cols = coarse * window
    wide = radix * box
    lanes = 128
    per = wide // pot_ref.shape[2]

    def columns(tile):
        return slice(tile * lanes, (tile + 1) * lanes), slice(wide + tile * lanes, wide + (tile + 1) * lanes)

    def right_of(tile):
        return [jnp.concatenate([right_ref[i, :, at] for at in columns(tile)], axis=1) for i in range(2)]

    def twist_of(low, at):
        return twist_ref[0, low : low + 1, at], twist_ref[1, low : low + 1, at]

    with jax.named_scope("fwd_mix"):
        parts = split_parts(grid_field)
        for tile in range(wide // lanes):
            at = columns(tile)[0]
            both = dot3(parts, right_of(tile))
            values = []
            for low in range(radix):
                real = both[low * window : (low + 1) * window, :lanes]
                imag = both[low * window : (low + 1) * window, lanes:]
                if low:
                    cos, sin = twist_of(low, at)
                    real, imag = real * cos - imag * sin, real * sin + imag * cos
                values.append((real, imag))
            for k, pair in enumerate(fft8(values, 1)):
                for c in range(2):
                    high, low = split_parts(pair[c])
                    mixed_ref[0, k, c * window : (c + 1) * window, at] = high
                    mixed_ref[1, k, c * window : (c + 1) * window, at] = low
    with jax.named_scope("wait_pot"):
        pot_ready()

    with jax.named_scope("left"):
        @pl.when(apart)
        def _():
            for k in range(radix):
                for n in range(2):
                    at = slice(n * 2 * lanes, (n + 1) * 2 * lanes)
                    high, low = mixed_ref[0, k, :, at], mixed_ref[1, k, :, at]
                    space = jnp.dot(
                        left_ref[...], jnp.concatenate([high, high, low, low], axis=0), preferred_element_type=F32
                    )
                    pot = jnp.concatenate([pot_ref[k * per + 2 * n + i] for i in range(2)], axis=1)
                    high, low = split_parts(space * jnp.concatenate([pot, pot], axis=0))
                    both = jnp.dot(back_ref[...], jnp.concatenate([high, low], axis=0), preferred_element_type=F32)
                    unmixed_ref[k, :, at] = both[: 2 * window] + both[2 * window :]

    def unmix(tile):
        at = columns(tile)[0]
        values = [(unmixed_ref[k, :window, at], unmixed_ref[k, window:, at]) for k in range(radix)]
        halves = [[], []]
        for low, (real, imag) in enumerate(fft8(values, -1)):
            if low:
                cos, sin = twist_of(low, at)
                real, imag = real * cos + imag * sin, imag * cos - real * sin
            split = [split_parts(real), split_parts(imag)]
            for i in range(2):
                halves[i].append(jnp.concatenate([split[0][i], split[1][i]], axis=1))
        turned = [jnp.concatenate(half, axis=0) for half in halves]
        return dot3(turned, right_of(tile), ((1,), (1,)))

    with jax.named_scope("unmix_back"):
        applied = unmix(0)
        for tile in range(1, wide // lanes):
            applied = applied + unmix(tile)

    kinetic = kinetic_ref[...]
    applied = applied + jnp.concatenate([kinetic, kinetic], axis=1) * grid_field
    for c in range(2):
        pieces = [
            applied[lo * window : (lo + 1) * window, c * cols + hi * window : c * cols + (hi + 1) * window]
            for hi in range(coarse)
            for lo in range(radix)
        ]
        out_ref[c] = jnp.concatenate(pieces, axis=1)
        ship(c)


def per_device(coefficients, rotation, potential, index_map, counts):
    box = potential.shape[0]
    window = box // 2
    radix = math.isqrt(box)
    assert radix * radix == box
    consts = [jnp.asarray(t) for t in tables(box, window, radix)]
    return run(coefficients, rotation, potential, index_map, counts, consts, box, window, radix)


def solution(mesh):
    placed = (P("band", None, "ga"), P(None, "band", "ga"), P(None, "ga"), P(), P())
    return jax.shard_map(
        per_device,
        mesh=mesh,
        in_specs=placed,
        out_specs=P(("band", "ga"), None, None, None),
        check_vma=False,
    )
```
